8 devices in a mesh: dp: 2 (over z, y), tp: 4 (over x, core).
Axes of the slice: x: 2, y: 2, z: 1, core: 2. Of those that a mesh axis runs over, the one named last changes fastest.
Arguments:
- hidden: bfloat16 [256, 512], P(('dp', 'tp')), parts along dimension 0
- ln_gain: float32 [512], replicated
- ln_bias: float32 [512], replicated
- out_embed: bfloat16 [50688, 512], P('tp')
- vocab_valid: int32 [50688], P('tp')
- targets: int32 [256], P(('dp', 'tp')), parts along dimension 0
- loss_mask: int32 [256], P(('dp', 'tp')), parts along dimension 0
Outputs:
- output 1: float32 [256], P(('dp', 'tp')), parts along dimension 0
- output 2: float32 [2], P('dp'), parts along dimension 0
- output 3: bfloat16 [256, 512], P(('dp', 'tp')), parts along dimension 0
- output 4: float32 [101376, 512], P(('dp', 'tp')), parts along dimension 0
- output 5: float32 [1024], P('dp'), parts along dimension 0
- output 6: float32 [1024], P('dp'), parts along dimension 0
There are 2 independent parts. The reference program is written for one: setup_inputs(seed, part) draws one part's arguments, and reference() takes and returns one part's arrays. A program takes and returns all parts, laid end to end along the dimension named above; an argument that names none is the same for every part.
All inputs are finite; a program needn't handle non-finite values.
Results may differ from the reference program's by a relative error of at most 0.001.
Values are sent between devices in bfloat16 or wider.
A program may use at most 1 GiB of HBM per device.

```python
import jax
import jax.numpy as jnp
from jax import lax

MODEL_DIM = 512
VOCAB_REAL = 50304
VOCAB_PAD = 50688
SEQ_LEN = 128
TOK_BLOCK = 32
BLOCK_COUNT = SEQ_LEN // TOK_BLOCK
SOFT_CAP = 30.0
Z_COEF = 1e-4
LN_EPS = 1e-5


def layer_norm(h_float, ln_gain, ln_bias):
    mean_val = jnp.mean(h_float, axis=-1, keepdims=True)
    centered = h_float - mean_val
    var_val = jnp.mean(centered * centered, axis=-1, keepdims=True)
    return centered * lax.rsqrt(var_val + LN_EPS) * ln_gain + ln_bias


def draw_layout(shared_key, part_key):
    col_idx = jnp.arange(VOCAB_PAD)
    coin_draw = jax.random.randint(shared_key, (VOCAB_PAD,), 0, 8)
    dropped = (col_idx % 2 == 0) & (coin_draw == 0) & (col_idx < VOCAB_REAL - 1)
    vocab_valid = ((col_idx < VOCAB_REAL) & jnp.logical_not(dropped)).astype(jnp.int32)
    key_tgt, key_pre, key_post, key_hole = jax.random.split(part_key, 4)
    raw_tgt = jax.random.randint(key_tgt, (SEQ_LEN,), 0, VOCAB_REAL)
    targets = raw_tgt + 1 - vocab_valid[raw_tgt]
    positions = jnp.arange(SEQ_LEN)
    prefix_len = jax.random.randint(key_pre, (), 0, SEQ_LEN // 4 + 1)
    suffix_len = jax.random.randint(key_post, (), 0, SEQ_LEN // 4 + 1)
    hole_draw = jax.random.randint(key_hole, (SEQ_LEN,), 0, 8)
    keep_tok = (positions >= prefix_len) & (positions < SEQ_LEN - suffix_len) & (hole_draw != 0)
    keep_tok = keep_tok | (positions == SEQ_LEN // 2)
    return vocab_valid, targets.astype(jnp.int32), keep_tok.astype(jnp.int32)


def setup_inputs(seed: int = 0, part: int = 0) -> dict:
    shared_key = jax.random.key(seed)
    part_key = jax.random.fold_in(jax.random.key(seed + 1), part)
    key_gain, key_bias, key_embed, key_valid = jax.random.split(shared_key, 4)
    key_hidden, key_layout = jax.random.split(part_key, 2)
    hidden = 1.5 * jax.random.normal(key_hidden, (SEQ_LEN, MODEL_DIM), jnp.float32)
    ln_gain = 1.0 + 0.3 * jax.random.normal(key_gain, (MODEL_DIM,), jnp.float32)
    ln_bias = 0.3 * jax.random.normal(key_bias, (MODEL_DIM,), jnp.float32)
    out_embed = (3.0 * MODEL_DIM ** -0.5) * jax.random.normal(key_embed, (VOCAB_PAD, MODEL_DIM), jnp.float32)
    vocab_valid, targets, loss_mask = draw_layout(key_valid, key_layout)
    return {"hidden": hidden.astype(jnp.bfloat16), "ln_gain": ln_gain, "ln_bias": ln_bias, "out_embed": out_embed.astype(jnp.bfloat16), "vocab_valid": vocab_valid, "targets": targets, "loss_mask": loss_mask}


def reference(hidden, ln_gain, ln_bias, out_embed, vocab_valid, targets, loss_mask):
    normed, ln_back = jax.vjp(layer_norm, hidden.astype(jnp.float32), ln_gain, ln_bias)
    x_all = normed.astype(jnp.bfloat16)
    mask_f = loss_mask.astype(jnp.float32)
    tok_count = jnp.sum(mask_f)
    col_ok = (vocab_valid != 0)[None, :]
    col_ids = jnp.arange(VOCAB_PAD)[None, :]

    def block_step(embed_grad, blk_data):
        x_blk, tgt_blk, mask_blk = blk_data
        logits = jnp.dot(x_blk, out_embed.T, preferred_element_type=jnp.float32)
        tanh_val = jnp.tanh(logits / SOFT_CAP)
        capped = SOFT_CAP * tanh_val
        masked = jnp.where(col_ok, capped, -SOFT_CAP)
        row_max = jnp.max(masked, axis=1, keepdims=True)
        exp_vals = jnp.where(col_ok, jnp.exp(masked - row_max), 0.0)
        sum_exp = jnp.sum(exp_vals, axis=1, keepdims=True)
        lse = row_max[:, 0] + jnp.log(sum_exp[:, 0])
        is_target = tgt_blk[:, None] == col_ids
        tgt_logit = jnp.sum(jnp.where(is_target, capped, 0.0), axis=1)
        tok_loss = (lse - tgt_logit + Z_COEF * lse * lse) * mask_blk
        tok_coef = mask_blk / tok_count
        d_capped = ((1.0 + 2.0 * Z_COEF * lse) * tok_coef)[:, None] * (exp_vals / sum_exp) - jnp.where(is_target, tok_coef[:, None], 0.0)
        d_logits = (d_capped * (1.0 - tanh_val * tanh_val)).astype(jnp.bfloat16)
        new_grad = embed_grad + jnp.dot(d_logits.T, x_blk, preferred_element_type=jnp.float32)
        d_normed = jnp.dot(d_logits, out_embed, preferred_element_type=jnp.float32)
        return new_grad, (tok_loss, d_normed)

    init_grad = jnp.zeros((VOCAB_PAD, MODEL_DIM), jnp.float32)
    blk_inputs = (x_all.reshape(BLOCK_COUNT, TOK_BLOCK, MODEL_DIM), targets.reshape(BLOCK_COUNT, TOK_BLOCK), mask_f.reshape(BLOCK_COUNT, TOK_BLOCK))
    d_embed, (tok_loss, d_normed) = lax.scan(block_step, init_grad, blk_inputs)
    tok_loss = tok_loss.reshape(SEQ_LEN)
    d_normed = d_normed.reshape(SEQ_LEN, MODEL_DIM)
    mean_loss = jnp.sum(tok_loss) / tok_count
    d_hidden, d_gain, d_bias = ln_back(d_normed)
    return tok_loss, mean_loss.reshape(1), d_hidden.astype(jnp.bfloat16), d_embed, d_gain, d_bias
```

```python
import functools

import jax
import jax.numpy as jnp
from jax import lax
from jax.experimental import pallas as pl
from jax.experimental.pallas import tpu as pltpu
from jax.sharding import PartitionSpec as P

SOFT_CAP = 30.0
Z_COEF = 1e-4
LN_EPS = 1e-5
LOG2E = 1.4426950408889634
MESH = pl.DeviceIdType.MESH
F32 = jnp.float32
BF16 = jnp.bfloat16

TP = 4
TOK = 128
LOC = TOK // TP
DIM = 512
VOCAB = 12672
TILE = 256
GROUP = 7 * TILE
GROUPS = VOCAB // GROUP
TAIL = VOCAB - GROUP * GROUPS
ROWS_B = 1152


def row_sum(val):
    return jnp.sum(val, axis=-1, keepdims=True)


def main_kernel(
    hid_ref, gain_ref, bias_ref, emb_ref, valid_ref, tgt_ref, mask_ref,
    small_ref, dhid_ref, dz_ref, x_ref,
    emb_v, g_v, hid_all, xh_v, rstd_v, meta_v, stat_v, dx_v, dx_recv, gb_v, acc_v,
    emb_sem, send_sem, recv_sem, dz_sem,
):
    me = lax.axis_index("tp")
    dp = lax.axis_index("dp")
    chunks = [(j * GROUP, GROUP) for j in range(GROUPS - 1)]
    chunks.append(((GROUPS - 1) * GROUP, GROUP + TAIL))
    emb_copies = [
        pltpu.make_async_copy(emb_ref.at[pl.ds(s, n), :], emb_v.at[pl.ds(s, n), :], emb_sem.at[k])
        for k, (s, n) in enumerate(chunks)
    ]
    for cp in emb_copies:
        cp.start()

    barrier = pltpu.get_barrier_semaphore()
    for k in range(1, TP):
        pl.semaphore_signal(barrier, inc=1, device_id=(dp, lax.rem(me + k, TP)), device_id_type=MESH)

    lane = lax.broadcasted_iota(jnp.int32, (1, TOK), 1)
    mine = (lane // LOC) == me
    tgt4 = jnp.concatenate([tgt_ref[...]] * TP, axis=1)
    mask4 = jnp.concatenate([mask_ref[...]] * TP, axis=1)
    my_rows = pl.ds(pl.multiple_of(me * LOC, LOC), LOC)
    my_meta = pl.ds(pl.multiple_of(me * 8, 8), 8)
    meta_v[my_meta, :] = jnp.concatenate(
        [jnp.where(mine, tgt4, 0), jnp.where(mine, mask4, 0), jnp.zeros((6, TOK), jnp.int32)], axis=0
    )
    hid_all[my_rows, :] = hid_ref[...]
    pl.semaphore_wait(barrier, TP - 1)

    def push(src, dst, idx):
        copies = []
        for k in range(1, TP):
            cp = pltpu.make_async_remote_copy(
                src_ref=src(k), dst_ref=dst, send_sem=send_sem.at[3 * idx + k - 1], recv_sem=recv_sem.at[3 * idx + k - 1],
                device_id=(dp, lax.rem(me + k, TP)), device_id_type=MESH,
            )
            cp.start()
            copies.append(cp)
        return copies

    first = push(lambda k: hid_ref, hid_all.at[my_rows, :], 0)
    first += push(lambda k: meta_v.at[my_meta, :], meta_v.at[my_meta, :], 1)
    for cp in first:
        cp.wait_recv()

    meta = meta_v[0:8, :] + meta_v[8:16, :] + meta_v[16:24, :] + meta_v[24:32, :]
    tgt_row = meta[0:1, :]
    mask_row = meta[1:2, :].astype(F32)
    tok_count = row_sum(mask_row)
    tgt_col = jnp.transpose(jnp.broadcast_to(tgt_row, (TOK, TOK)))

    h = hid_all[...].astype(F32)
    mean_val = row_sum(h) * (1.0 / DIM)
    cent = h - mean_val
    var_val = row_sum(cent * cent) * (1.0 / DIM)
    rstd = lax.rsqrt(var_val + LN_EPS)
    xh = cent * rstd
    xh_v[...] = xh
    rstd_v[...] = jnp.broadcast_to(rstd, (TOK, TOK))
    x_ref[...] = (xh * gain_ref[...] + bias_ref[...]).astype(BF16)

    col0 = lax.broadcasted_iota(jnp.int32, (TOK, TOK), 1)
    base = me * VOCAB
    tgt_loc = tgt_col - base

    def fwd(start, size):
        z = lax.dot_general(
            x_ref[...], emb_v[pl.ds(start, size), :], (((1,), (1,)), ((), ())), preferred_element_type=F32
        )
        t = jnp.tanh(z * (1.0 / SOFT_CAP))
        ok = valid_ref[:, pl.ds(start, size)].astype(F32)
        e = jnp.exp2(t * (SOFT_CAP * LOG2E)) * ok
        g_v[:, pl.ds(start, size)] = e * (1.0 - t * t)
        s_sum = 0.0
        t_sum = 0.0
        for c in range(size // TOK):
            cols = slice(c * TOK, (c + 1) * TOK)
            s_sum += e[:, cols]
            t_sum += jnp.where(tgt_loc - (start + c * TOK) == col0, t[:, cols], 0.0)
        return s_sum, t_sum

    acc_v[...] = jnp.zeros_like(acc_v)
    for j, (g0, n) in enumerate(chunks):
        emb_copies[j].wait()
        s_acc = 0.0
        t_acc = 0.0
        for s in range(0, n, TILE):
            ds, dt = fwd(g0 + s, min(TILE, n - s))
            s_acc += ds
            t_acc += dt
        acc_v[0] += s_acc
        acc_v[1] += t_acc

    s_loc = jnp.sum(jnp.transpose(acc_v[0]), axis=0, keepdims=True)
    t_loc = jnp.sum(jnp.transpose(acc_v[1]), axis=0, keepdims=True)
    stat_v[my_meta, :] = jnp.concatenate([s_loc, t_loc, jnp.zeros((6, TOK), F32)], axis=0)
    second = push(lambda k: stat_v.at[my_meta, :], stat_v.at[my_meta, :], 2)
    for cp in second:
        cp.wait_recv()
    stats = stat_v[0:8, :] + stat_v[8:16, :] + stat_v[16:24, :] + stat_v[24:32, :]
    sum_exp = stats[0:1, :]
    t_tgt = stats[1:2, :]
    lse = jnp.log(sum_exp)
    loss = (lse - SOFT_CAP * t_tgt + Z_COEF * lse * lse) * mask_row
    mean_loss = row_sum(loss) / tok_count
    coef = mask_row / tok_count
    a_row = (1.0 + 2.0 * Z_COEF * lse) * coef / sum_exp
    c_row = coef * (1.0 - t_tgt * t_tgt)
    a_col = jnp.transpose(jnp.broadcast_to(a_row, (TOK, TOK)))
    c_col = jnp.transpose(jnp.broadcast_to(c_row, (TOK, TOK)))

    def grad(start, size):
        parts = []
        for c in range(size // TOK):
            hit = tgt_loc - (start + c * TOK) == col0
            parts.append(a_col * g_v[:, pl.ds(start + c * TOK, TOK)] - jnp.where(hit, c_col, 0.0))
        return jnp.concatenate(parts, axis=1).astype(BF16)

    dz_copies = []
    for j, (g0, n) in enumerate(chunks):
        dz = grad(g0, n)
        dz_ref[:, pl.ds(g0, n)] = dz
        part = jnp.dot(dz, emb_v[pl.ds(g0, n), :], preferred_element_type=F32)
        dx_v[...] = part if j == 0 else dx_v[...] + part

    dx = dx_v[...]
    gb_v[my_meta, :] = jnp.concatenate(
        [jnp.sum(dx * xh_v[...], axis=0, keepdims=True), jnp.sum(dx, axis=0, keepdims=True), jnp.zeros((6, DIM), F32)], axis=0
    )
    dx_recv[my_rows, :] = dx_v[my_rows, :]

    def peer_rows(k):
        return dx_v.at[pl.ds(pl.multiple_of(lax.rem(me + k, TP) * LOC, LOC), LOC), :]

    third = push(peer_rows, dx_recv.at[my_rows, :], 3)
    third += push(lambda k: gb_v.at[my_meta, :], gb_v.at[my_meta, :], 4)
    for cp in third:
        cp.wait_recv()
    d_norm = dx_recv[0:LOC, :] + dx_recv[LOC:2 * LOC, :] + dx_recv[2 * LOC:3 * LOC, :] + dx_recv[3 * LOC:, :]
    gb = gb_v[0:8, :] + gb_v[8:16, :] + gb_v[16:24, :] + gb_v[24:32, :]
    xh_me = xh_v[my_rows, :]
    dxh = d_norm * gain_ref[...]
    m1 = row_sum(dxh) * (1.0 / DIM)
    m2 = row_sum(dxh * xh_me) * (1.0 / DIM)
    dhid_ref[...] = (rstd_v[my_rows, 0:1] * (dxh - m1 - xh_me * m2)).astype(BF16)
    loss_me = pltpu.roll(loss, lax.rem(TOK - me * LOC, TOK), 1)
    pad = jnp.zeros((1, DIM - TOK), F32)
    small_ref[...] = jnp.concatenate(
        [
            gb[0:2, :],
            jnp.concatenate([loss_me, pad], axis=1),
            jnp.broadcast_to(mean_loss, (1, DIM)),
            jnp.zeros((4, DIM), F32),
        ],
        axis=0,
    )
    for cp in first + second + third:
        cp.wait_send()


def embed_kernel(dz_ref, x_ref, small_ref, dhid_in, demb_ref, tok_ref, mean_ref, dhid_ref, gain_ref, bias_ref):
    demb_ref[...] = lax.dot_general(dz_ref[...], x_ref[...], (((0,), (0,)), ((), ())), preferred_element_type=F32)

    @pl.when(pl.program_id(0) == 0)
    def _():
        gain_ref[...] = small_ref[0:1, :]
        bias_ref[...] = small_ref[1:2, :]
        tok_ref[...] = small_ref[2:3, 0:LOC]
        mean_ref[...] = small_ref[3:4, 0:1]
        dhid_ref[...] = dhid_in[...]


def solution(mesh):
    vmem = pl.BlockSpec(memory_space=pltpu.VMEM)
    hbm = pl.BlockSpec(memory_space=pl.ANY)

    def group_step(hidden, ln_gain, ln_bias, out_embed, vocab_valid, targets, loss_mask):
        small, dhid, dz, x_all = pl.pallas_call(
            main_kernel,
            out_shape=(
                jax.ShapeDtypeStruct((8, DIM), F32),
                jax.ShapeDtypeStruct((LOC, DIM), BF16),
                jax.ShapeDtypeStruct((TOK, VOCAB), BF16),
                jax.ShapeDtypeStruct((TOK, DIM), BF16),
            ),
            in_specs=[vmem, vmem, vmem, hbm, vmem, vmem, vmem],
            out_specs=(vmem, vmem, vmem, vmem),
            scratch_shapes=[
                pltpu.VMEM((VOCAB, DIM), BF16),
                pltpu.VMEM((TOK, VOCAB), F32),
                pltpu.VMEM((TOK, DIM), BF16),
                pltpu.VMEM((TOK, DIM), F32),
                pltpu.VMEM((TOK, TOK), F32),
                pltpu.VMEM((8 * TP, TOK), jnp.int32),
                pltpu.VMEM((8 * TP, TOK), F32),
                pltpu.VMEM((TOK, DIM), F32),
                pltpu.VMEM((TOK, DIM), F32),
                pltpu.VMEM((8 * TP, DIM), F32),
                pltpu.VMEM((2, TOK, TOK), F32),
                pltpu.SemaphoreType.DMA((GROUPS,)),
                pltpu.SemaphoreType.DMA((15,)),
                pltpu.SemaphoreType.DMA((15,)),
                pltpu.SemaphoreType.DMA((GROUPS,)),
            ],
            compiler_params=pltpu.CompilerParams(collective_id=0, has_side_effects=True, vmem_limit_bytes=40 * 1024 * 1024),
            name="main",
        )(
            hidden, ln_gain.reshape(1, DIM), ln_bias.reshape(1, DIM), out_embed, vocab_valid.reshape(1, VOCAB),
            targets.reshape(1, LOC), loss_mask.reshape(1, LOC),
        )
        keep = lambda r, c: pl.BlockSpec((r, c), lambda i: (0, 0))
        d_embed, tok, mean, d_hidden, d_gain, d_bias = pl.pallas_call(
            embed_kernel,
            grid=(VOCAB // ROWS_B,),
            out_shape=(
                jax.ShapeDtypeStruct((VOCAB, DIM), F32),
                jax.ShapeDtypeStruct((1, LOC), F32),
                jax.ShapeDtypeStruct((1, 1), F32),
                jax.ShapeDtypeStruct((LOC, DIM), BF16),
                jax.ShapeDtypeStruct((1, DIM), F32),
                jax.ShapeDtypeStruct((1, DIM), F32),
            ),
            in_specs=[pl.BlockSpec((TOK, ROWS_B), lambda i: (0, i)), keep(TOK, DIM), keep(8, DIM), keep(LOC, DIM)],
            out_specs=(
                pl.BlockSpec((ROWS_B, DIM), lambda i: (i, 0)),
                keep(1, LOC), keep(1, 1), keep(LOC, DIM), keep(1, DIM), keep(1, DIM),
            ),
            compiler_params=pltpu.CompilerParams(vmem_limit_bytes=24 * 1024 * 1024),
            name="embed",
        )(dz, x_all, small, dhid)
        return tok.reshape(LOC), mean.reshape(1), d_hidden, d_embed, d_gain.reshape(DIM), d_bias.reshape(DIM)

    row_spec = P(("dp", "tp"))
    mat_spec = P(("dp", "tp"), None)
    return jax.shard_map(
        group_step, mesh=mesh,
        in_specs=(mat_spec, P(None), P(None), P("tp", None), P("tp"), row_spec, row_spec),
        out_specs=(row_spec, P("dp"), mat_spec, mat_spec, P("dp"), P("dp")), check_vma=False,
    )
```

```python
import functools

import jax
import jax.numpy as jnp
from jax import lax
from jax.experimental import pallas as pl
from jax.experimental.pallas import tpu as pltpu
from jax.sharding import PartitionSpec as P

SOFT_CAP = 30.0
Z_COEF = 1e-4
LN_EPS = 1e-5
LOG2E = 1.4426950408889634
MESH = pl.DeviceIdType.MESH
F32 = jnp.float32
BF16 = jnp.bfloat16

TP = 4
TOK = 128
LOC = TOK // TP
DIM = 512
VOCAB = 12672
TILE = 256
GROUP = 7 * TILE
GROUPS = VOCAB // GROUP
TAIL = VOCAB - GROUP * GROUPS


def row_sum(val):
    return jnp.sum(val, axis=-1, keepdims=True)


def main_kernel(
    hid_hbm, gain_hbm, bias_hbm, emb_ref, valid_hbm, tgt_hbm, mask_hbm,
    small_ref, dhid_ref, dz_ref, x_ref,
    hid_ref, gain_ref, bias_ref, valid_ref, tgt_ref, mask_ref,
    emb_v, g_v, hid_all, xh_v, rstd_v, meta_v, stat_v, dx_v, dx_recv, gb_v, acc_v,
    emb_sem, send_sem, recv_sem, in_sem,
):
    me = lax.axis_index("tp")
    dp = lax.axis_index("dp")
    ins = [
        pltpu.make_async_copy(src, dst, in_sem.at[k])
        for k, (src, dst) in enumerate([
            (hid_hbm, hid_ref), (tgt_hbm, tgt_ref), (mask_hbm, mask_ref),
            (gain_hbm, gain_ref), (bias_hbm, bias_ref), (valid_hbm, valid_ref),
        ])
    ]
    for cp in ins:
        cp.start()
    chunks = [(j * GROUP, GROUP) for j in range(GROUPS - 1)]
    chunks.append(((GROUPS - 1) * GROUP, GROUP + TAIL))
    emb_copies = [
        pltpu.make_async_copy(emb_ref.at[pl.ds(s, n), :], emb_v.at[pl.ds(s, n), :], emb_sem.at[k])
        for k, (s, n) in enumerate(chunks)
    ]
    for cp in emb_copies:
        cp.start()

    barrier = pltpu.get_barrier_semaphore()
    for k in range(1, TP):
        pl.semaphore_signal(barrier, inc=1, device_id=(dp, lax.rem(me + k, TP)), device_id_type=MESH)

    for cp in ins[:3]:
        cp.wait()
    lane = lax.broadcasted_iota(jnp.int32, (1, TOK), 1)
    mine = (lane // LOC) == me
    tgt4 = jnp.concatenate([tgt_ref[...]] * TP, axis=1)
    mask4 = jnp.concatenate([mask_ref[...]] * TP, axis=1)
    my_rows = pl.ds(pl.multiple_of(me * LOC, LOC), LOC)
    my_meta = pl.ds(pl.multiple_of(me * 8, 8), 8)
    meta_v[my_meta, :] = jnp.concatenate(
        [jnp.where(mine, tgt4, 0), jnp.where(mine, mask4, 0), jnp.zeros((6, TOK), jnp.int32)], axis=0
    )
    hid_all[my_rows, :] = hid_ref[...]
    pl.semaphore_wait(barrier, TP - 1)

    def push(src, dst, idx):
        copies = []
        for k in range(1, TP):
            cp = pltpu.make_async_remote_copy(
                src_ref=src(k), dst_ref=dst, send_sem=send_sem.at[3 * idx + k - 1], recv_sem=recv_sem.at[3 * idx + k - 1],
                device_id=(dp, lax.rem(me + k, TP)), device_id_type=MESH,
            )
            cp.start()
            copies.append(cp)
        return copies

    first = push(lambda k: hid_ref, hid_all.at[my_rows, :], 0)
    first += push(lambda k: meta_v.at[my_meta, :], meta_v.at[my_meta, :], 1)
    for cp in ins[3:]:
        cp.wait()
    for cp in first:
        cp.wait_recv()

    meta = meta_v[0:8, :] + meta_v[8:16, :] + meta_v[16:24, :] + meta_v[24:32, :]
    tgt_row = meta[0:1, :]
    mask_row = meta[1:2, :].astype(F32)
    tok_count = row_sum(mask_row)
    tgt_col = jnp.transpose(jnp.broadcast_to(tgt_row, (TOK, TOK)))

    h = hid_all[...].astype(F32)
    mean_val = row_sum(h) * (1.0 / DIM)
    cent = h - mean_val
    var_val = row_sum(cent * cent) * (1.0 / DIM)
    rstd = lax.rsqrt(var_val + LN_EPS)
    xh = cent * rstd
    xh_v[...] = xh
    rstd_v[...] = jnp.broadcast_to(rstd, (TOK, TOK))
    x_ref[...] = (xh * gain_ref[...] + bias_ref[...]).astype(BF16)

    col0 = lax.broadcasted_iota(jnp.int32, (TOK, TOK), 1)
    base = me * VOCAB
    tgt_loc = tgt_col - base

    def fwd(start, size):
        z = lax.dot_general(
            x_ref[...], emb_v[pl.ds(start, size), :], (((1,), (1,)), ((), ())), preferred_element_type=F32
        )
        t = jnp.tanh(z * (1.0 / SOFT_CAP))
        ok = jnp.concatenate([valid_ref[c:c + 1, :] for c in range(start // TOK, (start + size) // TOK)], axis=1)
        e = jnp.exp2(t * (SOFT_CAP * LOG2E)) * ok.astype(F32)
        g_v[:, pl.ds(start, size)] = e * (1.0 - t * t)
        s_sum = 0.0
        t_sum = 0.0
        for c in range(size // TOK):
            cols = slice(c * TOK, (c + 1) * TOK)
            s_sum += e[:, cols]
            t_sum += jnp.where(tgt_loc - (start + c * TOK) == col0, t[:, cols], 0.0)
        return s_sum, t_sum

    acc_v[...] = jnp.zeros_like(acc_v)
    for j, (g0, n) in enumerate(chunks):
        emb_copies[j].wait()
        s_acc = 0.0
        t_acc = 0.0
        for s in range(0, n, TILE):
            ds, dt = fwd(g0 + s, min(TILE, n - s))
            s_acc += ds
            t_acc += dt
        acc_v[0] += s_acc
        acc_v[1] += t_acc

    s_loc = jnp.sum(jnp.transpose(acc_v[0]), axis=0, keepdims=True)
    t_loc = jnp.sum(jnp.transpose(acc_v[1]), axis=0, keepdims=True)
    stat_v[my_meta, :] = jnp.concatenate([s_loc, t_loc, jnp.zeros((6, TOK), F32)], axis=0)
    second = push(lambda k: stat_v.at[my_meta, :], stat_v.at[my_meta, :], 2)
    for cp in second:
        cp.wait_recv()
    stats = stat_v[0:8, :] + stat_v[8:16, :] + stat_v[16:24, :] + stat_v[24:32, :]
    sum_exp = stats[0:1, :]
    t_tgt = stats[1:2, :]
    lse = jnp.log(sum_exp)
    loss = (lse - SOFT_CAP * t_tgt + Z_COEF * lse * lse) * mask_row
    mean_loss = row_sum(loss) / tok_count
    coef = mask_row / tok_count
    a_row = (1.0 + 2.0 * Z_COEF * lse) * coef / sum_exp
    c_row = coef * (1.0 - t_tgt * t_tgt)
    a_col = jnp.transpose(jnp.broadcast_to(a_row, (TOK, TOK)))
    c_col = jnp.transpose(jnp.broadcast_to(c_row, (TOK, TOK)))

    def grad(start, size):
        parts = []
        for c in range(size // TOK):
            hit = tgt_loc - (start + c * TOK) == col0
            parts.append(a_col * g_v[:, pl.ds(start + c * TOK, TOK)] - jnp.where(hit, c_col, 0.0))
        return jnp.concatenate(parts, axis=1).astype(BF16)

    dz_copies = []
    for j, (g0, n) in enumerate(chunks):
        dz = grad(g0, n)
        dz_ref[:, pl.ds(g0, n)] = dz
        part = jnp.dot(dz, emb_v[pl.ds(g0, n), :], preferred_element_type=F32)
        dx_v[...] = part if j == 0 else dx_v[...] + part

    dx = dx_v[...]
    gb_v[my_meta, :] = jnp.concatenate(
        [jnp.sum(dx * xh_v[...], axis=0, keepdims=True), jnp.sum(dx, axis=0, keepdims=True), jnp.zeros((6, DIM), F32)], axis=0
    )
    dx_recv[my_rows, :] = dx_v[my_rows, :]

    def peer_rows(k):
        return dx_v.at[pl.ds(pl.multiple_of(lax.rem(me + k, TP) * LOC, LOC), LOC), :]

    third = push(peer_rows, dx_recv.at[my_rows, :], 3)
    third += push(lambda k: gb_v.at[my_meta, :], gb_v.at[my_meta, :], 4)
    for cp in third:
        cp.wait_recv()
    d_norm = dx_recv[0:LOC, :] + dx_recv[LOC:2 * LOC, :] + dx_recv[2 * LOC:3 * LOC, :] + dx_recv[3 * LOC:, :]
    gb = gb_v[0:8, :] + gb_v[8:16, :] + gb_v[16:24, :] + gb_v[24:32, :]
    xh_me = xh_v[my_rows, :]
    dxh = d_norm * gain_ref[...]
    m1 = row_sum(dxh) * (1.0 / DIM)
    m2 = row_sum(dxh * xh_me) * (1.0 / DIM)
    dhid_ref[...] = (rstd_v[my_rows, 0:1] * (dxh - m1 - xh_me * m2)).astype(BF16)
    loss_me = pltpu.roll(loss, lax.rem(TOK - me * LOC, TOK), 1)
    pad = jnp.zeros((1, DIM - TOK), F32)
    small_ref[...] = jnp.concatenate(
        [
            gb[0:2, :],
            jnp.concatenate([loss_me, pad], axis=1),
            jnp.broadcast_to(mean_loss, (1, DIM)),
            jnp.zeros((4, DIM), F32),
        ],
        axis=0,
    )
    for cp in first + second + third:
        cp.wait_send()


OUT_TILES = [384] + [768] * 16


def embed_kernel(dz_ref, x_ref, small_ref, dhid_in, demb_ref, tok_ref, mean_ref, dhid_ref, gain_ref, bias_ref, stage, out_sem):
    copies = []
    start = 0
    for k, n in enumerate(OUT_TILES):
        rows = pl.ds(start, n)
        stage[rows, :] = lax.dot_general(
            dz_ref[:, rows], x_ref[...], (((0,), (0,)), ((), ())), preferred_element_type=F32
        )
        cp = pltpu.make_async_copy(stage.at[rows, :], demb_ref.at[rows, :], out_sem.at[k])
        cp.start()
        copies.append(cp)
        start += n
    gain_ref[...] = small_ref[0:1, :]
    bias_ref[...] = small_ref[1:2, :]
    tok_ref[...] = small_ref[2:3, 0:LOC]
    mean_ref[...] = small_ref[3:4, 0:1]
    dhid_ref[...] = dhid_in[...]
    for cp in copies:
        cp.wait()


def solution(mesh):
    vmem = pl.BlockSpec(memory_space=pltpu.VMEM)
    hbm = pl.BlockSpec(memory_space=pltpu.HBM)

    def group_step(hidden, ln_gain, ln_bias, out_embed, vocab_valid, targets, loss_mask):
        small, dhid, dz, x_all = pl.pallas_call(
            main_kernel,
            out_shape=(
                jax.ShapeDtypeStruct((8, DIM), F32),
                jax.ShapeDtypeStruct((LOC, DIM), BF16),
                jax.ShapeDtypeStruct((TOK, VOCAB), BF16),
                jax.ShapeDtypeStruct((TOK, DIM), BF16),
            ),
            in_specs=[hbm] * 7,
            out_specs=(vmem, vmem, vmem, vmem),
            scratch_shapes=[
                pltpu.VMEM((LOC, DIM), BF16),
                pltpu.VMEM((1, DIM), F32),
                pltpu.VMEM((1, DIM), F32),
                pltpu.VMEM((VOCAB // TOK, TOK), jnp.int32),
                pltpu.VMEM((1, LOC), jnp.int32),
                pltpu.VMEM((1, LOC), jnp.int32),
                pltpu.VMEM((VOCAB, DIM), BF16),
                pltpu.VMEM((TOK, VOCAB), F32),
                pltpu.VMEM((TOK, DIM), BF16),
                pltpu.VMEM((TOK, DIM), F32),
                pltpu.VMEM((TOK, TOK), F32),
                pltpu.VMEM((8 * TP, TOK), jnp.int32),
                pltpu.VMEM((8 * TP, TOK), F32),
                pltpu.VMEM((TOK, DIM), F32),
                pltpu.VMEM((TOK, DIM), F32),
                pltpu.VMEM((8 * TP, DIM), F32),
                pltpu.VMEM((2, TOK, TOK), F32),
                pltpu.SemaphoreType.DMA((GROUPS,)),
                pltpu.SemaphoreType.DMA((15,)),
                pltpu.SemaphoreType.DMA((15,)),
                pltpu.SemaphoreType.DMA((6,)),
            ],
            compiler_params=pltpu.CompilerParams(collective_id=0, has_side_effects=True, vmem_limit_bytes=40 * 1024 * 1024),
            name="main",
        )(
            *(
                pltpu.with_memory_space_constraint(val, pltpu.HBM)
                for val in (
                    hidden, ln_gain.reshape(1, DIM), ln_bias.reshape(1, DIM), out_embed,
                    vocab_valid.reshape(VOCAB // TOK, TOK), targets.reshape(1, LOC), loss_mask.reshape(1, LOC),
                )
            )
        )
        d_embed, tok, mean, d_hidden, d_gain, d_bias = pl.pallas_call(
            embed_kernel,
            out_shape=(
                jax.ShapeDtypeStruct((VOCAB, DIM), F32),
                jax.ShapeDtypeStruct((1, LOC), F32),
                jax.ShapeDtypeStruct((1, 1), F32),
                jax.ShapeDtypeStruct((LOC, DIM), BF16),
                jax.ShapeDtypeStruct((1, DIM), F32),
                jax.ShapeDtypeStruct((1, DIM), F32),
            ),
            in_specs=[vmem] * 4,
            out_specs=(hbm, vmem, vmem, vmem, vmem, vmem),
            scratch_shapes=[pltpu.VMEM((VOCAB, DIM), F32), pltpu.SemaphoreType.DMA((len(OUT_TILES),))],
            compiler_params=pltpu.CompilerParams(vmem_limit_bytes=36 * 1024 * 1024),
            name="embed",
        )(dz, x_all, small, dhid)
        return tok.reshape(LOC), mean.reshape(1), d_hidden, d_embed, d_gain.reshape(DIM), d_bias.reshape(DIM)

    row_spec = P(("dp", "tp"))
    mat_spec = P(("dp", "tp"), None)
    return jax.shard_map(
        group_step, mesh=mesh,
        in_specs=(mat_spec, P(None), P(None), P("tp", None), P("tp"), row_spec, row_spec),
        out_specs=(row_spec, P("dp"), mat_spec, mat_spec, P("dp"), P("dp")), check_vma=False,
    )
```

```python
import functools

import jax
import jax.numpy as jnp
from jax import lax
from jax.experimental import pallas as pl
from jax.experimental.pallas import tpu as pltpu
from jax.sharding import PartitionSpec as P

SOFT_CAP = 30.0
Z_COEF = 1e-4
LN_EPS = 1e-5
LOG2E = 1.4426950408889634
MESH = pl.DeviceIdType.MESH
F32 = jnp.float32
BF16 = jnp.bfloat16

TP = 4
TOK = 128
LOC = TOK // TP
DIM = 512
VOCAB = 12672
TILE = 256
GROUP = 7 * TILE
GROUPS = VOCAB // GROUP
TAIL = VOCAB - GROUP * GROUPS


def row_sum(val):
    return jnp.sum(val, axis=-1, keepdims=True)


def main_kernel(
    hid_hbm, gain_hbm, bias_hbm, emb_ref, valid_hbm, tgt_hbm, mask_hbm,
    small_ref, norm_ref, rstd_ref, dz_ref, x_ref, pay0, pay1, pay2, pay3,
    hid_ref, gain_ref, bias_ref, valid_ref, tgt_ref, mask_ref,
    emb_v, g_v, hid_all, xh_v, rstd_v, meta_v, stat_v, dx_v, acc_v,
    emb_sem, send_sem, recv_sem, in_sem,
):
    me = lax.axis_index("tp")
    dp = lax.axis_index("dp")
    pays = (pay0, pay1, pay2, pay3)
    ins = [
        pltpu.make_async_copy(src, dst, in_sem.at[k])
        for k, (src, dst) in enumerate([
            (hid_hbm, hid_ref), (tgt_hbm, tgt_ref), (mask_hbm, mask_ref),
            (gain_hbm, gain_ref), (bias_hbm, bias_ref), (valid_hbm, valid_ref),
        ])
    ]
    for cp in ins:
        cp.start()
    chunks = [(j * GROUP, GROUP) for j in range(GROUPS - 1)]
    chunks.append(((GROUPS - 1) * GROUP, GROUP + TAIL))
    emb_copies = [
        pltpu.make_async_copy(emb_ref.at[pl.ds(s, n), :], emb_v.at[pl.ds(s, n), :], emb_sem.at[k])
        for k, (s, n) in enumerate(chunks)
    ]
    for cp in emb_copies:
        cp.start()

    barrier = pltpu.get_barrier_semaphore()
    for k in range(1, TP):
        pl.semaphore_signal(barrier, inc=1, device_id=(dp, lax.rem(me + k, TP)), device_id_type=MESH)

    for cp in ins[:3]:
        cp.wait()
    lane = lax.broadcasted_iota(jnp.int32, (1, TOK), 1)
    mine = (lane // LOC) == me
    tgt4 = jnp.concatenate([tgt_ref[...]] * TP, axis=1)
    mask4 = jnp.concatenate([mask_ref[...]] * TP, axis=1)
    my_rows = pl.ds(pl.multiple_of(me * LOC, LOC), LOC)
    my_meta = pl.ds(pl.multiple_of(me * 8, 8), 8)
    meta_v[my_meta, :] = jnp.concatenate(
        [jnp.where(mine, tgt4, 0), jnp.where(mine, mask4, 0), jnp.zeros((6, TOK), jnp.int32)], axis=0
    )
    hid_all[my_rows, :] = hid_ref[...]
    pl.semaphore_wait(barrier, TP - 1)

    def push(src, dst, idx):
        copies = []
        for k in range(1, TP):
            cp = pltpu.make_async_remote_copy(
                src_ref=src(k), dst_ref=dst, send_sem=send_sem.at[3 * idx + k - 1], recv_sem=recv_sem.at[3 * idx + k - 1],
                device_id=(dp, lax.rem(me + k, TP)), device_id_type=MESH,
            )
            cp.start()
            copies.append(cp)
        return copies

    first = push(lambda k: hid_ref, hid_all.at[my_rows, :], 0)
    first += push(lambda k: meta_v.at[my_meta, :], meta_v.at[my_meta, :], 1)
    for cp in ins[3:]:
        cp.wait()
    for cp in first:
        cp.wait_recv()

    meta = meta_v[0:8, :] + meta_v[8:16, :] + meta_v[16:24, :] + meta_v[24:32, :]
    tgt_row = meta[0:1, :]
    mask_row = meta[1:2, :].astype(F32)
    tok_count = row_sum(mask_row)
    tgt_col = jnp.transpose(jnp.broadcast_to(tgt_row, (TOK, TOK)))

    h = hid_all[...].astype(F32)
    mean_val = row_sum(h) * (1.0 / DIM)
    cent = h - mean_val
    var_val = row_sum(cent * cent) * (1.0 / DIM)
    rstd = lax.rsqrt(var_val + LN_EPS)
    xh = cent * rstd
    xh_v[...] = xh
    rstd_v[...] = jnp.broadcast_to(rstd, (TOK, TOK))
    x_ref[...] = (xh * gain_ref[...] + bias_ref[...]).astype(BF16)

    col0 = lax.broadcasted_iota(jnp.int32, (TOK, TOK), 1)
    base = me * VOCAB
    tgt_loc = tgt_col - base

    def fwd(start, size):
        z = lax.dot_general(
            x_ref[...], emb_v[pl.ds(start, size), :], (((1,), (1,)), ((), ())), preferred_element_type=F32
        )
        t = jnp.tanh(z * (1.0 / SOFT_CAP))
        ok = jnp.concatenate([valid_ref[c:c + 1, :] for c in range(start // TOK, (start + size) // TOK)], axis=1)
        e = jnp.exp2(t * (SOFT_CAP * LOG2E)) * ok.astype(F32)
        g_v[:, pl.ds(start, size)] = e * (1.0 - t * t)
        s_sum = 0.0
        t_sum = 0.0
        for c in range(size // TOK):
            cols = slice(c * TOK, (c + 1) * TOK)
            s_sum += e[:, cols]
            t_sum += jnp.where(tgt_loc - (start + c * TOK) == col0, t[:, cols], 0.0)
        return s_sum, t_sum

    acc_v[...] = jnp.zeros_like(acc_v)
    for j, (g0, n) in enumerate(chunks):
        emb_copies[j].wait()
        s_acc = 0.0
        t_acc = 0.0
        for s in range(0, n, TILE):
            ds, dt = fwd(g0 + s, min(TILE, n - s))
            s_acc += ds
            t_acc += dt
        acc_v[0] += s_acc
        acc_v[1] += t_acc

    s_loc = jnp.sum(jnp.transpose(acc_v[0]), axis=0, keepdims=True)
    t_loc = jnp.sum(jnp.transpose(acc_v[1]), axis=0, keepdims=True)
    stat_v[my_meta, :] = jnp.concatenate([s_loc, t_loc, jnp.zeros((6, TOK), F32)], axis=0)
    second = push(lambda k: stat_v.at[my_meta, :], stat_v.at[my_meta, :], 2)
    for cp in second:
        cp.wait_recv()
    stats = stat_v[0:8, :] + stat_v[8:16, :] + stat_v[16:24, :] + stat_v[24:32, :]
    sum_exp = stats[0:1, :]
    t_tgt = stats[1:2, :]
    lse = jnp.log(sum_exp)
    loss = (lse - SOFT_CAP * t_tgt + Z_COEF * lse * lse) * mask_row
    mean_loss = row_sum(loss) / tok_count
    coef = mask_row / tok_count
    a_row = (1.0 + 2.0 * Z_COEF * lse) * coef / sum_exp
    c_row = coef * (1.0 - t_tgt * t_tgt)
    a_col = jnp.transpose(jnp.broadcast_to(a_row, (TOK, TOK)))
    c_col = jnp.transpose(jnp.broadcast_to(c_row, (TOK, TOK)))

    def grad(start, size):
        parts = []
        for c in range(size // TOK):
            hit = tgt_loc - (start + c * TOK) == col0
            parts.append(a_col * g_v[:, pl.ds(start + c * TOK, TOK)] - jnp.where(hit, c_col, 0.0))
        return jnp.concatenate(parts, axis=1).astype(BF16)

    dz_copies = []
    for j, (g0, n) in enumerate(chunks):
        dz = grad(g0, n)
        dz_ref[:, pl.ds(g0, n)] = dz
        part = jnp.dot(dz, emb_v[pl.ds(g0, n), :], preferred_element_type=F32)
        dx_v[...] = part if j == 0 else dx_v[...] + part

    dx = dx_v[...]
    gb = jnp.concatenate(
        [jnp.sum(dx * xh_v[...], axis=0, keepdims=True), jnp.sum(dx, axis=0, keepdims=True), jnp.zeros((6, DIM), F32)], axis=0
    )
    for k, pay in enumerate(pays):
        rows = pl.ds(pl.multiple_of(lax.rem(me + k, TP) * LOC, LOC), LOC)
        pay[0:LOC, :] = dx_v[rows, :]
        pay[LOC:, :] = gb
    norm_ref[0:LOC, :] = xh_v[my_rows, :]
    norm_ref[LOC:, :] = jnp.broadcast_to(gain_ref[...], (8, DIM))
    rstd_ref[...] = rstd_v[my_rows, :]
    loss_me = pltpu.roll(loss, lax.rem(TOK - me * LOC, TOK), 1)
    pad = jnp.zeros((1, DIM - TOK), F32)
    small_ref[...] = jnp.concatenate(
        [
            jnp.concatenate([loss_me, pad], axis=1),
            jnp.broadcast_to(mean_loss, (1, DIM)),
            jnp.zeros((6, DIM), F32),
        ],
        axis=0,
    )
    for cp in first + second:
        cp.wait_send()


OUT_TILES = [384] + [768] * 16


def embed_kernel(dz_ref, x_ref, small_ref, demb_ref, tok_ref, mean_ref, stage, out_sem):
    copies = []
    start = 0
    for k, n in enumerate(OUT_TILES):
        rows = pl.ds(start, n)
        stage[rows, :] = lax.dot_general(
            dz_ref[:, rows], x_ref[...], (((0,), (0,)), ((), ())), preferred_element_type=F32
        )
        cp = pltpu.make_async_copy(stage.at[rows, :], demb_ref.at[rows, :], out_sem.at[k])
        cp.start()
        copies.append(cp)
        start += n
    tok_ref[...] = small_ref[0:1, 0:LOC]
    mean_ref[...] = small_ref[1:2, 0:1]
    for cp in copies:
        cp.wait()


def norm_kernel(p0, p1, p2, p3, norm_ref, rstd_ref, dhid_ref, gain_ref, bias_ref, gb_v):
    me = lax.axis_index("tp")
    for k, pay in enumerate((p0, p1, p2, p3)):
        gb_v[lax.rem(me + TP - k, TP)] = pay[LOC:, :]
    gb = gb_v[0] + gb_v[1] + gb_v[2] + gb_v[3]
    gain_ref[...] = gb[0:1, :]
    bias_ref[...] = gb[1:2, :]
    xh = norm_ref[0:LOC, :]
    dxh = (p0[0:LOC, :] + p1[0:LOC, :] + p2[0:LOC, :] + p3[0:LOC, :]) * norm_ref[LOC:LOC + 1, :]
    m1 = row_sum(dxh) * (1.0 / DIM)
    m2 = row_sum(dxh * xh) * (1.0 / DIM)
    dhid_ref[...] = (rstd_ref[:, 0:1] * (dxh - m1 - xh * m2)).astype(BF16)


def solution(mesh):
    vmem = pl.BlockSpec(memory_space=pltpu.VMEM)
    hbm = pl.BlockSpec(memory_space=pltpu.HBM)

    def group_step(hidden, ln_gain, ln_bias, out_embed, vocab_valid, targets, loss_mask):
        small, norm, rstd, dz, x_all, *pays = pl.pallas_call(
            main_kernel,
            out_shape=(
                jax.ShapeDtypeStruct((8, DIM), F32),
                jax.ShapeDtypeStruct((LOC + 8, DIM), F32),
                jax.ShapeDtypeStruct((LOC, TOK), F32),
                jax.ShapeDtypeStruct((TOK, VOCAB), BF16),
                jax.ShapeDtypeStruct((TOK, DIM), BF16),
                *[jax.ShapeDtypeStruct((LOC + 8, DIM), F32)] * TP,
            ),
            in_specs=[hbm] * 7,
            out_specs=(vmem,) * 9,
            scratch_shapes=[
                pltpu.VMEM((LOC, DIM), BF16),
                pltpu.VMEM((1, DIM), F32),
                pltpu.VMEM((1, DIM), F32),
                pltpu.VMEM((VOCAB // TOK, TOK), jnp.int32),
                pltpu.VMEM((1, LOC), jnp.int32),
                pltpu.VMEM((1, LOC), jnp.int32),
                pltpu.VMEM((VOCAB, DIM), BF16),
                pltpu.VMEM((TOK, VOCAB), F32),
                pltpu.VMEM((TOK, DIM), BF16),
                pltpu.VMEM((TOK, DIM), F32),
                pltpu.VMEM((TOK, TOK), F32),
                pltpu.VMEM((8 * TP, TOK), jnp.int32),
                pltpu.VMEM((8 * TP, TOK), F32),
                pltpu.VMEM((TOK, DIM), F32),
                pltpu.VMEM((2, TOK, TOK), F32),
                pltpu.SemaphoreType.DMA((GROUPS,)),
                pltpu.SemaphoreType.DMA((9,)),
                pltpu.SemaphoreType.DMA((9,)),
                pltpu.SemaphoreType.DMA((6,)),
            ],
            compiler_params=pltpu.CompilerParams(collective_id=0, has_side_effects=True, vmem_limit_bytes=40 * 1024 * 1024),
            name="main",
        )(
            *(
                pltpu.with_memory_space_constraint(val, pltpu.HBM)
                for val in (
                    hidden, ln_gain.reshape(1, DIM), ln_bias.reshape(1, DIM), out_embed,
                    vocab_valid.reshape(VOCAB // TOK, TOK), targets.reshape(1, LOC), loss_mask.reshape(1, LOC),
                )
            )
        )
        moved = [lax.ppermute(pays[k], "tp", [(i, (i + k) % TP) for i in range(TP)]) for k in range(1, TP)]
        d_embed, tok, mean = pl.pallas_call(
            embed_kernel,
            out_shape=(
                jax.ShapeDtypeStruct((VOCAB, DIM), F32),
                jax.ShapeDtypeStruct((1, LOC), F32),
                jax.ShapeDtypeStruct((1, 1), F32),
            ),
            in_specs=[vmem] * 3,
            out_specs=(hbm, vmem, vmem),
            scratch_shapes=[pltpu.VMEM((VOCAB, DIM), F32), pltpu.SemaphoreType.DMA((len(OUT_TILES),))],
            compiler_params=pltpu.CompilerParams(vmem_limit_bytes=36 * 1024 * 1024),
            cost_estimate=pl.CostEstimate(flops=2 * TOK * VOCAB * DIM, bytes_accessed=4 * VOCAB * DIM, transcendentals=0),
            name="embed",
        )(dz, x_all, small)
        d_hidden, d_gain, d_bias = pl.pallas_call(
            norm_kernel,
            out_shape=(
                jax.ShapeDtypeStruct((LOC, DIM), BF16),
                jax.ShapeDtypeStruct((1, DIM), F32),
                jax.ShapeDtypeStruct((1, DIM), F32),
            ),
            in_specs=[vmem] * 6,
            out_specs=(vmem,) * 3,
            scratch_shapes=[pltpu.VMEM((TP, 8, DIM), F32)],
            compiler_params=pltpu.CompilerParams(vmem_limit_bytes=8 * 1024 * 1024),
            name="norm",
        )(pays[0], *moved, norm, rstd)
        return tok.reshape(LOC), mean.reshape(1), d_hidden, d_embed, d_gain.reshape(DIM), d_bias.reshape(DIM)

    row_spec = P(("dp", "tp"))
    mat_spec = P(("dp", "tp"), None)
    return jax.shard_map(
        group_step, mesh=mesh,
        in_specs=(mat_spec, P(None), P(None), P("tp", None), P("tp"), row_spec, row_spec),
        out_specs=(row_spec, P("dp"), mat_spec, mat_spec, P("dp"), P("dp")), check_vma=False,
    )
```

```python
import functools

import jax
import jax.numpy as jnp
from jax import lax
from jax.experimental import pallas as pl
from jax.experimental.pallas import tpu as pltpu
from jax.sharding import PartitionSpec as P

SOFT_CAP = 30.0
Z_COEF = 1e-4
LN_EPS = 1e-5
LOG2E = 1.4426950408889634
MESH = pl.DeviceIdType.MESH
F32 = jnp.float32
BF16 = jnp.bfloat16

TP = 4
TOK = 128
LOC = TOK // TP
DIM = 512
VOCAB = 12672
TILE = 256
GROUP = 7 * TILE
GROUPS = VOCAB // GROUP
TAIL = VOCAB - GROUP * GROUPS


def row_sum(val):
    return jnp.sum(val, axis=-1, keepdims=True)


def main_kernel(
    hid_hbm, gain_hbm, bias_hbm, emb_ref, valid_hbm, tgt_hbm, mask_hbm,
    small_ref, norm_ref, rstd_ref, dz_ref, x_ref, pay_ref,
    hid_ref, gain_ref, bias_ref, valid_ref, tgt_ref, mask_ref,
    emb_v, g_v, hid_all, xh_v, rstd_v, meta_v, stat_v, dx_v, acc_v,
    emb_sem, send_sem, recv_sem, in_sem,
):
    me = lax.axis_index("tp")
    dp = lax.axis_index("dp")
    ins = [
        pltpu.make_async_copy(src, dst, in_sem.at[k])
        for k, (src, dst) in enumerate([
            (hid_hbm, hid_ref), (tgt_hbm, tgt_ref), (mask_hbm, mask_ref),
            (gain_hbm, gain_ref), (bias_hbm, bias_ref), (valid_hbm, valid_ref),
        ])
    ]
    for cp in ins:
        cp.start()
    chunks = [(j * GROUP, GROUP) for j in range(GROUPS - 1)]
    chunks.append(((GROUPS - 1) * GROUP, GROUP + TAIL))
    emb_copies = [
        pltpu.make_async_copy(emb_ref.at[pl.ds(s, n), :], emb_v.at[pl.ds(s, n), :], emb_sem.at[k])
        for k, (s, n) in enumerate(chunks)
    ]
    for cp in emb_copies:
        cp.start()

    barrier = pltpu.get_barrier_semaphore()
    for k in range(1, TP):
        pl.semaphore_signal(barrier, inc=1, device_id=(dp, lax.rem(me + k, TP)), device_id_type=MESH)

    for cp in ins[:3]:
        cp.wait()
    lane = lax.broadcasted_iota(jnp.int32, (1, TOK), 1)
    mine = (lane // LOC) == me
    tgt4 = jnp.concatenate([tgt_ref[...]] * TP, axis=1)
    mask4 = jnp.concatenate([mask_ref[...]] * TP, axis=1)
    my_rows = pl.ds(pl.multiple_of(me * LOC, LOC), LOC)
    my_meta = pl.ds(pl.multiple_of(me * 8, 8), 8)
    meta_v[my_meta, :] = jnp.concatenate(
        [jnp.where(mine, tgt4, 0), jnp.where(mine, mask4, 0), jnp.zeros((6, TOK), jnp.int32)], axis=0
    )
    hid_all[my_rows, :] = hid_ref[...]
    pl.semaphore_wait(barrier, TP - 1)

    def push(src, dst, idx):
        copies = []
        for k in range(1, TP):
            cp = pltpu.make_async_remote_copy(
                src_ref=src(k), dst_ref=dst, send_sem=send_sem.at[3 * idx + k - 1], recv_sem=recv_sem.at[3 * idx + k - 1],
                device_id=(dp, lax.rem(me + k, TP)), device_id_type=MESH,
            )
            cp.start()
            copies.append(cp)
        return copies

    first = push(lambda k: hid_ref, hid_all.at[my_rows, :], 0)
    first += push(lambda k: meta_v.at[my_meta, :], meta_v.at[my_meta, :], 1)
    for cp in ins[3:]:
        cp.wait()
    for cp in first:
        cp.wait_recv()

    meta = meta_v[0:8, :] + meta_v[8:16, :] + meta_v[16:24, :] + meta_v[24:32, :]
    tgt_row = meta[0:1, :]
    mask_row = meta[1:2, :].astype(F32)
    tok_count = row_sum(mask_row)
    tgt_col = jnp.transpose(jnp.broadcast_to(tgt_row, (TOK, TOK)))

    h = hid_all[...].astype(F32)
    mean_val = row_sum(h) * (1.0 / DIM)
    cent = h - mean_val
    var_val = row_sum(cent * cent) * (1.0 / DIM)
    rstd = lax.rsqrt(var_val + LN_EPS)
    xh = cent * rstd
    xh_v[...] = xh
    rstd_v[...] = jnp.broadcast_to(rstd, (TOK, TOK))
    x_ref[...] = (xh * gain_ref[...] + bias_ref[...]).astype(BF16)

    col0 = lax.broadcasted_iota(jnp.int32, (TOK, TOK), 1)
    base = me * VOCAB
    tgt_loc = tgt_col - base

    def fwd(start, size):
        z = lax.dot_general(
            x_ref[...], emb_v[pl.ds(start, size), :], (((1,), (1,)), ((), ())), preferred_element_type=F32
        )
        t = jnp.tanh(z * (1.0 / SOFT_CAP))
        ok = jnp.concatenate([valid_ref[c:c + 1, :] for c in range(start // TOK, (start + size) // TOK)], axis=1)
        e = jnp.exp2(t * (SOFT_CAP * LOG2E)) * ok.astype(F32)
        g_v[:, pl.ds(start, size)] = e * (1.0 - t * t)
        s_sum = 0.0
        t_sum = 0.0
        for c in range(size // TOK):
            cols = slice(c * TOK, (c + 1) * TOK)
            s_sum += e[:, cols]
            t_sum += jnp.where(tgt_loc - (start + c * TOK) == col0, t[:, cols], 0.0)
        return s_sum, t_sum

    acc_v[...] = jnp.zeros_like(acc_v)
    for j, (g0, n) in enumerate(chunks):
        emb_copies[j].wait()
        s_acc = 0.0
        t_acc = 0.0
        for s in range(0, n, TILE):
            ds, dt = fwd(g0 + s, min(TILE, n - s))
            s_acc += ds
            t_acc += dt
        acc_v[0] += s_acc
        acc_v[1] += t_acc

    s_loc = jnp.sum(jnp.transpose(acc_v[0]), axis=0, keepdims=True)
    t_loc = jnp.sum(jnp.transpose(acc_v[1]), axis=0, keepdims=True)
    stat_v[my_meta, :] = jnp.concatenate([s_loc, t_loc, jnp.zeros((6, TOK), F32)], axis=0)
    second = push(lambda k: stat_v.at[my_meta, :], stat_v.at[my_meta, :], 2)
    for cp in second:
        cp.wait_recv()
    stats = stat_v[0:8, :] + stat_v[8:16, :] + stat_v[16:24, :] + stat_v[24:32, :]
    sum_exp = stats[0:1, :]
    t_tgt = stats[1:2, :]
    lse = jnp.log(sum_exp)
    loss = (lse - SOFT_CAP * t_tgt + Z_COEF * lse * lse) * mask_row
    mean_loss = row_sum(loss) / tok_count
    coef = mask_row / tok_count
    a_row = (1.0 + 2.0 * Z_COEF * lse) * coef / sum_exp
    c_row = coef * (1.0 - t_tgt * t_tgt)
    a_col = jnp.transpose(jnp.broadcast_to(a_row, (TOK, TOK)))
    c_col = jnp.transpose(jnp.broadcast_to(c_row, (TOK, TOK)))

    def grad(start, size):
        parts = []
        for c in range(size // TOK):
            hit = tgt_loc - (start + c * TOK) == col0
            parts.append(a_col * g_v[:, pl.ds(start + c * TOK, TOK)] - jnp.where(hit, c_col, 0.0))
        return jnp.concatenate(parts, axis=1).astype(BF16)

    dz_copies = []
    for j, (g0, n) in enumerate(chunks):
        dz = grad(g0, n)
        dz_ref[:, pl.ds(g0, n)] = dz
        part = jnp.dot(dz, emb_v[pl.ds(g0, n), :], preferred_element_type=F32)
        dx_v[...] = part if j == 0 else dx_v[...] + part

    dx = dx_v[...]
    gb = jnp.concatenate(
        [jnp.sum(dx * xh_v[...], axis=0, keepdims=True), jnp.sum(dx, axis=0, keepdims=True), jnp.zeros((6, DIM), F32)], axis=0
    )
    for k in range(TP):
        pay_ref[k, 0:LOC, :] = dx[k * LOC:(k + 1) * LOC, :]
        pay_ref[k, LOC:, :] = gb
    norm_ref[0:LOC, :] = xh_v[my_rows, :]
    norm_ref[LOC:, :] = jnp.broadcast_to(gain_ref[...], (8, DIM))
    rstd_ref[...] = rstd_v[my_rows, :]
    loss_me = pltpu.roll(loss, lax.rem(TOK - me * LOC, TOK), 1)
    pad = jnp.zeros((1, DIM - TOK), F32)
    small_ref[...] = jnp.concatenate(
        [
            jnp.concatenate([loss_me, pad], axis=1),
            jnp.broadcast_to(mean_loss, (1, DIM)),
            jnp.zeros((6, DIM), F32),
        ],
        axis=0,
    )
    for cp in first + second:
        cp.wait_send()


OUT_TILES = [384] + [768] * 16


def embed_kernel(dz_ref, x_ref, small_ref, demb_ref, tok_ref, mean_ref, stage, out_sem):
    copies = []
    start = 0
    for k, n in enumerate(OUT_TILES):
        rows = pl.ds(start, n)
        stage[rows, :] = lax.dot_general(
            dz_ref[:, rows], x_ref[...], (((0,), (0,)), ((), ())), preferred_element_type=F32
        )
        cp = pltpu.make_async_copy(stage.at[rows, :], demb_ref.at[rows, :], out_sem.at[k])
        cp.start()
        copies.append(cp)
        start += n
    tok_ref[...] = small_ref[0:1, 0:LOC]
    mean_ref[...] = small_ref[1:2, 0:1]
    for cp in copies:
        cp.wait()


def norm_kernel(pay_ref, norm_ref, rstd_ref, dhid_ref, gain_ref, bias_ref):
    total = pay_ref[0] + pay_ref[1] + pay_ref[2] + pay_ref[3]
    gb = total[LOC:, :]
    gain_ref[...] = gb[0:1, :]
    bias_ref[...] = gb[1:2, :]
    xh = norm_ref[0:LOC, :]
    dxh = total[0:LOC, :] * norm_ref[LOC:LOC + 1, :]
    m1 = row_sum(dxh) * (1.0 / DIM)
    m2 = row_sum(dxh * xh) * (1.0 / DIM)
    dhid_ref[...] = (rstd_ref[:, 0:1] * (dxh - m1 - xh * m2)).astype(BF16)


def solution(mesh):
    vmem = pl.BlockSpec(memory_space=pltpu.VMEM)
    hbm = pl.BlockSpec(memory_space=pltpu.HBM)

    def group_step(hidden, ln_gain, ln_bias, out_embed, vocab_valid, targets, loss_mask):
        small, norm, rstd, dz, x_all, pay = pl.pallas_call(
            main_kernel,
            out_shape=(
                jax.ShapeDtypeStruct((8, DIM), F32),
                jax.ShapeDtypeStruct((LOC + 8, DIM), F32),
                jax.ShapeDtypeStruct((LOC, TOK), F32),
                jax.ShapeDtypeStruct((TOK, VOCAB), BF16),
                jax.ShapeDtypeStruct((TOK, DIM), BF16),
                jax.ShapeDtypeStruct((TP, LOC + 8, DIM), F32),
            ),
            in_specs=[hbm] * 7,
            out_specs=(vmem,) * 6,
            scratch_shapes=[
                pltpu.VMEM((LOC, DIM), BF16),
                pltpu.VMEM((1, DIM), F32),
                pltpu.VMEM((1, DIM), F32),
                pltpu.VMEM((VOCAB // TOK, TOK), jnp.int32),
                pltpu.VMEM((1, LOC), jnp.int32),
                pltpu.VMEM((1, LOC), jnp.int32),
                pltpu.VMEM((VOCAB, DIM), BF16),
                pltpu.VMEM((TOK, VOCAB), F32),
                pltpu.VMEM((TOK, DIM), BF16),
                pltpu.VMEM((TOK, DIM), F32),
                pltpu.VMEM((TOK, TOK), F32),
                pltpu.VMEM((8 * TP, TOK), jnp.int32),
                pltpu.VMEM((8 * TP, TOK), F32),
                pltpu.VMEM((TOK, DIM), F32),
                pltpu.VMEM((2, TOK, TOK), F32),
                pltpu.SemaphoreType.DMA((GROUPS,)),
                pltpu.SemaphoreType.DMA((9,)),
                pltpu.SemaphoreType.DMA((9,)),
                pltpu.SemaphoreType.DMA((6,)),
            ],
            compiler_params=pltpu.CompilerParams(collective_id=0, has_side_effects=True, vmem_limit_bytes=40 * 1024 * 1024),
            name="main",
        )(
            *(
                pltpu.with_memory_space_constraint(val, pltpu.HBM)
                for val in (
                    hidden, ln_gain.reshape(1, DIM), ln_bias.reshape(1, DIM), out_embed,
                    vocab_valid.reshape(VOCAB // TOK, TOK), targets.reshape(1, LOC), loss_mask.reshape(1, LOC),
                )
            )
        )
        moved = lax.all_to_all(pay, "tp", 0, 0)
        d_embed, tok, mean = pl.pallas_call(
            embed_kernel,
            out_shape=(
                jax.ShapeDtypeStruct((VOCAB, DIM), F32),
                jax.ShapeDtypeStruct((1, LOC), F32),
                jax.ShapeDtypeStruct((1, 1), F32),
            ),
            in_specs=[vmem] * 3,
            out_specs=(hbm, vmem, vmem),
            scratch_shapes=[pltpu.VMEM((VOCAB, DIM), F32), pltpu.SemaphoreType.DMA((len(OUT_TILES),))],
            compiler_params=pltpu.CompilerParams(vmem_limit_bytes=36 * 1024 * 1024),
            cost_estimate=pl.CostEstimate(flops=2 * TOK * VOCAB * DIM, bytes_accessed=4 * VOCAB * DIM, transcendentals=0),
            name="embed",
        )(dz, x_all, small)
        d_hidden, d_gain, d_bias = pl.pallas_call(
            norm_kernel,
            out_shape=(
                jax.ShapeDtypeStruct((LOC, DIM), BF16),
                jax.ShapeDtypeStruct((1, DIM), F32),
                jax.ShapeDtypeStruct((1, DIM), F32),
            ),
            in_specs=[vmem] * 3,
            out_specs=(vmem,) * 3,
            compiler_params=pltpu.CompilerParams(vmem_limit_bytes=8 * 1024 * 1024),
            name="norm",
        )(moved, norm, rstd)
        return tok.reshape(LOC), mean.reshape(1), d_hidden, d_embed, d_gain.reshape(DIM), d_bias.reshape(DIM)

    row_spec = P(("dp", "tp"))
    mat_spec = P(("dp", "tp"), None)
    return jax.shard_map(
        group_step, mesh=mesh,
        in_specs=(mat_spec, P(None), P(None), P("tp", None), P("tp"), row_spec, row_spec),
        out_specs=(row_spec, P("dp"), mat_spec, mat_spec, P("dp"), P("dp")), check_vma=False,
    )
```

```python
import functools

import jax
import jax.numpy as jnp
from jax import lax
from jax.experimental import pallas as pl
from jax.experimental.pallas import tpu as pltpu
from jax.sharding import PartitionSpec as P

SOFT_CAP = 30.0
Z_COEF = 1e-4
LN_EPS = 1e-5
LOG2E = 1.4426950408889634
MESH = pl.DeviceIdType.MESH
F32 = jnp.float32
BF16 = jnp.bfloat16

TP = 4
TOK = 128
LOC = TOK // TP
DIM = 512
VOCAB = 12672
TILE = 256
GROUP = 7 * TILE
GROUPS = VOCAB // GROUP
TAIL = VOCAB - GROUP * GROUPS
BLK = 32


def row_sum(val):
    return jnp.sum(val, axis=-1, keepdims=True)


def main_kernel(
    hid_hbm, gain_hbm, bias_hbm, emb_ref, valid_hbm, tgt_hbm, mask_hbm,
    small_ref, norm_ref, rstd_ref, dz_ref, x_ref, pay0, pay1, pay2, pay3,
    hid_ref, gain_ref, bias_ref, valid_ref, tgt_ref, mask_ref,
    emb_v, g_v, hid_all, xh_v, rstd_v, meta_v, stat_v, dx_v, acc_v, z_v, tgt_v,
    emb_sem, send_sem, recv_sem, in_sem,
):
    me = lax.axis_index("tp")
    dp = lax.axis_index("dp")
    pays = (pay0, pay1, pay2, pay3)
    ins = [
        pltpu.make_async_copy(src, dst, in_sem.at[k])
        for k, (src, dst) in enumerate([
            (hid_hbm, hid_ref), (tgt_hbm, tgt_ref), (mask_hbm, mask_ref),
            (gain_hbm, gain_ref), (bias_hbm, bias_ref), (valid_hbm, valid_ref),
        ])
    ]
    for cp in ins:
        cp.start()
    chunks = [(j * GROUP, GROUP) for j in range(GROUPS - 1)]
    chunks.append(((GROUPS - 1) * GROUP, GROUP + TAIL))
    emb_copies = [
        pltpu.make_async_copy(emb_ref.at[pl.ds(s, n), :], emb_v.at[pl.ds(s, n), :], emb_sem.at[k])
        for k, (s, n) in enumerate(chunks)
    ]
    for cp in emb_copies:
        cp.start()

    barrier = pltpu.get_barrier_semaphore()
    for k in range(1, TP):
        pl.semaphore_signal(barrier, inc=1, device_id=(dp, lax.rem(me + k, TP)), device_id_type=MESH)

    for cp in ins[:3]:
        cp.wait()
    lane = lax.broadcasted_iota(jnp.int32, (1, TOK), 1)
    mine = (lane // LOC) == me
    tgt4 = jnp.concatenate([tgt_ref[...]] * TP, axis=1)
    mask4 = jnp.concatenate([mask_ref[...]] * TP, axis=1)
    my_rows = pl.ds(pl.multiple_of(me * LOC, LOC), LOC)
    my_meta = pl.ds(pl.multiple_of(me * 8, 8), 8)
    meta_v[my_meta, :] = jnp.concatenate(
        [jnp.where(mine, tgt4, 0), jnp.where(mine, mask4, 0), jnp.zeros((6, TOK), jnp.int32)], axis=0
    )
    hid_all[my_rows, :] = hid_ref[...]
    pl.semaphore_wait(barrier, TP - 1)

    def push(src, dst, idx):
        copies = []
        for k in range(1, TP):
            cp = pltpu.make_async_remote_copy(
                src_ref=src(k), dst_ref=dst, send_sem=send_sem.at[3 * idx + k - 1], recv_sem=recv_sem.at[3 * idx + k - 1],
                device_id=(dp, lax.rem(me + k, TP)), device_id_type=MESH,
            )
            cp.start()
            copies.append(cp)
        return copies

    first = push(lambda k: hid_ref, hid_all.at[my_rows, :], 0)
    first += push(lambda k: meta_v.at[my_meta, :], meta_v.at[my_meta, :], 1)
    for cp in ins[3:]:
        cp.wait()
    for cp in first:
        cp.wait_recv()

    meta = meta_v[0:8, :] + meta_v[8:16, :] + meta_v[16:24, :] + meta_v[24:32, :]
    tgt_row = meta[0:1, :]
    mask_row = meta[1:2, :].astype(F32)
    tok_count = row_sum(mask_row)
    tgt_col = jnp.transpose(jnp.broadcast_to(tgt_row, (TOK, TOK)))

    h = hid_all[...].astype(F32)
    mean_val = row_sum(h) * (1.0 / DIM)
    cent = h - mean_val
    var_val = row_sum(cent * cent) * (1.0 / DIM)
    rstd = lax.rsqrt(var_val + LN_EPS)
    xh = cent * rstd
    xh_v[...] = xh
    rstd_v[...] = jnp.broadcast_to(rstd, (TOK, TOK))
    x_ref[...] = (xh * gain_ref[...] + bias_ref[...]).astype(BF16)

    tgt_v[...] = tgt_col - me * VOCAB
    lane_blk = lax.broadcasted_iota(jnp.int32, (BLK, TOK), 1)
    groups = [(j * GROUP, GROUP) for j in range(GROUPS - 1)]
    groups.append(((GROUPS - 1) * GROUP, GROUP + TAIL))

    def softmax_pass(buf, g0, n):
        for tb in range(TOK // BLK):
            rows = pl.ds(tb * BLK, BLK)
            tgt = tgt_v[rows, :]
            s_acc = acc_v[0, rows, :]
            t_acc = acc_v[1, rows, :]
            for c in range(n // TOK):
                col = g0 + c * TOK
                t = jnp.tanh(z_v[buf, rows, pl.ds(c * TOK, TOK)] * (1.0 / SOFT_CAP))
                ok = valid_ref[col // TOK:col // TOK + 1, :].astype(F32)
                e = jnp.exp2(t * (SOFT_CAP * LOG2E)) * ok
                s_acc += e
                t_acc += jnp.where(tgt == lane_blk + col, t, 0.0)
                g_v[rows, pl.ds(col, TOK)] = e * (1.0 - t * t)
            acc_v[0, rows, :] = s_acc
            acc_v[1, rows, :] = t_acc

    for cp in emb_copies:
        cp.wait()
    acc_v[...] = jnp.zeros_like(acc_v)
    for j, (g0, n) in enumerate(groups):
        for s in range(0, n, TILE):
            w = min(TILE, n - s)
            z_v[j % 2, :, pl.ds(s, w)] = lax.dot_general(
                x_ref[...], emb_v[pl.ds(g0 + s, w), :], (((1,), (1,)), ((), ())), preferred_element_type=F32
            )
        if j > 0:
            softmax_pass((j - 1) % 2, *groups[j - 1])
    softmax_pass((GROUPS - 1) % 2, *groups[-1])

    s_loc = jnp.sum(jnp.transpose(acc_v[0]), axis=0, keepdims=True)
    t_loc = jnp.sum(jnp.transpose(acc_v[1]), axis=0, keepdims=True)
    stat_v[my_meta, :] = jnp.concatenate([s_loc, t_loc, jnp.zeros((6, TOK), F32)], axis=0)
    second = push(lambda k: stat_v.at[my_meta, :], stat_v.at[my_meta, :], 2)
    for cp in second:
        cp.wait_recv()
    stats = stat_v[0:8, :] + stat_v[8:16, :] + stat_v[16:24, :] + stat_v[24:32, :]
    sum_exp = stats[0:1, :]
    t_tgt = stats[1:2, :]
    lse = jnp.log(sum_exp)
    loss = (lse - SOFT_CAP * t_tgt + Z_COEF * lse * lse) * mask_row
    mean_loss = row_sum(loss) / tok_count
    coef = mask_row / tok_count
    a_row = (1.0 + 2.0 * Z_COEF * lse) * coef / sum_exp
    c_row = coef * (1.0 - t_tgt * t_tgt)
    acc_v[0] = jnp.transpose(jnp.broadcast_to(a_row, (TOK, TOK)))
    acc_v[1] = jnp.transpose(jnp.broadcast_to(c_row, (TOK, TOK)))

    dx = 0.0
    for g0, n in groups:
        for tb in range(TOK // BLK):
            rows = pl.ds(tb * BLK, BLK)
            tgt = tgt_v[rows, :]
            a_blk = acc_v[0, rows, :]
            c_blk = acc_v[1, rows, :]
            for c in range(n // TOK):
                cols = pl.ds(g0 + c * TOK, TOK)
                hit = tgt == lane_blk + (g0 + c * TOK)
                dz_ref[rows, cols] = (a_blk * g_v[rows, cols] - jnp.where(hit, c_blk, 0.0)).astype(BF16)
        dx += jnp.dot(dz_ref[:, pl.ds(g0, n)], emb_v[pl.ds(g0, n), :], preferred_element_type=F32)
    dx_v[...] = dx

    gb = jnp.concatenate(
        [jnp.sum(dx * xh_v[...], axis=0, keepdims=True), jnp.sum(dx, axis=0, keepdims=True), jnp.zeros((6, DIM), F32)], axis=0
    )
    for k, pay in enumerate(pays):
        rows = pl.ds(pl.multiple_of((me ^ k) * LOC, LOC), LOC)
        pay[0:LOC, :] = dx_v[rows, :]
        pay[LOC:, :] = gb
    norm_ref[0:LOC, :] = xh_v[my_rows, :]
    norm_ref[LOC:, :] = jnp.broadcast_to(gain_ref[...], (8, DIM))
    rstd_ref[...] = rstd_v[my_rows, :]
    loss_me = pltpu.roll(loss, lax.rem(TOK - me * LOC, TOK), 1)
    pad = jnp.zeros((1, DIM - TOK), F32)
    small_ref[...] = jnp.concatenate(
        [
            jnp.concatenate([loss_me, pad], axis=1),
            jnp.broadcast_to(mean_loss, (1, DIM)),
            jnp.zeros((6, DIM), F32),
        ],
        axis=0,
    )
    for cp in first + second:
        cp.wait_send()


OUT_TILES = [384] + [768] * 16


def embed_kernel(dz_ref, x_ref, small_ref, demb_ref, tok_ref, mean_ref, stage, out_sem):
    copies = []
    start = 0
    for k, n in enumerate(OUT_TILES):
        rows = pl.ds(start, n)
        stage[rows, :] = lax.dot_general(
            dz_ref[:, rows], x_ref[...], (((0,), (0,)), ((), ())), preferred_element_type=F32
        )
        cp = pltpu.make_async_copy(stage.at[rows, :], demb_ref.at[rows, :], out_sem.at[k])
        cp.start()
        copies.append(cp)
        start += n
    tok_ref[...] = small_ref[0:1, 0:LOC]
    mean_ref[...] = small_ref[1:2, 0:1]
    for cp in copies:
        cp.wait()


def norm_kernel(p0, p1, p2, p3, norm_ref, rstd_ref, dhid_ref, gain_ref, bias_ref, gb_v):
    me = lax.axis_index("tp")
    for k, pay in enumerate((p0, p1, p2, p3)):
        gb_v[me ^ k] = pay[LOC:, :]
    gb = gb_v[0] + gb_v[1] + gb_v[2] + gb_v[3]
    gain_ref[...] = gb[0:1, :]
    bias_ref[...] = gb[1:2, :]
    xh = norm_ref[0:LOC, :]
    dxh = (p0[0:LOC, :] + p1[0:LOC, :] + p2[0:LOC, :] + p3[0:LOC, :]) * norm_ref[LOC:LOC + 1, :]
    m1 = row_sum(dxh) * (1.0 / DIM)
    m2 = row_sum(dxh * xh) * (1.0 / DIM)
    dhid_ref[...] = (rstd_ref[:, 0:1] * (dxh - m1 - xh * m2)).astype(BF16)


def solution(mesh):
    vmem = pl.BlockSpec(memory_space=pltpu.VMEM)
    hbm = pl.BlockSpec(memory_space=pltpu.HBM)

    def group_step(hidden, ln_gain, ln_bias, out_embed, vocab_valid, targets, loss_mask):
        small, norm, rstd, dz, x_all, *pays = pl.pallas_call(
            main_kernel,
            out_shape=(
                jax.ShapeDtypeStruct((8, DIM), F32),
                jax.ShapeDtypeStruct((LOC + 8, DIM), F32),
                jax.ShapeDtypeStruct((LOC, TOK), F32),
                jax.ShapeDtypeStruct((TOK, VOCAB), BF16),
                jax.ShapeDtypeStruct((TOK, DIM), BF16),
                *[jax.ShapeDtypeStruct((LOC + 8, DIM), F32)] * TP,
            ),
            in_specs=[hbm] * 7,
            out_specs=(vmem,) * 9,
            scratch_shapes=[
                pltpu.VMEM((LOC, DIM), BF16),
                pltpu.VMEM((1, DIM), F32),
                pltpu.VMEM((1, DIM), F32),
                pltpu.VMEM((VOCAB // TOK, TOK), jnp.int32),
                pltpu.VMEM((1, LOC), jnp.int32),
                pltpu.VMEM((1, LOC), jnp.int32),
                pltpu.VMEM((VOCAB, DIM), BF16),
                pltpu.VMEM((TOK, VOCAB), F32),
                pltpu.VMEM((TOK, DIM), BF16),
                pltpu.VMEM((TOK, DIM), F32),
                pltpu.VMEM((TOK, TOK), F32),
                pltpu.VMEM((8 * TP, TOK), jnp.int32),
                pltpu.VMEM((8 * TP, TOK), F32),
                pltpu.VMEM((TOK, DIM), F32),
                pltpu.VMEM((2, TOK, TOK), F32),
                pltpu.VMEM((2, TOK, GROUP + TAIL), F32),
                pltpu.VMEM((TOK, TOK), jnp.int32),
                pltpu.SemaphoreType.DMA((GROUPS,)),
                pltpu.SemaphoreType.DMA((9,)),
                pltpu.SemaphoreType.DMA((9,)),
                pltpu.SemaphoreType.DMA((6,)),
            ],
            compiler_params=pltpu.CompilerParams(collective_id=0, has_side_effects=True, vmem_limit_bytes=40 * 1024 * 1024),
            name="main",
        )(
            *(
                pltpu.with_memory_space_constraint(val, pltpu.HBM)
                for val in (
                    hidden, ln_gain.reshape(1, DIM), ln_bias.reshape(1, DIM), out_embed,
                    vocab_valid.reshape(VOCAB // TOK, TOK), targets.reshape(1, LOC), loss_mask.reshape(1, LOC),
                )
            )
        )
        moved = [lax.ppermute(pays[k], "tp", [(i, i ^ k) for i in range(TP)]) for k in range(1, TP)]
        d_embed, tok, mean = pl.pallas_call(
            embed_kernel,
            out_shape=(
                jax.ShapeDtypeStruct((VOCAB, DIM), F32),
                jax.ShapeDtypeStruct((1, LOC), F32),
                jax.ShapeDtypeStruct((1, 1), F32),
            ),
            in_specs=[vmem] * 3,
            out_specs=(hbm, vmem, vmem),
            scratch_shapes=[pltpu.VMEM((VOCAB, DIM), F32), pltpu.SemaphoreType.DMA((len(OUT_TILES),))],
            compiler_params=pltpu.CompilerParams(vmem_limit_bytes=36 * 1024 * 1024),
            cost_estimate=pl.CostEstimate(flops=2 * TOK * VOCAB * DIM, bytes_accessed=4 * VOCAB * DIM, transcendentals=0),
            name="embed",
        )(dz, x_all, small)
        d_hidden, d_gain, d_bias = pl.pallas_call(
            norm_kernel,
            out_shape=(
                jax.ShapeDtypeStruct((LOC, DIM), BF16),
                jax.ShapeDtypeStruct((1, DIM), F32),
                jax.ShapeDtypeStruct((1, DIM), F32),
            ),
            in_specs=[vmem] * 6,
            out_specs=(vmem,) * 3,
            scratch_shapes=[pltpu.VMEM((TP, 8, DIM), F32)],
            compiler_params=pltpu.CompilerParams(vmem_limit_bytes=8 * 1024 * 1024),
            name="norm",
        )(pays[0], *moved, norm, rstd)
        return tok.reshape(LOC), mean.reshape(1), d_hidden, d_embed, d_gain.reshape(DIM), d_bias.reshape(DIM)

    row_spec = P(("dp", "tp"))
    mat_spec = P(("dp", "tp"), None)
    return jax.shard_map(
        group_step, mesh=mesh,
        in_specs=(mat_spec, P(None), P(None), P("tp", None), P("tp"), row_spec, row_spec),
        out_specs=(row_spec, P("dp"), mat_spec, mat_spec, P("dp"), P("dp")), check_vma=False,
    )
```

```python
import functools

import jax
import jax.numpy as jnp
from jax import lax
from jax.experimental import pallas as pl
from jax.experimental.pallas import tpu as pltpu
from jax.sharding import PartitionSpec as P

SOFT_CAP = 30.0
Z_COEF = 1e-4
LN_EPS = 1e-5
LOG2E = 1.4426950408889634
MESH = pl.DeviceIdType.MESH
F32 = jnp.float32
BF16 = jnp.bfloat16

TP = 4
TOK = 128
LOC = TOK // TP
DIM = 512
VOCAB = 12672
TILE = 256
GROUP = 7 * TILE
GROUPS = VOCAB // GROUP
TAIL = VOCAB - GROUP * GROUPS
BLK = 32


def row_sum(val):
    return jnp.sum(val, axis=-1, keepdims=True)


def main_kernel(
    hid_hbm, gain_hbm, bias_hbm, emb_ref, valid_hbm, tgt_hbm, mask_hbm,
    small_ref, xh_v, rstd_v, coef_ref, tgt_v, x_ref, g_v, emb_v,
    hid_ref, gain_ref, bias_ref, valid_ref, tgt_ref, mask_ref,
    hid_all, meta_v, stat_v, acc_v, z_v,
    emb_sem, send_sem, recv_sem, in_sem,
):
    me = lax.axis_index("tp")
    dp = lax.axis_index("dp")
    ins = [
        pltpu.make_async_copy(src, dst, in_sem.at[k])
        for k, (src, dst) in enumerate([
            (hid_hbm, hid_ref), (tgt_hbm, tgt_ref), (mask_hbm, mask_ref),
            (gain_hbm, gain_ref), (bias_hbm, bias_ref), (valid_hbm, valid_ref),
        ])
    ]
    for cp in ins:
        cp.start()
    chunks = [(j * GROUP, GROUP) for j in range(GROUPS - 1)]
    chunks.append(((GROUPS - 1) * GROUP, GROUP + TAIL))
    emb_copies = [
        pltpu.make_async_copy(emb_ref.at[pl.ds(s, n), :], emb_v.at[pl.ds(s, n), :], emb_sem.at[k])
        for k, (s, n) in enumerate(chunks)
    ]
    for cp in emb_copies:
        cp.start()

    barrier = pltpu.get_barrier_semaphore()
    for k in range(1, TP):
        pl.semaphore_signal(barrier, inc=1, device_id=(dp, lax.rem(me + k, TP)), device_id_type=MESH)

    for cp in ins[:3]:
        cp.wait()
    lane = lax.broadcasted_iota(jnp.int32, (1, TOK), 1)
    mine = (lane // LOC) == me
    tgt4 = jnp.concatenate([tgt_ref[...]] * TP, axis=1)
    mask4 = jnp.concatenate([mask_ref[...]] * TP, axis=1)
    my_rows = pl.ds(pl.multiple_of(me * LOC, LOC), LOC)
    my_meta = pl.ds(pl.multiple_of(me * 8, 8), 8)
    meta_v[my_meta, :] = jnp.concatenate(
        [jnp.where(mine, tgt4, 0), jnp.where(mine, mask4, 0), jnp.zeros((6, TOK), jnp.int32)], axis=0
    )
    hid_all[my_rows, :] = hid_ref[...]
    pl.semaphore_wait(barrier, TP - 1)

    def push(src, dst, idx):
        copies = []
        for k in range(1, TP):
            cp = pltpu.make_async_remote_copy(
                src_ref=src(k), dst_ref=dst, send_sem=send_sem.at[3 * idx + k - 1], recv_sem=recv_sem.at[3 * idx + k - 1],
                device_id=(dp, lax.rem(me + k, TP)), device_id_type=MESH,
            )
            cp.start()
            copies.append(cp)
        return copies

    first = push(lambda k: hid_ref, hid_all.at[my_rows, :], 0)
    first += push(lambda k: meta_v.at[my_meta, :], meta_v.at[my_meta, :], 1)
    for cp in ins[3:]:
        cp.wait()
    for cp in first:
        cp.wait_recv()

    meta = meta_v[0:8, :] + meta_v[8:16, :] + meta_v[16:24, :] + meta_v[24:32, :]
    tgt_row = meta[0:1, :]
    mask_row = meta[1:2, :].astype(F32)
    tok_count = row_sum(mask_row)
    tgt_col = jnp.transpose(jnp.broadcast_to(tgt_row, (TOK, TOK)))

    h = hid_all[...].astype(F32)
    mean_val = row_sum(h) * (1.0 / DIM)
    cent = h - mean_val
    var_val = row_sum(cent * cent) * (1.0 / DIM)
    rstd = lax.rsqrt(var_val + LN_EPS)
    xh = cent * rstd
    xh_v[...] = xh
    rstd_v[...] = jnp.broadcast_to(rstd, (TOK, TOK))
    x_ref[...] = (xh * gain_ref[...] + bias_ref[...]).astype(BF16)

    tgt_v[...] = tgt_col - me * VOCAB
    lane_blk = lax.broadcasted_iota(jnp.int32, (BLK, TOK), 1)
    groups = [(j * GROUP, GROUP) for j in range(GROUPS - 1)]
    groups.append(((GROUPS - 1) * GROUP, GROUP + TAIL))

    def softmax_pass(buf, g0, n):
        for tb in range(TOK // BLK):
            rows = pl.ds(tb * BLK, BLK)
            tgt = tgt_v[rows, :]
            s_acc = acc_v[0, rows, :]
            t_acc = acc_v[1, rows, :]
            for c in range(n // TOK):
                col = g0 + c * TOK
                t = jnp.tanh(z_v[buf, rows, pl.ds(c * TOK, TOK)] * (1.0 / SOFT_CAP))
                ok = valid_ref[col // TOK:col // TOK + 1, :].astype(F32)
                e = jnp.exp2(t * (SOFT_CAP * LOG2E)) * ok
                s_acc += e
                t_acc += jnp.where(tgt == lane_blk + col, t, 0.0)
                g_v[rows, pl.ds(col, TOK)] = e * (1.0 - t * t)
            acc_v[0, rows, :] = s_acc
            acc_v[1, rows, :] = t_acc

    for cp in emb_copies:
        cp.wait()
    acc_v[...] = jnp.zeros_like(acc_v)
    for j, (g0, n) in enumerate(groups):
        for s in range(0, n, TILE):
            w = min(TILE, n - s)
            z_v[j % 2, :, pl.ds(s, w)] = lax.dot_general(
                x_ref[...], emb_v[pl.ds(g0 + s, w), :], (((1,), (1,)), ((), ())), preferred_element_type=F32
            )
        if j > 0:
            softmax_pass((j - 1) % 2, *groups[j - 1])
    softmax_pass((GROUPS - 1) % 2, *groups[-1])

    s_loc = jnp.sum(jnp.transpose(acc_v[0]), axis=0, keepdims=True)
    t_loc = jnp.sum(jnp.transpose(acc_v[1]), axis=0, keepdims=True)
    stat_v[my_meta, :] = jnp.concatenate([s_loc, t_loc, jnp.zeros((6, TOK), F32)], axis=0)
    second = push(lambda k: stat_v.at[my_meta, :], stat_v.at[my_meta, :], 2)
    for cp in second:
        cp.wait_recv()
    stats = stat_v[0:8, :] + stat_v[8:16, :] + stat_v[16:24, :] + stat_v[24:32, :]
    sum_exp = stats[0:1, :]
    t_tgt = stats[1:2, :]
    lse = jnp.log(sum_exp)
    loss = (lse - SOFT_CAP * t_tgt + Z_COEF * lse * lse) * mask_row
    mean_loss = row_sum(loss) / tok_count
    coef = mask_row / tok_count
    a_row = (1.0 + 2.0 * Z_COEF * lse) * coef / sum_exp
    c_row = coef * (1.0 - t_tgt * t_tgt)
    coef_ref[0] = jnp.transpose(jnp.broadcast_to(a_row, (TOK, TOK)))
    coef_ref[1] = jnp.transpose(jnp.broadcast_to(c_row, (TOK, TOK)))
    loss_me = pltpu.roll(loss, lax.rem(TOK - me * LOC, TOK), 1)
    pad = jnp.zeros((1, DIM - TOK), F32)
    small_ref[...] = jnp.concatenate(
        [
            jnp.concatenate([loss_me, pad], axis=1),
            jnp.broadcast_to(mean_loss, (1, DIM)),
            gain_ref[...],
            jnp.zeros((5, DIM), F32),
        ],
        axis=0,
    )
    for cp in first + second:
        cp.wait_send()


EARLY = 2
EARLY_ROWS = EARLY * GROUP
EARLY_TILES = [256, 640, 896, 896, 896]
LATE_TILES = [256, 512] + [832] * 10


def write_rows(dz_ref, x_ref, out_ref, stage, sem, start, first, tiles):
    copies = []
    for k, n in enumerate(tiles):
        rows = pl.ds(start, n)
        local = pl.ds(start - first, n)
        stage[local, :] = lax.dot_general(
            dz_ref[:, rows], x_ref[...], (((0,), (0,)), ((), ())), preferred_element_type=F32
        )
        cp = pltpu.make_async_copy(stage.at[local, :], out_ref.at[rows, :], sem.at[k])
        cp.start()
        copies.append(cp)
        start += n
    return copies


def grad_kernel(
    g_ref, emb_ref, x_ref, xh_ref, coef_ref, tgt_ref, demb_ref, dz_ref, pay0, pay1, pay2, pay3, stage, dx_v, out_sem
):
    me = lax.axis_index("tp")
    lane_blk = lax.broadcasted_iota(jnp.int32, (BLK, TOK), 1)
    groups = [(j * GROUP, GROUP) for j in range(GROUPS - 1)]
    groups.append(((GROUPS - 1) * GROUP, GROUP + TAIL))

    def logit_grad(g0, n):
        for tb in range(TOK // BLK):
            rows = pl.ds(tb * BLK, BLK)
            tgt = tgt_ref[rows, :]
            a_blk = coef_ref[0, rows, :]
            c_blk = coef_ref[1, rows, :]
            for c in range(n // TOK):
                cols = pl.ds(g0 + c * TOK, TOK)
                hit = tgt == lane_blk + (g0 + c * TOK)
                dz_ref[rows, cols] = (a_blk * g_ref[rows, cols] - jnp.where(hit, c_blk, 0.0)).astype(BF16)

    for g0, n in groups[:EARLY]:
        logit_grad(g0, n)
    copies = write_rows(dz_ref, x_ref, demb_ref, stage, out_sem, 0, 0, EARLY_TILES)
    dx = 0.0
    for j, (g0, n) in enumerate(groups):
        if j >= EARLY:
            logit_grad(g0, n)
        dx += jnp.dot(dz_ref[:, pl.ds(g0, n)], emb_ref[pl.ds(g0, n), :], preferred_element_type=F32)
    dx_v[...] = dx
    gb = jnp.concatenate(
        [jnp.sum(dx * xh_ref[...], axis=0, keepdims=True), jnp.sum(dx, axis=0, keepdims=True), jnp.zeros((6, DIM), F32)], axis=0
    )
    for k, pay in enumerate((pay0, pay1, pay2, pay3)):
        pay[0:LOC, :] = dx_v[pl.ds(pl.multiple_of((me ^ k) * LOC, LOC), LOC), :]
        pay[LOC:, :] = gb
    for cp in copies:
        cp.wait()


def embed_kernel(demb_in, dz_ref, x_ref, small_ref, demb_ref, tok_ref, mean_ref, stage, out_sem):
    copies = write_rows(dz_ref, x_ref, demb_ref, stage, out_sem, EARLY_ROWS, EARLY_ROWS, LATE_TILES)
    tok_ref[...] = small_ref[0:1, 0:LOC]
    mean_ref[...] = small_ref[1:2, 0:1]
    for cp in copies:
        cp.wait()


def norm_kernel(p0, p1, p2, p3, xh_ref, rstd_ref, gain_in, dhid_ref, gain_ref, bias_ref, gb_v):
    me = lax.axis_index("tp")
    for k, pay in enumerate((p0, p1, p2, p3)):
        gb_v[me ^ k] = pay[LOC:, :]
    gb = gb_v[0] + gb_v[1] + gb_v[2] + gb_v[3]
    gain_ref[...] = gb[0:1, :]
    bias_ref[...] = gb[1:2, :]
    my_rows = pl.ds(pl.multiple_of(me * LOC, LOC), LOC)
    xh = xh_ref[my_rows, :]
    dxh = (p0[0:LOC, :] + p1[0:LOC, :] + p2[0:LOC, :] + p3[0:LOC, :]) * gain_in[2:3, :]
    m1 = row_sum(dxh) * (1.0 / DIM)
    m2 = row_sum(dxh * xh) * (1.0 / DIM)
    dhid_ref[...] = (rstd_ref[my_rows, 0:1] * (dxh - m1 - xh * m2)).astype(BF16)


def solution(mesh):
    vmem = pl.BlockSpec(memory_space=pltpu.VMEM)
    hbm = pl.BlockSpec(memory_space=pltpu.HBM)

    def group_step(hidden, ln_gain, ln_bias, out_embed, vocab_valid, targets, loss_mask):
        shape = jax.ShapeDtypeStruct
        small, xh, rstd, coef, tgt, x_all, g_all, emb = pl.pallas_call(
            main_kernel,
            out_shape=(
                shape((8, DIM), F32), shape((TOK, DIM), F32), shape((TOK, TOK), F32), shape((2, TOK, TOK), F32),
                shape((TOK, TOK), jnp.int32), shape((TOK, DIM), BF16), shape((TOK, VOCAB), F32), shape((VOCAB, DIM), BF16),
            ),
            in_specs=[hbm] * 7,
            out_specs=(vmem,) * 8,
            scratch_shapes=[
                pltpu.VMEM((LOC, DIM), BF16),
                pltpu.VMEM((1, DIM), F32),
                pltpu.VMEM((1, DIM), F32),
                pltpu.VMEM((VOCAB // TOK, TOK), jnp.int32),
                pltpu.VMEM((1, LOC), jnp.int32),
                pltpu.VMEM((1, LOC), jnp.int32),
                pltpu.VMEM((TOK, DIM), BF16),
                pltpu.VMEM((8 * TP, TOK), jnp.int32),
                pltpu.VMEM((8 * TP, TOK), F32),
                pltpu.VMEM((2, TOK, TOK), F32),
                pltpu.VMEM((2, TOK, GROUP + TAIL), F32),
                pltpu.SemaphoreType.DMA((GROUPS,)),
                pltpu.SemaphoreType.DMA((9,)),
                pltpu.SemaphoreType.DMA((9,)),
                pltpu.SemaphoreType.DMA((6,)),
            ],
            compiler_params=pltpu.CompilerParams(collective_id=0, has_side_effects=True, vmem_limit_bytes=30 * 1024 * 1024),
            name="main",
        )(
            *(
                pltpu.with_memory_space_constraint(val, pltpu.HBM)
                for val in (
                    hidden, ln_gain.reshape(1, DIM), ln_bias.reshape(1, DIM), out_embed,
                    vocab_valid.reshape(VOCAB // TOK, TOK), targets.reshape(1, LOC), loss_mask.reshape(1, LOC),
                )
            )
        )
        part = shape((LOC + 8, DIM), F32)
        early, dz, *pays = pl.pallas_call(
            grad_kernel,
            out_shape=(shape((VOCAB, DIM), F32), shape((TOK, VOCAB), BF16), part, part, part, part),
            in_specs=[vmem] * 6,
            out_specs=(hbm,) + (vmem,) * 5,
            scratch_shapes=[
                pltpu.VMEM((EARLY_ROWS, DIM), F32), pltpu.VMEM((TOK, DIM), F32), pltpu.SemaphoreType.DMA((len(EARLY_TILES),)),
            ],
            compiler_params=pltpu.CompilerParams(vmem_limit_bytes=16 * 1024 * 1024),
            name="grad",
        )(g_all, emb, x_all, xh, coef, tgt)
        moved = [lax.ppermute(pays[k], "tp", [(i, i ^ k) for i in range(TP)]) for k in range(1, TP)]
        d_embed, tok, mean = pl.pallas_call(
            embed_kernel,
            out_shape=(shape((VOCAB, DIM), F32), shape((1, LOC), F32), shape((1, 1), F32)),
            in_specs=[hbm] + [vmem] * 3,
            out_specs=(hbm, vmem, vmem),
            input_output_aliases={0: 0},
            scratch_shapes=[pltpu.VMEM((VOCAB - EARLY_ROWS, DIM), F32), pltpu.SemaphoreType.DMA((len(LATE_TILES),))],
            compiler_params=pltpu.CompilerParams(vmem_limit_bytes=30 * 1024 * 1024),
            cost_estimate=pl.CostEstimate(flops=2 * TOK * VOCAB * DIM, bytes_accessed=4 * VOCAB * DIM, transcendentals=0),
            name="embed",
        )(early, dz, x_all, small)
        d_hidden, d_gain, d_bias = pl.pallas_call(
            norm_kernel,
            out_shape=(shape((LOC, DIM), BF16), shape((1, DIM), F32), shape((1, DIM), F32)),
            in_specs=[vmem] * 7,
            out_specs=(vmem,) * 3,
            scratch_shapes=[pltpu.VMEM((TP, 8, DIM), F32)],
            compiler_params=pltpu.CompilerParams(vmem_limit_bytes=8 * 1024 * 1024),
            name="norm",
        )(pays[0], *moved, xh, rstd, small)
        return tok.reshape(LOC), mean.reshape(1), d_hidden, d_embed, d_gain.reshape(DIM), d_bias.reshape(DIM)

    row_spec = P(("dp", "tp"))
    mat_spec = P(("dp", "tp"), None)
    return jax.shard_map(
        group_step, mesh=mesh,
        in_specs=(mat_spec, P(None), P(None), P("tp", None), P("tp"), row_spec, row_spec),
        out_specs=(row_spec, P("dp"), mat_spec, mat_spec, P("dp"), P("dp")), check_vma=False,
    )
```

```python
import functools

import jax
import jax.numpy as jnp
from jax import lax
from jax.experimental import pallas as pl
from jax.experimental.pallas import tpu as pltpu
from jax.sharding import PartitionSpec as P

SOFT_CAP = 30.0
Z_COEF = 1e-4
LN_EPS = 1e-5
LOG2E = 1.4426950408889634
MESH = pl.DeviceIdType.MESH
F32 = jnp.float32
BF16 = jnp.bfloat16

TP = 4
TOK = 128
LOC = TOK // TP
DIM = 512
VOCAB = 12672
TILE = 256
GROUP = 7 * TILE
GROUPS = VOCAB // GROUP
TAIL = VOCAB - GROUP * GROUPS
BLK = 32
HALF = 64
AHEAD = 2
BUFS = 3


def row_sum(val):
    return jnp.sum(val, axis=-1, keepdims=True)


def main_kernel(
    hid_hbm, gain_hbm, bias_hbm, emb_ref, valid_hbm, tgt_hbm, mask_hbm,
    small_ref, xh_v, rstd_v, coef_ref, tgt_v, x_ref, g_v, emb_v,
    hid_ref, gain_ref, bias_ref, valid_ref, tgt_ref, mask_ref,
    hid_all, meta_v, stat_v, acc_v, z_v, embt_v, tmp_v,
    emb_sem, send_sem, recv_sem, in_sem,
):
    me = lax.axis_index("tp")
    dp = lax.axis_index("dp")
    ins = [
        pltpu.make_async_copy(src, dst, in_sem.at[k])
        for k, (src, dst) in enumerate([
            (hid_hbm, hid_ref), (tgt_hbm, tgt_ref), (mask_hbm, mask_ref),
            (gain_hbm, gain_ref), (bias_hbm, bias_ref), (valid_hbm, valid_ref),
        ])
    ]
    for cp in ins:
        cp.start()
    chunks = [(j * GROUP, GROUP) for j in range(GROUPS - 1)]
    chunks.append(((GROUPS - 1) * GROUP, GROUP + TAIL))
    emb_copies = [
        pltpu.make_async_copy(emb_ref.at[pl.ds(s, n), :], emb_v.at[pl.ds(s, n), :], emb_sem.at[k])
        for k, (s, n) in enumerate(chunks)
    ]
    for cp in emb_copies:
        cp.start()

    barrier = pltpu.get_barrier_semaphore()
    for k in (2, 3, 1):
        pl.semaphore_signal(barrier, inc=1, device_id=(dp, me ^ k), device_id_type=MESH)

    for cp in ins[:3]:
        cp.wait()
    lane = lax.broadcasted_iota(jnp.int32, (1, TOK), 1)
    mine = (lane // LOC) == me
    tgt4 = jnp.concatenate([tgt_ref[...]] * TP, axis=1)
    mask4 = jnp.concatenate([mask_ref[...]] * TP, axis=1)
    my_rows = pl.ds(pl.multiple_of(me * LOC, LOC), LOC)

    def slot(dev):
        return pl.ds(pl.multiple_of(dev * 8, 8), 8)

    meta_v[slot(me), :] = jnp.concatenate(
        [jnp.where(mine, tgt4, 0), jnp.where(mine, mask4, 0), jnp.zeros((6, TOK), jnp.int32)], axis=0
    )
    hid_all[my_rows, :] = hid_ref[...]
    pl.semaphore_wait(barrier, TP - 1)

    def push(src, dst, idx, k):
        cp = pltpu.make_async_remote_copy(
            src_ref=src, dst_ref=dst, send_sem=send_sem.at[3 * idx + k - 1], recv_sem=recv_sem.at[3 * idx + k - 1],
            device_id=(dp, me ^ k), device_id_type=MESH,
        )
        cp.start()
        return cp

    first = {}
    for k in (2, 3, 1):
        first[k] = [
            push(hid_ref, hid_all.at[my_rows, :], 0, k),
            push(meta_v.at[slot(me), :], meta_v.at[slot(me), :], 1, k),
        ]
    for cp in ins[3:]:
        cp.wait()

    here = me // 2
    lane_blk = lax.broadcasted_iota(jnp.int32, (BLK, TOK), 1)
    groups = [(j * GROUP, GROUP) for j in range(GROUPS - 1)]
    groups.append(((GROUPS - 1) * GROUP, GROUP + TAIL))

    def half_rows(half):
        return pl.ds(pl.multiple_of(half * HALF, HALF), HALF)

    def prepare(half):
        tgt = meta_v[slot(2 * half), :][0:1, :] + meta_v[slot(2 * half + 1), :][0:1, :]
        tmp_v[...] = jnp.transpose(jnp.broadcast_to(tgt, (TOK, TOK))) - me * VOCAB
        rows = half_rows(half)
        tgt_v[rows, :] = tmp_v[rows, :]
        h = hid_all[rows, :].astype(F32)
        cent = h - row_sum(h) * (1.0 / DIM)
        rstd = lax.rsqrt(row_sum(cent * cent) * (1.0 / DIM) + LN_EPS)
        xh = cent * rstd
        xh_v[rows, :] = xh
        rstd_v[rows, :] = jnp.broadcast_to(rstd, (HALF, TOK))
        x_ref[rows, :] = (xh * gain_ref[...] + bias_ref[...]).astype(BF16)

    def turn(j):
        g0, n = groups[j]
        for s in range(0, n, TILE):
            w = min(TILE, n - s)
            embt_v[:, pl.ds(g0 + s, w)] = jnp.transpose(emb_v[pl.ds(g0 + s, w), :])

    def logits(half, j, buf):
        g0, n = groups[j]
        z_v[buf, :, pl.ds(0, n)] = jnp.dot(x_ref[half_rows(half), :], embt_v[:, pl.ds(g0, n)], preferred_element_type=F32)

    def softmax_pass(half, j, buf):
        g0, n = groups[j]
        for tb in range(HALF // BLK):
            rows = pl.ds(pl.multiple_of(half * HALF + tb * BLK, BLK), BLK)
            tgt = tgt_v[rows, :]
            s_acc = 0.0
            t_acc = 0.0
            for c in range(n // TOK):
                col = g0 + c * TOK
                t = jnp.tanh(z_v[buf, pl.ds(tb * BLK, BLK), pl.ds(c * TOK, TOK)] * (1.0 / SOFT_CAP))
                ok = valid_ref[col // TOK:col // TOK + 1, :].astype(F32)
                e = jnp.exp2(t * (SOFT_CAP * LOG2E)) * ok
                s_acc += e
                t_acc += jnp.where(tgt == lane_blk + col, t, 0.0)
                g_v[rows, pl.ds(col, TOK)] = e * (1.0 - t * t)
            if j == 0:
                acc_v[0, rows, :] = s_acc
                acc_v[1, rows, :] = t_acc
            else:
                acc_v[0, rows, :] += s_acc
                acc_v[1, rows, :] += t_acc

    steps = [(here, j) for j in range(GROUPS)] + [(1 - here, j) for j in range(GROUPS)]

    def advance(i):
        if i < len(steps):
            logits(*steps[i], i % BUFS)
        if i > 0:
            softmax_pass(*steps[i - 1], (i - 1) % BUFS)

    for j in range(AHEAD):
        emb_copies[j].wait()
        turn(j)
    for cp in first[1]:
        cp.wait_recv()
    prepare(here)
    todo = 0
    for j in range(AHEAD, GROUPS):
        emb_copies[j].wait()
        turn(j)
        while todo < min(j, 2 * (j - AHEAD + 1)):
            advance(todo)
            todo += 1
    for cp in first[2] + first[3]:
        cp.wait_recv()
    prepare(1 - here)
    for i in range(todo, len(steps) + 1):
        advance(i)

    meta = meta_v[0:8, :] + meta_v[8:16, :] + meta_v[16:24, :] + meta_v[24:32, :]
    mask_row = meta[1:2, :].astype(F32)
    tok_count = row_sum(mask_row)
    s_loc = jnp.sum(jnp.transpose(acc_v[0]), axis=0, keepdims=True)
    t_loc = jnp.sum(jnp.transpose(acc_v[1]), axis=0, keepdims=True)
    stat_v[slot(me), :] = jnp.concatenate([s_loc, t_loc, jnp.zeros((6, TOK), F32)], axis=0)
    second = [push(stat_v.at[slot(me), :], stat_v.at[slot(me), :], 2, k) for k in (2, 3, 1)]
    for cp in second:
        cp.wait_recv()
    stats = stat_v[0:8, :] + stat_v[8:16, :] + stat_v[16:24, :] + stat_v[24:32, :]
    sum_exp = stats[0:1, :]
    t_tgt = stats[1:2, :]
    lse = jnp.log(sum_exp)
    loss = (lse - SOFT_CAP * t_tgt + Z_COEF * lse * lse) * mask_row
    mean_loss = row_sum(loss) / tok_count
    coef = mask_row / tok_count
    a_row = (1.0 + 2.0 * Z_COEF * lse) * coef / sum_exp
    c_row = coef * (1.0 - t_tgt * t_tgt)
    coef_ref[0] = jnp.transpose(jnp.broadcast_to(a_row, (TOK, TOK)))
    coef_ref[1] = jnp.transpose(jnp.broadcast_to(c_row, (TOK, TOK)))
    loss_me = pltpu.roll(loss, lax.rem(TOK - me * LOC, TOK), 1)
    pad = jnp.zeros((1, DIM - TOK), F32)
    small_ref[...] = jnp.concatenate(
        [
            jnp.concatenate([loss_me, pad], axis=1),
            jnp.broadcast_to(mean_loss, (1, DIM)),
            gain_ref[...],
            jnp.zeros((5, DIM), F32),
        ],
        axis=0,
    )
    for cp in first[1] + first[2] + first[3] + second:
        cp.wait_send()


EARLY = 2
EARLY_ROWS = EARLY * GROUP
EARLY_TILES = [256, 640, 896, 896, 896]
LATE_TILES = [256, 512] + [832] * 10


def write_rows(dz_ref, x_ref, out_ref, stage, sem, start, first, tiles):
    copies = []
    for k, n in enumerate(tiles):
        rows = pl.ds(start, n)
        local = pl.ds(start - first, n)
        stage[local, :] = lax.dot_general(
            dz_ref[:, rows], x_ref[...], (((0,), (0,)), ((), ())), preferred_element_type=F32
        )
        cp = pltpu.make_async_copy(stage.at[local, :], out_ref.at[rows, :], sem.at[k])
        cp.start()
        copies.append(cp)
        start += n
    return copies


def grad_kernel(
    g_ref, emb_ref, x_ref, xh_ref, coef_ref, tgt_ref, demb_ref, dz_ref, pay0, pay1, pay2, pay3, stage, dx_v, out_sem
):
    me = lax.axis_index("tp")
    lane_blk = lax.broadcasted_iota(jnp.int32, (BLK, TOK), 1)
    groups = [(j * GROUP, GROUP) for j in range(GROUPS - 1)]
    groups.append(((GROUPS - 1) * GROUP, GROUP + TAIL))

    def logit_grad(g0, n):
        for tb in range(TOK // BLK):
            rows = pl.ds(tb * BLK, BLK)
            tgt = tgt_ref[rows, :]
            a_blk = coef_ref[0, rows, :]
            c_blk = coef_ref[1, rows, :]
            for c in range(n // TOK):
                cols = pl.ds(g0 + c * TOK, TOK)
                hit = tgt == lane_blk + (g0 + c * TOK)
                dz_ref[rows, cols] = (a_blk * g_ref[rows, cols] - jnp.where(hit, c_blk, 0.0)).astype(BF16)

    for g0, n in groups[:EARLY]:
        logit_grad(g0, n)
    copies = write_rows(dz_ref, x_ref, demb_ref, stage, out_sem, 0, 0, EARLY_TILES)
    dx = 0.0
    for j, (g0, n) in enumerate(groups):
        if j >= EARLY:
            logit_grad(g0, n)
        dx += jnp.dot(dz_ref[:, pl.ds(g0, n)], emb_ref[pl.ds(g0, n), :], preferred_element_type=F32)
    dx_v[...] = dx
    gb = jnp.concatenate(
        [jnp.sum(dx * xh_ref[...], axis=0, keepdims=True), jnp.sum(dx, axis=0, keepdims=True), jnp.zeros((6, DIM), F32)], axis=0
    )
    for k, pay in enumerate((pay0, pay1, pay2, pay3)):
        pay[0:LOC, :] = dx_v[pl.ds(pl.multiple_of((me ^ k) * LOC, LOC), LOC), :]
        pay[LOC:, :] = gb
    for cp in copies:
        cp.wait()


def embed_kernel(demb_in, dz_ref, x_ref, small_ref, demb_ref, tok_ref, mean_ref, stage, out_sem):
    copies = write_rows(dz_ref, x_ref, demb_ref, stage, out_sem, EARLY_ROWS, EARLY_ROWS, LATE_TILES)
    tok_ref[...] = small_ref[0:1, 0:LOC]
    mean_ref[...] = small_ref[1:2, 0:1]
    for cp in copies:
        cp.wait()


def norm_kernel(p0, p1, p2, p3, xh_ref, rstd_ref, gain_in, dhid_ref, gain_ref, bias_ref, gb_v):
    me = lax.axis_index("tp")
    for k, pay in enumerate((p0, p1, p2, p3)):
        gb_v[me ^ k] = pay[LOC:, :]
    gb = gb_v[0] + gb_v[1] + gb_v[2] + gb_v[3]
    gain_ref[...] = gb[0:1, :]
    bias_ref[...] = gb[1:2, :]
    my_rows = pl.ds(pl.multiple_of(me * LOC, LOC), LOC)
    xh = xh_ref[my_rows, :]
    dxh = (p0[0:LOC, :] + p1[0:LOC, :] + p2[0:LOC, :] + p3[0:LOC, :]) * gain_in[2:3, :]
    m1 = row_sum(dxh) * (1.0 / DIM)
    m2 = row_sum(dxh * xh) * (1.0 / DIM)
    dhid_ref[...] = (rstd_ref[my_rows, 0:1] * (dxh - m1 - xh * m2)).astype(BF16)


def solution(mesh):
    vmem = pl.BlockSpec(memory_space=pltpu.VMEM)
    hbm = pl.BlockSpec(memory_space=pltpu.HBM)

    def group_step(hidden, ln_gain, ln_bias, out_embed, vocab_valid, targets, loss_mask):
        shape = jax.ShapeDtypeStruct
        small, xh, rstd, coef, tgt, x_all, g_all, emb = pl.pallas_call(
            main_kernel,
            out_shape=(
                shape((8, DIM), F32), shape((TOK, DIM), F32), shape((TOK, TOK), F32), shape((2, TOK, TOK), F32),
                shape((TOK, TOK), jnp.int32), shape((TOK, DIM), BF16), shape((TOK, VOCAB), F32), shape((VOCAB, DIM), BF16),
            ),
            in_specs=[hbm] * 7,
            out_specs=(vmem,) * 8,
            scratch_shapes=[
                pltpu.VMEM((LOC, DIM), BF16),
                pltpu.VMEM((1, DIM), F32),
                pltpu.VMEM((1, DIM), F32),
                pltpu.VMEM((VOCAB // TOK, TOK), jnp.int32),
                pltpu.VMEM((1, LOC), jnp.int32),
                pltpu.VMEM((1, LOC), jnp.int32),
                pltpu.VMEM((TOK, DIM), BF16),
                pltpu.VMEM((8 * TP, TOK), jnp.int32),
                pltpu.VMEM((8 * TP, TOK), F32),
                pltpu.VMEM((2, TOK, TOK), F32),
                pltpu.VMEM((BUFS, HALF, GROUP + TAIL), F32),
                pltpu.VMEM((DIM, VOCAB), BF16),
                pltpu.VMEM((TOK, TOK), jnp.int32),
                pltpu.SemaphoreType.DMA((GROUPS,)),
                pltpu.SemaphoreType.DMA((9,)),
                pltpu.SemaphoreType.DMA((9,)),
                pltpu.SemaphoreType.DMA((6,)),
            ],
            compiler_params=pltpu.CompilerParams(collective_id=0, has_side_effects=True, vmem_limit_bytes=30 * 1024 * 1024),
            name="main",
        )(
            *(
                pltpu.with_memory_space_constraint(val, pltpu.HBM)
                for val in (
                    hidden, ln_gain.reshape(1, DIM), ln_bias.reshape(1, DIM), out_embed,
                    vocab_valid.reshape(VOCAB // TOK, TOK), targets.reshape(1, LOC), loss_mask.reshape(1, LOC),
                )
            )
        )
        part = shape((LOC + 8, DIM), F32)
        early, dz, *pays = pl.pallas_call(
            grad_kernel,
            out_shape=(shape((VOCAB, DIM), F32), shape((TOK, VOCAB), BF16), part, part, part, part),
            in_specs=[vmem] * 6,
            out_specs=(hbm,) + (vmem,) * 5,
            scratch_shapes=[
                pltpu.VMEM((EARLY_ROWS, DIM), F32), pltpu.VMEM((TOK, DIM), F32), pltpu.SemaphoreType.DMA((len(EARLY_TILES),)),
            ],
            compiler_params=pltpu.CompilerParams(vmem_limit_bytes=16 * 1024 * 1024),
            name="grad",
        )(g_all, emb, x_all, xh, coef, tgt)
        moved = [lax.ppermute(pays[k], "tp", [(i, i ^ k) for i in range(TP)]) for k in range(1, TP)]
        d_embed, tok, mean = pl.pallas_call(
            embed_kernel,
            out_shape=(shape((VOCAB, DIM), F32), shape((1, LOC), F32), shape((1, 1), F32)),
            in_specs=[hbm] + [vmem] * 3,
            out_specs=(hbm, vmem, vmem),
            input_output_aliases={0: 0},
            scratch_shapes=[pltpu.VMEM((VOCAB - EARLY_ROWS, DIM), F32), pltpu.SemaphoreType.DMA((len(LATE_TILES),))],
            compiler_params=pltpu.CompilerParams(vmem_limit_bytes=30 * 1024 * 1024),
            cost_estimate=pl.CostEstimate(flops=2 * TOK * VOCAB * DIM, bytes_accessed=4 * VOCAB * DIM, transcendentals=0),
            name="embed",
        )(early, dz, x_all, small)
        d_hidden, d_gain, d_bias = pl.pallas_call(
            norm_kernel,
            out_shape=(shape((LOC, DIM), BF16), shape((1, DIM), F32), shape((1, DIM), F32)),
            in_specs=[vmem] * 7,
            out_specs=(vmem,) * 3,
            scratch_shapes=[pltpu.VMEM((TP, 8, DIM), F32)],
            compiler_params=pltpu.CompilerParams(vmem_limit_bytes=8 * 1024 * 1024),
            name="norm",
        )(pays[0], *moved, xh, rstd, small)
        return tok.reshape(LOC), mean.reshape(1), d_hidden, d_embed, d_gain.reshape(DIM), d_bias.reshape(DIM)

    row_spec = P(("dp", "tp"))
    mat_spec = P(("dp", "tp"), None)
    return jax.shard_map(
        group_step, mesh=mesh,
        in_specs=(mat_spec, P(None), P(None), P("tp", None), P("tp"), row_spec, row_spec),
        out_specs=(row_spec, P("dp"), mat_spec, mat_spec, P("dp"), P("dp")), check_vma=False,
    )
```

```python
import functools

import jax
import jax.numpy as jnp
from jax import lax
from jax.experimental import pallas as pl
from jax.experimental.pallas import tpu as pltpu
from jax.sharding import PartitionSpec as P

SOFT_CAP = 30.0
Z_COEF = 1e-4
LN_EPS = 1e-5
LOG2E = 1.4426950408889634
MESH = pl.DeviceIdType.MESH
F32 = jnp.float32
BF16 = jnp.bfloat16

TP = 4
TOK = 128
LOC = TOK // TP
DIM = 512
VOCAB = 12672
TILE = 256
GROUP = 7 * TILE
GROUPS = VOCAB // GROUP
TAIL = VOCAB - GROUP * GROUPS
BLK = 32
FWD = [GROUP] * 6 + [1024, 512, 384]


def row_sum(val):
    return jnp.sum(val, axis=-1, keepdims=True)


def main_kernel(
    hid_hbm, gain_hbm, bias_hbm, emb_ref, valid_hbm, tgt_hbm, mask_hbm,
    small_ref, xh_v, rstd_v, coef_ref, tgt_v, x_ref, g_v, emb_v,
    hid_ref, gain_ref, bias_ref, valid_ref, tgt_ref, mask_ref,
    hid_all, meta_v, stat_v, acc_v, z_v,
    emb_sem, send_sem, recv_sem, in_sem,
):
    me = lax.axis_index("tp")
    dp = lax.axis_index("dp")
    ins = [
        pltpu.make_async_copy(src, dst, in_sem.at[k])
        for k, (src, dst) in enumerate([
            (hid_hbm, hid_ref), (tgt_hbm, tgt_ref), (mask_hbm, mask_ref),
            (gain_hbm, gain_ref), (bias_hbm, bias_ref), (valid_hbm, valid_ref),
        ])
    ]
    for cp in ins:
        cp.start()
    chunks = [(j * GROUP, GROUP) for j in range(GROUPS - 1)]
    chunks.append(((GROUPS - 1) * GROUP, GROUP + TAIL))
    emb_copies = [
        pltpu.make_async_copy(emb_ref.at[pl.ds(s, n), :], emb_v.at[pl.ds(s, n), :], emb_sem.at[k])
        for k, (s, n) in enumerate(chunks)
    ]
    for cp in emb_copies:
        cp.start()

    barrier = pltpu.get_barrier_semaphore()
    for k in range(1, TP):
        pl.semaphore_signal(barrier, inc=1, device_id=(dp, lax.rem(me + k, TP)), device_id_type=MESH)

    for cp in ins[:3]:
        cp.wait()
    lane = lax.broadcasted_iota(jnp.int32, (1, TOK), 1)
    mine = (lane // LOC) == me
    tgt4 = jnp.concatenate([tgt_ref[...]] * TP, axis=1)
    mask4 = jnp.concatenate([mask_ref[...]] * TP, axis=1)
    my_rows = pl.ds(pl.multiple_of(me * LOC, LOC), LOC)
    my_meta = pl.ds(pl.multiple_of(me * 8, 8), 8)
    meta_v[my_meta, :] = jnp.concatenate(
        [jnp.where(mine, tgt4, 0), jnp.where(mine, mask4, 0), jnp.zeros((6, TOK), jnp.int32)], axis=0
    )
    hid_all[my_rows, :] = hid_ref[...]
    pl.semaphore_wait(barrier, TP - 1)

    def push(src, dst, idx):
        copies = []
        for k in range(1, TP):
            cp = pltpu.make_async_remote_copy(
                src_ref=src(k), dst_ref=dst, send_sem=send_sem.at[3 * idx + k - 1], recv_sem=recv_sem.at[3 * idx + k - 1],
                device_id=(dp, lax.rem(me + k, TP)), device_id_type=MESH,
            )
            cp.start()
            copies.append(cp)
        return copies

    first = push(lambda k: hid_ref, hid_all.at[my_rows, :], 0)
    first += push(lambda k: meta_v.at[my_meta, :], meta_v.at[my_meta, :], 1)
    for cp in ins[3:]:
        cp.wait()
    for cp in emb_copies:
        cp.wait()
    for cp in first:
        cp.wait_recv()

    meta = meta_v[0:8, :] + meta_v[8:16, :] + meta_v[16:24, :] + meta_v[24:32, :]
    tgt_row = meta[0:1, :]
    mask_row = meta[1:2, :].astype(F32)
    tok_count = row_sum(mask_row)
    tgt_col = jnp.transpose(jnp.broadcast_to(tgt_row, (TOK, TOK)))

    h = hid_all[...].astype(F32)
    mean_val = row_sum(h) * (1.0 / DIM)
    cent = h - mean_val
    var_val = row_sum(cent * cent) * (1.0 / DIM)
    rstd = lax.rsqrt(var_val + LN_EPS)
    xh = cent * rstd
    xh_v[...] = xh
    rstd_v[...] = jnp.broadcast_to(rstd, (TOK, TOK))
    x_ref[...] = (xh * gain_ref[...] + bias_ref[...]).astype(BF16)

    tgt_v[...] = tgt_col - me * VOCAB
    lane_blk = lax.broadcasted_iota(jnp.int32, (BLK, TOK), 1)
    groups = [(sum(FWD[:j]), n) for j, n in enumerate(FWD)]

    def softmax_pass(buf, g0, n):
        for tb in range(TOK // BLK):
            rows = pl.ds(tb * BLK, BLK)
            tgt = tgt_v[rows, :]
            s_acc = acc_v[0, rows, :]
            t_acc = acc_v[1, rows, :]
            for c in range(n // TOK):
                col = g0 + c * TOK
                t = jnp.tanh(z_v[buf, rows, pl.ds(c * TOK, TOK)] * (1.0 / SOFT_CAP))
                ok = valid_ref[col // TOK:col // TOK + 1, :].astype(F32)
                e = jnp.exp2(t * (SOFT_CAP * LOG2E)) * ok
                s_acc += e
                t_acc += jnp.where(tgt == lane_blk + col, t, 0.0)
                g_v[rows, pl.ds(col, TOK)] = e * (1.0 - t * t)
            acc_v[0, rows, :] = s_acc
            acc_v[1, rows, :] = t_acc

    acc_v[...] = jnp.zeros_like(acc_v)
    for j, (g0, n) in enumerate(groups):
        for s in range(0, n, TILE):
            w = min(TILE, n - s)
            z_v[j % 2, :, pl.ds(s, w)] = lax.dot_general(
                x_ref[...], emb_v[pl.ds(g0 + s, w), :], (((1,), (1,)), ((), ())), preferred_element_type=F32
            )
        if j > 0:
            softmax_pass((j - 1) % 2, *groups[j - 1])
    softmax_pass((len(FWD) - 1) % 2, *groups[-1])

    s_loc = jnp.sum(jnp.transpose(acc_v[0]), axis=0, keepdims=True)
    t_loc = jnp.sum(jnp.transpose(acc_v[1]), axis=0, keepdims=True)
    stat_v[my_meta, :] = jnp.concatenate([s_loc, t_loc, jnp.zeros((6, TOK), F32)], axis=0)
    second = push(lambda k: stat_v.at[my_meta, :], stat_v.at[my_meta, :], 2)
    for cp in second:
        cp.wait_recv()
    stats = stat_v[0:8, :] + stat_v[8:16, :] + stat_v[16:24, :] + stat_v[24:32, :]
    sum_exp = stats[0:1, :]
    t_tgt = stats[1:2, :]
    lse = jnp.log(sum_exp)
    loss = (lse - SOFT_CAP * t_tgt + Z_COEF * lse * lse) * mask_row
    mean_loss = row_sum(loss) / tok_count
    coef = mask_row / tok_count
    a_row = (1.0 + 2.0 * Z_COEF * lse) * coef / sum_exp
    c_row = coef * (1.0 - t_tgt * t_tgt)
    coef_ref[0] = jnp.transpose(jnp.broadcast_to(a_row, (TOK, TOK)))
    coef_ref[1] = jnp.transpose(jnp.broadcast_to(c_row, (TOK, TOK)))
    loss_me = pltpu.roll(loss, lax.rem(TOK - me * LOC, TOK), 1)
    pad = jnp.zeros((1, DIM - TOK), F32)
    small_ref[...] = jnp.concatenate(
        [
            jnp.concatenate([loss_me, pad], axis=1),
            jnp.broadcast_to(mean_loss, (1, DIM)),
            gain_ref[...],
            jnp.zeros((5, DIM), F32),
        ],
        axis=0,
    )
    for cp in first + second:
        cp.wait_send()


EARLY = 2
EARLY_ROWS = EARLY * GROUP
EARLY_TILES = [256, 640, 896, 896, 896]
HEAD = 256
LATE_TILES = [512] + [832] * 10


def write_rows(dz_ref, x_ref, out_ref, stage, sem, start, first, tiles):
    copies = []
    for k, n in enumerate(tiles):
        rows = pl.ds(start, n)
        local = pl.ds(start - first, n)
        stage[local, :] = lax.dot_general(
            dz_ref[:, rows], x_ref[...], (((0,), (0,)), ((), ())), preferred_element_type=F32
        )
        cp = pltpu.make_async_copy(stage.at[local, :], out_ref.at[rows, :], sem.at[k])
        cp.start()
        copies.append(cp)
        start += n
    return copies


def grad_kernel(
    g_ref, emb_ref, x_ref, xh_ref, coef_ref, tgt_ref, demb_ref, dz_ref, head_ref, pay0, pay1, pay2, pay3, stage, dx_v, out_sem
):
    me = lax.axis_index("tp")
    lane_blk = lax.broadcasted_iota(jnp.int32, (BLK, TOK), 1)
    groups = [(j * GROUP, GROUP) for j in range(GROUPS - 1)]
    groups.append(((GROUPS - 1) * GROUP, GROUP + TAIL))

    def logit_grad(g0, n):
        for tb in range(TOK // BLK):
            rows = pl.ds(tb * BLK, BLK)
            tgt = tgt_ref[rows, :]
            a_blk = coef_ref[0, rows, :]
            c_blk = coef_ref[1, rows, :]
            for c in range(n // TOK):
                cols = pl.ds(g0 + c * TOK, TOK)
                hit = tgt == lane_blk + (g0 + c * TOK)
                dz_ref[rows, cols] = (a_blk * g_ref[rows, cols] - jnp.where(hit, c_blk, 0.0)).astype(BF16)

    for g0, n in groups[:EARLY]:
        logit_grad(g0, n)
    copies = write_rows(dz_ref, x_ref, demb_ref, stage, out_sem, 0, 0, EARLY_TILES)
    dx = 0.0
    for j, (g0, n) in enumerate(groups):
        if j >= EARLY:
            logit_grad(g0, n)
        dx += jnp.dot(dz_ref[:, pl.ds(g0, n)], emb_ref[pl.ds(g0, n), :], preferred_element_type=F32)
    dx_v[...] = dx
    head_ref[...] = lax.dot_general(
        dz_ref[:, pl.ds(EARLY_ROWS, HEAD)], x_ref[...], (((0,), (0,)), ((), ())), preferred_element_type=F32
    )
    gb = jnp.concatenate(
        [jnp.sum(dx * xh_ref[...], axis=0, keepdims=True), jnp.sum(dx, axis=0, keepdims=True), jnp.zeros((6, DIM), F32)], axis=0
    )
    for k, pay in enumerate((pay0, pay1, pay2, pay3)):
        pay[0:LOC, :] = dx_v[pl.ds(pl.multiple_of((me ^ k) * LOC, LOC), LOC), :]
        pay[LOC:, :] = gb
    for cp in copies:
        cp.wait()


def embed_kernel(demb_in, dz_ref, head_ref, x_ref, small_ref, demb_ref, tok_ref, mean_ref, stage, out_sem, head_sem):
    head = pltpu.make_async_copy(head_ref, demb_ref.at[pl.ds(EARLY_ROWS, HEAD), :], head_sem)
    head.start()
    copies = write_rows(dz_ref, x_ref, demb_ref, stage, out_sem, EARLY_ROWS + HEAD, EARLY_ROWS + HEAD, LATE_TILES)
    copies.append(head)
    tok_ref[...] = small_ref[0:1, 0:LOC]
    mean_ref[...] = small_ref[1:2, 0:1]
    for cp in copies:
        cp.wait()


def norm_kernel(p0, p2, p3, p1, xh_ref, rstd_ref, gain_in, dhid_ref, gain_ref, bias_ref, gb_v):
    me = lax.axis_index("tp")
    for k, pay in enumerate((p0, p1, p2, p3)):
        gb_v[me ^ k] = pay[LOC:, :]
    gb = gb_v[0] + gb_v[1] + gb_v[2] + gb_v[3]
    gain_ref[...] = gb[0:1, :]
    bias_ref[...] = gb[1:2, :]
    my_rows = pl.ds(pl.multiple_of(me * LOC, LOC), LOC)
    xh = xh_ref[my_rows, :]
    dxh = (p0[0:LOC, :] + p1[0:LOC, :] + p2[0:LOC, :] + p3[0:LOC, :]) * gain_in[2:3, :]
    m1 = row_sum(dxh) * (1.0 / DIM)
    m2 = row_sum(dxh * xh) * (1.0 / DIM)
    dhid_ref[...] = (rstd_ref[my_rows, 0:1] * (dxh - m1 - xh * m2)).astype(BF16)


def solution(mesh):
    vmem = pl.BlockSpec(memory_space=pltpu.VMEM)
    hbm = pl.BlockSpec(memory_space=pltpu.HBM)

    def group_step(hidden, ln_gain, ln_bias, out_embed, vocab_valid, targets, loss_mask):
        shape = jax.ShapeDtypeStruct
        small, xh, rstd, coef, tgt, x_all, g_all, emb = pl.pallas_call(
            main_kernel,
            out_shape=(
                shape((8, DIM), F32), shape((TOK, DIM), F32), shape((TOK, TOK), F32), shape((2, TOK, TOK), F32),
                shape((TOK, TOK), jnp.int32), shape((TOK, DIM), BF16), shape((TOK, VOCAB), F32), shape((VOCAB, DIM), BF16),
            ),
            in_specs=[hbm] * 7,
            out_specs=(vmem,) * 8,
            scratch_shapes=[
                pltpu.VMEM((LOC, DIM), BF16),
                pltpu.VMEM((1, DIM), F32),
                pltpu.VMEM((1, DIM), F32),
                pltpu.VMEM((VOCAB // TOK, TOK), jnp.int32),
                pltpu.VMEM((1, LOC), jnp.int32),
                pltpu.VMEM((1, LOC), jnp.int32),
                pltpu.VMEM((TOK, DIM), BF16),
                pltpu.VMEM((8 * TP, TOK), jnp.int32),
                pltpu.VMEM((8 * TP, TOK), F32),
                pltpu.VMEM((2, TOK, TOK), F32),
                pltpu.VMEM((2, TOK, GROUP), F32),
                pltpu.SemaphoreType.DMA((GROUPS,)),
                pltpu.SemaphoreType.DMA((9,)),
                pltpu.SemaphoreType.DMA((9,)),
                pltpu.SemaphoreType.DMA((6,)),
            ],
            compiler_params=pltpu.CompilerParams(collective_id=0, has_side_effects=True, vmem_limit_bytes=30 * 1024 * 1024),
            name="main",
        )(
            *(
                pltpu.with_memory_space_constraint(val, pltpu.HBM)
                for val in (
                    hidden, ln_gain.reshape(1, DIM), ln_bias.reshape(1, DIM), out_embed,
                    vocab_valid.reshape(VOCAB // TOK, TOK), targets.reshape(1, LOC), loss_mask.reshape(1, LOC),
                )
            )
        )
        part = shape((LOC + 8, DIM), F32)
        early, dz, head, *pays = pl.pallas_call(
            grad_kernel,
            out_shape=(shape((VOCAB, DIM), F32), shape((TOK, VOCAB), BF16), shape((HEAD, DIM), F32), part, part, part, part),
            in_specs=[vmem] * 6,
            out_specs=(hbm,) + (vmem,) * 6,
            scratch_shapes=[
                pltpu.VMEM((EARLY_ROWS, DIM), F32), pltpu.VMEM((TOK, DIM), F32), pltpu.SemaphoreType.DMA((len(EARLY_TILES),)),
            ],
            compiler_params=pltpu.CompilerParams(vmem_limit_bytes=16 * 1024 * 1024),
            name="grad",
        )(g_all, emb, x_all, xh, coef, tgt)
        moved = [lax.ppermute(pays[k], "tp", [(i, i ^ k) for i in range(TP)]) for k in (2, 3, 1)]
        d_embed, tok, mean = pl.pallas_call(
            embed_kernel,
            out_shape=(shape((VOCAB, DIM), F32), shape((1, LOC), F32), shape((1, 1), F32)),
            in_specs=[hbm] + [vmem] * 4,
            out_specs=(hbm, vmem, vmem),
            input_output_aliases={0: 0},
            scratch_shapes=[
                pltpu.VMEM((VOCAB - EARLY_ROWS - HEAD, DIM), F32), pltpu.SemaphoreType.DMA((len(LATE_TILES),)), pltpu.SemaphoreType.DMA,
            ],
            compiler_params=pltpu.CompilerParams(vmem_limit_bytes=30 * 1024 * 1024),
            cost_estimate=pl.CostEstimate(flops=2 * TOK * VOCAB * DIM, bytes_accessed=4 * VOCAB * DIM, transcendentals=0),
            name="embed",
        )(early, dz, head, x_all, small)
        d_hidden, d_gain, d_bias = pl.pallas_call(
            norm_kernel,
            out_shape=(shape((LOC, DIM), BF16), shape((1, DIM), F32), shape((1, DIM), F32)),
            in_specs=[vmem] * 7,
            out_specs=(vmem,) * 3,
            scratch_shapes=[pltpu.VMEM((TP, 8, DIM), F32)],
            compiler_params=pltpu.CompilerParams(vmem_limit_bytes=8 * 1024 * 1024),
            name="norm",
        )(pays[0], *moved, xh, rstd, small)
        return tok.reshape(LOC), mean.reshape(1), d_hidden, d_embed, d_gain.reshape(DIM), d_bias.reshape(DIM)

    row_spec = P(("dp", "tp"))
    mat_spec = P(("dp", "tp"), None)
    return jax.shard_map(
        group_step, mesh=mesh,
        in_specs=(mat_spec, P(None), P(None), P("tp", None), P("tp"), row_spec, row_spec),
        out_specs=(row_spec, P("dp"), mat_spec, mat_spec, P("dp"), P("dp")), check_vma=False,
    )
```

```python
import functools

import jax
import jax.numpy as jnp
from jax import lax
from jax.experimental import pallas as pl
from jax.experimental.pallas import tpu as pltpu
from jax.sharding import PartitionSpec as P

SOFT_CAP = 30.0
Z_COEF = 1e-4
LN_EPS = 1e-5
LOG2E = 1.4426950408889634
MESH = pl.DeviceIdType.MESH
F32 = jnp.float32
BF16 = jnp.bfloat16

TP = 4
TOK = 128
LOC = TOK // TP
DIM = 512
VOCAB = 12672
TILE = 256
GROUP = 7 * TILE
GROUPS = VOCAB // GROUP
TAIL = VOCAB - GROUP * GROUPS
BLK = 32
TURN = 3
TURNED = TURN * GROUP
FWD = [7] * 6 + [4, 2, 2]


def row_sum(val):
    return jnp.sum(val, axis=-1, keepdims=True)


def main_kernel(
    hid_hbm, gain_hbm, bias_hbm, emb_ref, valid_hbm, tgt_hbm, mask_hbm,
    small_ref, xh_v, rstd_v, coef_ref, tgt_v, x_ref, g_v, emb_v,
    hid_ref, gain_ref, bias_ref, valid_ref, tgt_ref, mask_ref,
    hid_all, meta_v, stat_v, acc_v, z_v, embt_v,
    emb_sem, send_sem, recv_sem, in_sem,
):
    me = lax.axis_index("tp")
    dp = lax.axis_index("dp")
    ins = [
        pltpu.make_async_copy(src, dst, in_sem.at[k])
        for k, (src, dst) in enumerate([
            (hid_hbm, hid_ref), (tgt_hbm, tgt_ref), (mask_hbm, mask_ref),
            (gain_hbm, gain_ref), (bias_hbm, bias_ref), (valid_hbm, valid_ref),
        ])
    ]
    for cp in ins:
        cp.start()
    chunks = [(j * GROUP, GROUP) for j in range(GROUPS - 1)]
    chunks.append(((GROUPS - 1) * GROUP, GROUP + TAIL))
    emb_copies = [
        pltpu.make_async_copy(emb_ref.at[pl.ds(s, n), :], emb_v.at[pl.ds(s, n), :], emb_sem.at[k])
        for k, (s, n) in enumerate(chunks)
    ]
    for cp in emb_copies:
        cp.start()

    barrier = pltpu.get_barrier_semaphore()
    for k in range(1, TP):
        pl.semaphore_signal(barrier, inc=1, device_id=(dp, lax.rem(me + k, TP)), device_id_type=MESH)

    for cp in ins[:3]:
        cp.wait()
    lane = lax.broadcasted_iota(jnp.int32, (1, TOK), 1)
    mine = (lane // LOC) == me
    tgt4 = jnp.concatenate([tgt_ref[...]] * TP, axis=1)
    mask4 = jnp.concatenate([mask_ref[...]] * TP, axis=1)
    my_rows = pl.ds(pl.multiple_of(me * LOC, LOC), LOC)
    my_meta = pl.ds(pl.multiple_of(me * 8, 8), 8)
    meta_v[my_meta, :] = jnp.concatenate(
        [jnp.where(mine, tgt4, 0), jnp.where(mine, mask4, 0), jnp.zeros((6, TOK), jnp.int32)], axis=0
    )
    hid_all[my_rows, :] = hid_ref[...]
    pl.semaphore_wait(barrier, TP - 1)

    def push(src, dst, idx):
        copies = []
        for k in range(1, TP):
            cp = pltpu.make_async_remote_copy(
                src_ref=src(k), dst_ref=dst, send_sem=send_sem.at[3 * idx + k - 1], recv_sem=recv_sem.at[3 * idx + k - 1],
                device_id=(dp, lax.rem(me + k, TP)), device_id_type=MESH,
            )
            cp.start()
            copies.append(cp)
        return copies

    first = push(lambda k: hid_ref, hid_all.at[my_rows, :], 0)
    first += push(lambda k: meta_v.at[my_meta, :], meta_v.at[my_meta, :], 1)
    for cp in ins[3:]:
        cp.wait()
    for cp, (g0, n) in zip(emb_copies[:TURN], chunks):
        cp.wait()
        for s in range(g0, g0 + n, TILE):
            embt_v[:, pl.ds(s, TILE)] = jnp.transpose(emb_v[pl.ds(s, TILE), :])
    for cp in first:
        cp.wait_recv()

    meta = meta_v[0:8, :] + meta_v[8:16, :] + meta_v[16:24, :] + meta_v[24:32, :]
    tgt_row = meta[0:1, :]
    mask_row = meta[1:2, :].astype(F32)
    tok_count = row_sum(mask_row)
    tgt_col = jnp.transpose(jnp.broadcast_to(tgt_row, (TOK, TOK)))

    h = hid_all[...].astype(F32)
    mean_val = row_sum(h) * (1.0 / DIM)
    cent = h - mean_val
    var_val = row_sum(cent * cent) * (1.0 / DIM)
    rstd = lax.rsqrt(var_val + LN_EPS)
    xh = cent * rstd
    xh_v[...] = xh
    rstd_v[...] = jnp.broadcast_to(rstd, (TOK, TOK))
    x_ref[...] = (xh * gain_ref[...] + bias_ref[...]).astype(BF16)

    tgt_v[...] = tgt_col - me * VOCAB
    lane_blk = lax.broadcasted_iota(jnp.int32, (BLK, TOK), 1)
    plain = [(s, TILE) for s in range(0, TURNED, TILE)]
    other = [(s, min(TILE, VOCAB - s)) for s in range(TURNED, VOCAB, TILE)]
    tiles = []
    while plain or other:
        if other:
            tiles.append(other.pop(0))
        if plain:
            tiles.append(plain.pop(0))
    groups = []
    for n in FWD:
        groups.append(tiles[:n])
        tiles = tiles[n:]

    def logits(j):
        pos = 0
        for col, w in groups[j]:
            if col < TURNED:
                z = jnp.dot(x_ref[...], embt_v[:, pl.ds(col, w)], preferred_element_type=F32)
            else:
                z = lax.dot_general(
                    x_ref[...], emb_v[pl.ds(col, w), :], (((1,), (1,)), ((), ())), preferred_element_type=F32
                )
            z_v[j % 2, :, pl.ds(pos, w)] = z
            pos += w

    def softmax_pass(j):
        cols = [c for col, w in groups[j] for c in range(col, col + w, TOK)]
        for tb in range(TOK // BLK):
            rows = pl.ds(tb * BLK, BLK)
            tgt = tgt_v[rows, :]
            s_acc = acc_v[0, rows, :]
            t_acc = acc_v[1, rows, :]
            for c, col in enumerate(cols):
                t = jnp.tanh(z_v[j % 2, rows, pl.ds(c * TOK, TOK)] * (1.0 / SOFT_CAP))
                ok = valid_ref[col // TOK:col // TOK + 1, :].astype(F32)
                e = jnp.exp2(t * (SOFT_CAP * LOG2E)) * ok
                s_acc += e
                t_acc += jnp.where(tgt == lane_blk + col, t, 0.0)
                g_v[rows, pl.ds(col, TOK)] = e * (1.0 - t * t)
            acc_v[0, rows, :] = s_acc
            acc_v[1, rows, :] = t_acc

    for cp in emb_copies[TURN:]:
        cp.wait()
    acc_v[...] = jnp.zeros_like(acc_v)
    for j in range(len(groups)):
        logits(j)
        if j > 0:
            softmax_pass(j - 1)
    softmax_pass(len(groups) - 1)

    s_loc = jnp.sum(jnp.transpose(acc_v[0]), axis=0, keepdims=True)
    t_loc = jnp.sum(jnp.transpose(acc_v[1]), axis=0, keepdims=True)
    stat_v[my_meta, :] = jnp.concatenate([s_loc, t_loc, jnp.zeros((6, TOK), F32)], axis=0)
    second = push(lambda k: stat_v.at[my_meta, :], stat_v.at[my_meta, :], 2)
    for cp in second:
        cp.wait_recv()
    stats = stat_v[0:8, :] + stat_v[8:16, :] + stat_v[16:24, :] + stat_v[24:32, :]
    sum_exp = stats[0:1, :]
    t_tgt = stats[1:2, :]
    lse = jnp.log(sum_exp)
    loss = (lse - SOFT_CAP * t_tgt + Z_COEF * lse * lse) * mask_row
    mean_loss = row_sum(loss) / tok_count
    coef = mask_row / tok_count
    a_row = (1.0 + 2.0 * Z_COEF * lse) * coef / sum_exp
    c_row = coef * (1.0 - t_tgt * t_tgt)
    coef_ref[0] = jnp.transpose(jnp.broadcast_to(a_row, (TOK, TOK)))
    coef_ref[1] = jnp.transpose(jnp.broadcast_to(c_row, (TOK, TOK)))
    loss_me = pltpu.roll(loss, lax.rem(TOK - me * LOC, TOK), 1)
    pad = jnp.zeros((1, DIM - TOK), F32)
    small_ref[...] = jnp.concatenate(
        [
            jnp.concatenate([loss_me, pad], axis=1),
            jnp.broadcast_to(mean_loss, (1, DIM)),
            gain_ref[...],
            jnp.zeros((5, DIM), F32),
        ],
        axis=0,
    )
    for cp in first + second:
        cp.wait_send()


EARLY = 2
EARLY_ROWS = EARLY * GROUP
EARLY_TILES = [256, 640, 896, 896, 896]
LATE_TILES = [256, 512] + [832] * 10


def write_rows(dz_ref, x_ref, out_ref, stage, sem, start, first, tiles):
    copies = []
    for k, n in enumerate(tiles):
        rows = pl.ds(start, n)
        local = pl.ds(start - first, n)
        stage[local, :] = lax.dot_general(
            dz_ref[:, rows], x_ref[...], (((0,), (0,)), ((), ())), preferred_element_type=F32
        )
        cp = pltpu.make_async_copy(stage.at[local, :], out_ref.at[rows, :], sem.at[k])
        cp.start()
        copies.append(cp)
        start += n
    return copies


def grad_kernel(
    g_ref, emb_ref, x_ref, xh_ref, coef_ref, tgt_ref, demb_ref, dz_ref, pay0, pay1, pay2, pay3, stage, dx_v, out_sem
):
    me = lax.axis_index("tp")
    lane_blk = lax.broadcasted_iota(jnp.int32, (BLK, TOK), 1)
    groups = [(j * GROUP, GROUP) for j in range(GROUPS - 1)]
    groups.append(((GROUPS - 1) * GROUP, GROUP + TAIL))

    def logit_grad(g0, n):
        for tb in range(TOK // BLK):
            rows = pl.ds(tb * BLK, BLK)
            tgt = tgt_ref[rows, :]
            a_blk = coef_ref[0, rows, :]
            c_blk = coef_ref[1, rows, :]
            for c in range(n // TOK):
                cols = pl.ds(g0 + c * TOK, TOK)
                hit = tgt == lane_blk + (g0 + c * TOK)
                dz_ref[rows, cols] = (a_blk * g_ref[rows, cols] - jnp.where(hit, c_blk, 0.0)).astype(BF16)

    for g0, n in groups[:EARLY]:
        logit_grad(g0, n)
    copies = write_rows(dz_ref, x_ref, demb_ref, stage, out_sem, 0, 0, EARLY_TILES)
    dx = 0.0
    for j, (g0, n) in enumerate(groups):
        if j >= EARLY:
            logit_grad(g0, n)
        dx += jnp.dot(dz_ref[:, pl.ds(g0, n)], emb_ref[pl.ds(g0, n), :], preferred_element_type=F32)
    dx_v[...] = dx
    gb = jnp.concatenate(
        [jnp.sum(dx * xh_ref[...], axis=0, keepdims=True), jnp.sum(dx, axis=0, keepdims=True), jnp.zeros((6, DIM), F32)], axis=0
    )
    for k, pay in enumerate((pay0, pay1, pay2, pay3)):
        pay[0:LOC, :] = dx_v[pl.ds(pl.multiple_of((me ^ k) * LOC, LOC), LOC), :]
        pay[LOC:, :] = gb
    for cp in copies:
        cp.wait()


def embed_kernel(demb_in, dz_ref, x_ref, small_ref, demb_ref, tok_ref, mean_ref, stage, out_sem):
    copies = write_rows(dz_ref, x_ref, demb_ref, stage, out_sem, EARLY_ROWS, EARLY_ROWS, LATE_TILES)
    tok_ref[...] = small_ref[0:1, 0:LOC]
    mean_ref[...] = small_ref[1:2, 0:1]
    for cp in copies:
        cp.wait()


def norm_kernel(p0, p1, p2, p3, xh_ref, rstd_ref, gain_in, dhid_ref, gain_ref, bias_ref, gb_v):
    me = lax.axis_index("tp")
    for k, pay in enumerate((p0, p1, p2, p3)):
        gb_v[me ^ k] = pay[LOC:, :]
    gb = gb_v[0] + gb_v[1] + gb_v[2] + gb_v[3]
    gain_ref[...] = gb[0:1, :]
    bias_ref[...] = gb[1:2, :]
    my_rows = pl.ds(pl.multiple_of(me * LOC, LOC), LOC)
    xh = xh_ref[my_rows, :]
    dxh = (p0[0:LOC, :] + p1[0:LOC, :] + p2[0:LOC, :] + p3[0:LOC, :]) * gain_in[2:3, :]
    m1 = row_sum(dxh) * (1.0 / DIM)
    m2 = row_sum(dxh * xh) * (1.0 / DIM)
    dhid_ref[...] = (rstd_ref[my_rows, 0:1] * (dxh - m1 - xh * m2)).astype(BF16)


def solution(mesh):
    vmem = pl.BlockSpec(memory_space=pltpu.VMEM)
    hbm = pl.BlockSpec(memory_space=pltpu.HBM)

    def group_step(hidden, ln_gain, ln_bias, out_embed, vocab_valid, targets, loss_mask):
        shape = jax.ShapeDtypeStruct
        small, xh, rstd, coef, tgt, x_all, g_all, emb = pl.pallas_call(
            main_kernel,
            out_shape=(
                shape((8, DIM), F32), shape((TOK, DIM), F32), shape((TOK, TOK), F32), shape((2, TOK, TOK), F32),
                shape((TOK, TOK), jnp.int32), shape((TOK, DIM), BF16), shape((TOK, VOCAB), F32), shape((VOCAB, DIM), BF16),
            ),
            in_specs=[hbm] * 7,
            out_specs=(vmem,) * 8,
            scratch_shapes=[
                pltpu.VMEM((LOC, DIM), BF16),
                pltpu.VMEM((1, DIM), F32),
                pltpu.VMEM((1, DIM), F32),
                pltpu.VMEM((VOCAB // TOK, TOK), jnp.int32),
                pltpu.VMEM((1, LOC), jnp.int32),
                pltpu.VMEM((1, LOC), jnp.int32),
                pltpu.VMEM((TOK, DIM), BF16),
                pltpu.VMEM((8 * TP, TOK), jnp.int32),
                pltpu.VMEM((8 * TP, TOK), F32),
                pltpu.VMEM((2, TOK, TOK), F32),
                pltpu.VMEM((2, TOK, GROUP), F32),
                pltpu.VMEM((DIM, TURNED), BF16),
                pltpu.SemaphoreType.DMA((GROUPS,)),
                pltpu.SemaphoreType.DMA((9,)),
                pltpu.SemaphoreType.DMA((9,)),
                pltpu.SemaphoreType.DMA((6,)),
            ],
            compiler_params=pltpu.CompilerParams(collective_id=0, has_side_effects=True, vmem_limit_bytes=30 * 1024 * 1024),
            name="main",
        )(
            *(
                pltpu.with_memory_space_constraint(val, pltpu.HBM)
                for val in (
                    hidden, ln_gain.reshape(1, DIM), ln_bias.reshape(1, DIM), out_embed,
                    vocab_valid.reshape(VOCAB // TOK, TOK), targets.reshape(1, LOC), loss_mask.reshape(1, LOC),
                )
            )
        )
        part = shape((LOC + 8, DIM), F32)
        early, dz, *pays = pl.pallas_call(
            grad_kernel,
            out_shape=(shape((VOCAB, DIM), F32), shape((TOK, VOCAB), BF16), part, part, part, part),
            in_specs=[vmem] * 6,
            out_specs=(hbm,) + (vmem,) * 5,
            scratch_shapes=[
                pltpu.VMEM((EARLY_ROWS, DIM), F32), pltpu.VMEM((TOK, DIM), F32), pltpu.SemaphoreType.DMA((len(EARLY_TILES),)),
            ],
            compiler_params=pltpu.CompilerParams(vmem_limit_bytes=16 * 1024 * 1024),
            name="grad",
        )(g_all, emb, x_all, xh, coef, tgt)
        moved = [lax.ppermute(pays[k], "tp", [(i, i ^ k) for i in range(TP)]) for k in range(1, TP)]
        d_embed, tok, mean = pl.pallas_call(
            embed_kernel,
            out_shape=(shape((VOCAB, DIM), F32), shape((1, LOC), F32), shape((1, 1), F32)),
            in_specs=[hbm] + [vmem] * 3,
            out_specs=(hbm, vmem, vmem),
            input_output_aliases={0: 0},
            scratch_shapes=[pltpu.VMEM((VOCAB - EARLY_ROWS, DIM), F32), pltpu.SemaphoreType.DMA((len(LATE_TILES),))],
            compiler_params=pltpu.CompilerParams(vmem_limit_bytes=30 * 1024 * 1024),
            cost_estimate=pl.CostEstimate(flops=2 * TOK * VOCAB * DIM, bytes_accessed=4 * VOCAB * DIM, transcendentals=0),
            name="embed",
        )(early, dz, x_all, small)
        d_hidden, d_gain, d_bias = pl.pallas_call(
            norm_kernel,
            out_shape=(shape((LOC, DIM), BF16), shape((1, DIM), F32), shape((1, DIM), F32)),
            in_specs=[vmem] * 7,
            out_specs=(vmem,) * 3,
            scratch_shapes=[pltpu.VMEM((TP, 8, DIM), F32)],
            compiler_params=pltpu.CompilerParams(vmem_limit_bytes=8 * 1024 * 1024),
            name="norm",
        )(pays[0], *moved, xh, rstd, small)
        return tok.reshape(LOC), mean.reshape(1), d_hidden, d_embed, d_gain.reshape(DIM), d_bias.reshape(DIM)

    row_spec = P(("dp", "tp"))
    mat_spec = P(("dp", "tp"), None)
    return jax.shard_map(
        group_step, mesh=mesh,
        in_specs=(mat_spec, P(None), P(None), P("tp", None), P("tp"), row_spec, row_spec),
        out_specs=(row_spec, P("dp"), mat_spec, mat_spec, P("dp"), P("dp")), check_vma=False,
    )
```

```python
import functools

import jax
import jax.numpy as jnp
from jax import lax
from jax.experimental import pallas as pl
from jax.experimental.pallas import tpu as pltpu
from jax.sharding import PartitionSpec as P

SOFT_CAP = 30.0
Z_COEF = 1e-4
LN_EPS = 1e-5
LOG2E = 1.4426950408889634
MESH = pl.DeviceIdType.MESH
F32 = jnp.float32
BF16 = jnp.bfloat16

TP = 4
TOK = 128
LOC = TOK // TP
DIM = 512
VOCAB = 12672
TILE = 256
GROUP = 7 * TILE
GROUPS = VOCAB // GROUP
TAIL = VOCAB - GROUP * GROUPS
BLK = 32
TURN = 3
TURNED = TURN * GROUP
FWD = [7] * 6 + [4, 2, 2]


def row_sum(val):
    return jnp.sum(val, axis=-1, keepdims=True)


def main_kernel(
    hid_hbm, gain_hbm, bias_hbm, emb_ref, valid_hbm, tgt_hbm, mask_hbm,
    small_ref, xh_v, rstd_v, coef_ref, tgt_v, x_ref, g_v, emb_v,
    hid_ref, gain_ref, bias_ref, valid_ref, tgt_ref, mask_ref,
    hid_all, meta_v, stat_v, acc_v, z_v, embt_v,
    emb_sem, send_sem, recv_sem, in_sem,
):
    me = lax.axis_index("tp")
    dp = lax.axis_index("dp")
    ins = [
        pltpu.make_async_copy(src, dst, in_sem.at[k])
        for k, (src, dst) in enumerate([
            (hid_hbm, hid_ref), (tgt_hbm, tgt_ref), (mask_hbm, mask_ref),
            (gain_hbm, gain_ref), (bias_hbm, bias_ref), (valid_hbm, valid_ref),
        ])
    ]
    for cp in ins:
        cp.start()
    chunks = [(j * GROUP, GROUP) for j in range(GROUPS - 1)]
    chunks.append(((GROUPS - 1) * GROUP, GROUP + TAIL))
    emb_copies = [
        pltpu.make_async_copy(emb_ref.at[pl.ds(s, n), :], emb_v.at[pl.ds(s, n), :], emb_sem.at[k])
        for k, (s, n) in enumerate(chunks)
    ]
    for cp in emb_copies:
        cp.start()

    barrier = pltpu.get_barrier_semaphore()
    for k in range(1, TP):
        pl.semaphore_signal(barrier, inc=1, device_id=(dp, lax.rem(me + k, TP)), device_id_type=MESH)

    for cp in ins[:3]:
        cp.wait()
    lane = lax.broadcasted_iota(jnp.int32, (1, TOK), 1)
    mine = (lane // LOC) == me
    tgt4 = jnp.concatenate([tgt_ref[...]] * TP, axis=1)
    mask4 = jnp.concatenate([mask_ref[...]] * TP, axis=1)
    my_rows = pl.ds(pl.multiple_of(me * LOC, LOC), LOC)
    my_meta = pl.ds(pl.multiple_of(me * 8, 8), 8)
    meta_v[my_meta, :] = jnp.concatenate(
        [jnp.where(mine, tgt4, 0), jnp.where(mine, mask4, 0), jnp.zeros((6, TOK), jnp.int32)], axis=0
    )
    hid_all[my_rows, :] = hid_ref[...]
    pl.semaphore_wait(barrier, TP - 1)

    def push(src, dst, idx):
        copies = []
        for k in range(1, TP):
            cp = pltpu.make_async_remote_copy(
                src_ref=src(k), dst_ref=dst, send_sem=send_sem.at[3 * idx + k - 1], recv_sem=recv_sem.at[3 * idx + k - 1],
                device_id=(dp, lax.rem(me + k, TP)), device_id_type=MESH,
            )
            cp.start()
            copies.append(cp)
        return copies

    first = push(lambda k: hid_ref, hid_all.at[my_rows, :], 0)
    first += push(lambda k: meta_v.at[my_meta, :], meta_v.at[my_meta, :], 1)
    for cp in ins[3:]:
        cp.wait()
    for cp, (g0, n) in zip(emb_copies[:TURN], chunks):
        cp.wait()
        for s in range(g0, g0 + n, TILE):
            embt_v[:, pl.ds(s, TILE)] = jnp.transpose(emb_v[pl.ds(s, TILE), :])
    for cp in first:
        cp.wait_recv()

    meta = meta_v[0:8, :] + meta_v[8:16, :] + meta_v[16:24, :] + meta_v[24:32, :]
    tgt_row = meta[0:1, :]
    mask_row = meta[1:2, :].astype(F32)
    tok_count = row_sum(mask_row)
    tgt_col = jnp.transpose(jnp.broadcast_to(tgt_row, (TOK, TOK)))

    h = hid_all[...].astype(F32)
    mean_val = row_sum(h) * (1.0 / DIM)
    cent = h - mean_val
    var_val = row_sum(cent * cent) * (1.0 / DIM)
    rstd = lax.rsqrt(var_val + LN_EPS)
    xh = cent * rstd
    xh_v[...] = xh
    rstd_v[...] = jnp.broadcast_to(rstd, (TOK, TOK))
    x_ref[...] = (xh * gain_ref[...] + bias_ref[...]).astype(BF16)

    tgt_v[...] = tgt_col - me * VOCAB
    lane_blk = lax.broadcasted_iota(jnp.int32, (BLK, TOK), 1)
    plain = [(s, TILE) for s in range(0, TURNED, TILE)]
    other = [(s, min(TILE, VOCAB - s)) for s in range(TURNED, VOCAB, TILE)]
    tiles = []
    while plain or other:
        if other:
            tiles.append(other.pop(0))
        if plain:
            tiles.append(plain.pop(0))
    groups = []
    for n in FWD:
        groups.append(tiles[:n])
        tiles = tiles[n:]

    def logits(j):
        pos = 0
        for col, w in groups[j]:
            if col < TURNED:
                z = jnp.dot(x_ref[...], embt_v[:, pl.ds(col, w)], preferred_element_type=F32)
            else:
                z = lax.dot_general(
                    x_ref[...], emb_v[pl.ds(col, w), :], (((1,), (1,)), ((), ())), preferred_element_type=F32
                )
            z_v[j % 2, :, pl.ds(pos, w)] = z
            pos += w

    def softmax_pass(j):
        cols = [c for col, w in groups[j] for c in range(col, col + w, TOK)]
        for tb in range(TOK // BLK):
            rows = pl.ds(tb * BLK, BLK)
            tgt = tgt_v[rows, :]
            s_acc = acc_v[0, rows, :]
            t_acc = acc_v[1, rows, :]
            for c, col in enumerate(cols):
                t = jnp.tanh(z_v[j % 2, rows, pl.ds(c * TOK, TOK)] * (1.0 / SOFT_CAP))
                ok = valid_ref[col // TOK:col // TOK + 1, :].astype(F32)
                e = jnp.exp2(t * (SOFT_CAP * LOG2E)) * ok
                s_acc += e
                t_acc += jnp.where(tgt == lane_blk + col, t, 0.0)
                g_v[rows, pl.ds(col, TOK)] = e * (1.0 - t * t)
            acc_v[0, rows, :] = s_acc
            acc_v[1, rows, :] = t_acc

    for cp in emb_copies[TURN:]:
        cp.wait()
    acc_v[...] = jnp.zeros_like(acc_v)
    for j in range(len(groups)):
        logits(j)
        if j > 0:
            softmax_pass(j - 1)
    softmax_pass(len(groups) - 1)

    s_loc = jnp.sum(jnp.transpose(acc_v[0]), axis=0, keepdims=True)
    t_loc = jnp.sum(jnp.transpose(acc_v[1]), axis=0, keepdims=True)
    stat_v[my_meta, :] = jnp.concatenate([s_loc, t_loc, jnp.zeros((6, TOK), F32)], axis=0)
    second = push(lambda k: stat_v.at[my_meta, :], stat_v.at[my_meta, :], 2)
    for cp in second:
        cp.wait_recv()
    stats = stat_v[0:8, :] + stat_v[8:16, :] + stat_v[16:24, :] + stat_v[24:32, :]
    sum_exp = stats[0:1, :]
    t_tgt = stats[1:2, :]
    lse = jnp.log(sum_exp)
    coef = mask_row / tok_count
    a_row = (1.0 + 2.0 * Z_COEF * lse) * coef / sum_exp
    c_row = coef * (1.0 - t_tgt * t_tgt)
    coef_ref[0] = jnp.transpose(jnp.broadcast_to(a_row, (TOK, TOK)))
    coef_ref[1] = jnp.transpose(jnp.broadcast_to(c_row, (TOK, TOK)))
    pad = jnp.zeros((1, DIM - TOK), F32)
    small_ref[...] = jnp.concatenate(
        [jnp.concatenate([row, pad], axis=1) for row in (sum_exp, t_tgt, mask_row)] + [gain_ref[...], jnp.zeros((4, DIM), F32)],
        axis=0,
    )
    for cp in first + second:
        cp.wait_send()


EARLY = 2
EARLY_ROWS = 2688
EARLY_TILES = [256, 640, 896, 896]
LATE_TILES = [256, 512] + [768] * 12


def write_rows(dz_ref, x_ref, out_ref, stage, sem, start, first, tiles):
    copies = []
    for k, n in enumerate(tiles):
        rows = pl.ds(start, n)
        local = pl.ds(start - first, n)
        stage[local, :] = lax.dot_general(
            dz_ref[:, rows], x_ref[...], (((0,), (0,)), ((), ())), preferred_element_type=F32
        )
        cp = pltpu.make_async_copy(stage.at[local, :], out_ref.at[rows, :], sem.at[k])
        cp.start(priority=k % 2)
        copies.append(cp)
        start += n
    return copies


def grad_kernel(
    g_ref, emb_ref, x_ref, xh_ref, coef_ref, tgt_ref, demb_ref, dz_ref, pay0, pay1, pay2, pay3, stage, dx_v, out_sem
):
    me = lax.axis_index("tp")
    lane_blk = lax.broadcasted_iota(jnp.int32, (BLK, TOK), 1)
    groups = [(j * GROUP, GROUP) for j in range(GROUPS - 1)]
    groups.append(((GROUPS - 1) * GROUP, GROUP + TAIL))

    def logit_grad(g0, n):
        for tb in range(TOK // BLK):
            rows = pl.ds(tb * BLK, BLK)
            tgt = tgt_ref[rows, :]
            a_blk = coef_ref[0, rows, :]
            c_blk = coef_ref[1, rows, :]
            for c in range(n // TOK):
                cols = pl.ds(g0 + c * TOK, TOK)
                hit = tgt == lane_blk + (g0 + c * TOK)
                dz_ref[rows, cols] = (a_blk * g_ref[rows, cols] - jnp.where(hit, c_blk, 0.0)).astype(BF16)

    for g0, n in groups[:EARLY]:
        logit_grad(g0, n)
    copies = write_rows(dz_ref, x_ref, demb_ref, stage, out_sem, 0, 0, EARLY_TILES)
    dx = 0.0
    for j, (g0, n) in enumerate(groups):
        if j >= EARLY:
            logit_grad(g0, n)
        dx += jnp.dot(dz_ref[:, pl.ds(g0, n)], emb_ref[pl.ds(g0, n), :], preferred_element_type=F32)
    dx_v[...] = dx
    gb = jnp.concatenate(
        [jnp.sum(dx * xh_ref[...], axis=0, keepdims=True), jnp.sum(dx, axis=0, keepdims=True), jnp.zeros((6, DIM), F32)], axis=0
    )
    for k, pay in enumerate((pay0, pay1, pay2, pay3)):
        pay[0:LOC, :] = dx_v[pl.ds(pl.multiple_of((me ^ k) * LOC, LOC), LOC), :]
        pay[LOC:, :] = gb
    for cp in copies:
        cp.wait()


def embed_kernel(demb_in, dz_ref, x_ref, small_ref, demb_ref, tok_ref, mean_ref, stage, out_sem):
    copies = write_rows(dz_ref, x_ref, demb_ref, stage, out_sem, EARLY_ROWS, EARLY_ROWS, LATE_TILES)
    mask_row = small_ref[2:3, 0:TOK]
    lse = jnp.log(small_ref[0:1, 0:TOK])
    loss = (lse - SOFT_CAP * small_ref[1:2, 0:TOK] + Z_COEF * lse * lse) * mask_row
    mean_ref[...] = row_sum(loss) / row_sum(mask_row)
    tok_ref[...] = pltpu.roll(loss, lax.rem(TOK - lax.axis_index("tp") * LOC, TOK), 1)[:, 0:LOC]
    for cp in copies:
        cp.wait()


def norm_kernel(p0, p1, p2, p3, xh_ref, rstd_ref, gain_in, dhid_ref, gain_ref, bias_ref, gb_v):
    me = lax.axis_index("tp")
    for k, pay in enumerate((p0, p1, p2, p3)):
        gb_v[me ^ k] = pay[LOC:, :]
    gb = gb_v[0] + gb_v[1] + gb_v[2] + gb_v[3]
    gain_ref[...] = gb[0:1, :]
    bias_ref[...] = gb[1:2, :]
    my_rows = pl.ds(pl.multiple_of(me * LOC, LOC), LOC)
    xh = xh_ref[my_rows, :]
    dxh = (p0[0:LOC, :] + p1[0:LOC, :] + p2[0:LOC, :] + p3[0:LOC, :]) * gain_in[3:4, :]
    m1 = row_sum(dxh) * (1.0 / DIM)
    m2 = row_sum(dxh * xh) * (1.0 / DIM)
    dhid_ref[...] = (rstd_ref[my_rows, 0:1] * (dxh - m1 - xh * m2)).astype(BF16)


def solution(mesh):
    vmem = pl.BlockSpec(memory_space=pltpu.VMEM)
    hbm = pl.BlockSpec(memory_space=pltpu.HBM)

    def group_step(hidden, ln_gain, ln_bias, out_embed, vocab_valid, targets, loss_mask):
        shape = jax.ShapeDtypeStruct
        small, xh, rstd, coef, tgt, x_all, g_all, emb = pl.pallas_call(
            main_kernel,
            out_shape=(
                shape((8, DIM), F32), shape((TOK, DIM), F32), shape((TOK, TOK), F32), shape((2, TOK, TOK), F32),
                shape((TOK, TOK), jnp.int32), shape((TOK, DIM), BF16), shape((TOK, VOCAB), F32), shape((VOCAB, DIM), BF16),
            ),
            in_specs=[hbm] * 7,
            out_specs=(vmem,) * 8,
            scratch_shapes=[
                pltpu.VMEM((LOC, DIM), BF16),
                pltpu.VMEM((1, DIM), F32),
                pltpu.VMEM((1, DIM), F32),
                pltpu.VMEM((VOCAB // TOK, TOK), jnp.int32),
                pltpu.VMEM((1, LOC), jnp.int32),
                pltpu.VMEM((1, LOC), jnp.int32),
                pltpu.VMEM((TOK, DIM), BF16),
                pltpu.VMEM((8 * TP, TOK), jnp.int32),
                pltpu.VMEM((8 * TP, TOK), F32),
                pltpu.VMEM((2, TOK, TOK), F32),
                pltpu.VMEM((2, TOK, GROUP), F32),
                pltpu.VMEM((DIM, TURNED), BF16),
                pltpu.SemaphoreType.DMA((GROUPS,)),
                pltpu.SemaphoreType.DMA((9,)),
                pltpu.SemaphoreType.DMA((9,)),
                pltpu.SemaphoreType.DMA((6,)),
            ],
            compiler_params=pltpu.CompilerParams(collective_id=0, has_side_effects=True, vmem_limit_bytes=30 * 1024 * 1024),
            name="main",
        )(
            *(
                pltpu.with_memory_space_constraint(val, pltpu.HBM)
                for val in (
                    hidden, ln_gain.reshape(1, DIM), ln_bias.reshape(1, DIM), out_embed,
                    vocab_valid.reshape(VOCAB // TOK, TOK), targets.reshape(1, LOC), loss_mask.reshape(1, LOC),
                )
            )
        )
        part = shape((LOC + 8, DIM), F32)
        early, dz, *pays = pl.pallas_call(
            grad_kernel,
            out_shape=(shape((VOCAB, DIM), F32), shape((TOK, VOCAB), BF16), part, part, part, part),
            in_specs=[vmem] * 6,
            out_specs=(hbm,) + (vmem,) * 5,
            scratch_shapes=[
                pltpu.VMEM((EARLY_ROWS, DIM), F32), pltpu.VMEM((TOK, DIM), F32), pltpu.SemaphoreType.DMA((len(EARLY_TILES),)),
            ],
            compiler_params=pltpu.CompilerParams(vmem_limit_bytes=16 * 1024 * 1024),
            name="grad",
        )(g_all, emb, x_all, xh, coef, tgt)
        moved = [lax.ppermute(pays[k], "tp", [(i, i ^ k) for i in range(TP)]) for k in range(1, TP)]
        d_embed, tok, mean = pl.pallas_call(
            embed_kernel,
            out_shape=(shape((VOCAB, DIM), F32), shape((1, LOC), F32), shape((1, 1), F32)),
            in_specs=[hbm] + [vmem] * 3,
            out_specs=(hbm, vmem, vmem),
            input_output_aliases={0: 0},
            scratch_shapes=[pltpu.VMEM((VOCAB - EARLY_ROWS, DIM), F32), pltpu.SemaphoreType.DMA((len(LATE_TILES),))],
            compiler_params=pltpu.CompilerParams(vmem_limit_bytes=30 * 1024 * 1024),
            cost_estimate=pl.CostEstimate(flops=2 * TOK * VOCAB * DIM, bytes_accessed=4 * VOCAB * DIM, transcendentals=0),
            name="embed",
        )(early, dz, x_all, small)
        d_hidden, d_gain, d_bias = pl.pallas_call(
            norm_kernel,
            out_shape=(shape((LOC, DIM), BF16), shape((1, DIM), F32), shape((1, DIM), F32)),
            in_specs=[vmem] * 7,
            out_specs=(vmem,) * 3,
            scratch_shapes=[pltpu.VMEM((TP, 8, DIM), F32)],
            compiler_params=pltpu.CompilerParams(vmem_limit_bytes=8 * 1024 * 1024),
            name="norm",
        )(pays[0], *moved, xh, rstd, small)
        return tok.reshape(LOC), mean.reshape(1), d_hidden, d_embed, d_gain.reshape(DIM), d_bias.reshape(DIM)

    row_spec = P(("dp", "tp"))
    mat_spec = P(("dp", "tp"), None)
    return jax.shard_map(
        group_step, mesh=mesh,
        in_specs=(mat_spec, P(None), P(None), P("tp", None), P("tp"), row_spec, row_spec),
        out_specs=(row_spec, P("dp"), mat_spec, mat_spec, P("dp"), P("dp")), check_vma=False,
    )
```

```python
import functools

import jax
import jax.numpy as jnp
from jax import lax
from jax.experimental import pallas as pl
from jax.experimental.pallas import tpu as pltpu
from jax.sharding import PartitionSpec as P

SOFT_CAP = 30.0
Z_COEF = 1e-4
LN_EPS = 1e-5
LOG2E = 1.4426950408889634
MESH = pl.DeviceIdType.MESH
F32 = jnp.float32
BF16 = jnp.bfloat16

TP = 4
TOK = 128
LOC = TOK // TP
DIM = 512
VOCAB = 12672
TILE = 256
GROUP = 7 * TILE
GROUPS = VOCAB // GROUP
TAIL = VOCAB - GROUP * GROUPS
BLK = 32
TURN = 3
TURNED = TURN * GROUP
FWD = [7] * 6 + [4, 2, 2]


def row_sum(val):
    return jnp.sum(val, axis=-1, keepdims=True)


def main_kernel(
    hid_hbm, gain_hbm, bias_hbm, emb_ref, valid_hbm, tgt_hbm, mask_hbm,
    small_ref, xh_v, rstd_v, coef_ref, tgt_v, x_ref, g_v, emb_v,
    hid_ref, gain_ref, bias_ref, valid_ref, tgt_ref, mask_ref,
    hid_all, meta_v, stat_v, acc_v, z_v, embt_v,
    emb_sem, send_sem, recv_sem, in_sem,
):
    me = lax.axis_index("tp")
    dp = lax.axis_index("dp")
    ins = [
        pltpu.make_async_copy(src, dst, in_sem.at[k])
        for k, (src, dst) in enumerate([
            (hid_hbm, hid_ref), (tgt_hbm, tgt_ref), (mask_hbm, mask_ref),
            (gain_hbm, gain_ref), (bias_hbm, bias_ref), (valid_hbm, valid_ref),
        ])
    ]
    for cp in ins:
        cp.start()
    chunks = [(j * GROUP, GROUP) for j in range(GROUPS - 1)]
    chunks.append(((GROUPS - 1) * GROUP, GROUP + TAIL))
    emb_copies = [
        pltpu.make_async_copy(emb_ref.at[pl.ds(s, n), :], emb_v.at[pl.ds(s, n), :], emb_sem.at[k])
        for k, (s, n) in enumerate(chunks)
    ]
    for cp in emb_copies:
        cp.start()

    barrier = pltpu.get_barrier_semaphore()
    for k in range(1, TP):
        pl.semaphore_signal(barrier, inc=1, device_id=(dp, lax.rem(me + k, TP)), device_id_type=MESH)

    for cp in ins[:3]:
        cp.wait()
    lane = lax.broadcasted_iota(jnp.int32, (1, TOK), 1)
    mine = (lane // LOC) == me
    tgt4 = jnp.concatenate([tgt_ref[...]] * TP, axis=1)
    mask4 = jnp.concatenate([mask_ref[...]] * TP, axis=1)
    my_rows = pl.ds(pl.multiple_of(me * LOC, LOC), LOC)
    my_meta = pl.ds(pl.multiple_of(me * 8, 8), 8)
    meta_v[my_meta, :] = jnp.concatenate(
        [jnp.where(mine, tgt4, 0), jnp.where(mine, mask4, 0), jnp.zeros((6, TOK), jnp.int32)], axis=0
    )
    hid_all[my_rows, :] = hid_ref[...]
    pl.semaphore_wait(barrier, TP - 1)

    def push(src, dst, idx):
        copies = []
        for k in range(1, TP):
            cp = pltpu.make_async_remote_copy(
                src_ref=src(k), dst_ref=dst, send_sem=send_sem.at[3 * idx + k - 1], recv_sem=recv_sem.at[3 * idx + k - 1],
                device_id=(dp, lax.rem(me + k, TP)), device_id_type=MESH,
            )
            cp.start()
            copies.append(cp)
        return copies

    first = push(lambda k: hid_ref, hid_all.at[my_rows, :], 0)
    first += push(lambda k: meta_v.at[my_meta, :], meta_v.at[my_meta, :], 1)
    for cp in ins[3:]:
        cp.wait()
    for cp, (g0, n) in zip(emb_copies[:TURN], chunks):
        cp.wait()
        for s in range(g0, g0 + n, TILE):
            embt_v[:, pl.ds(s, TILE)] = jnp.transpose(emb_v[pl.ds(s, TILE), :])
    for cp in first:
        cp.wait_recv()

    meta = meta_v[0:8, :] + meta_v[8:16, :] + meta_v[16:24, :] + meta_v[24:32, :]
    tgt_row = meta[0:1, :]
    mask_row = meta[1:2, :].astype(F32)
    tok_count = row_sum(mask_row)
    tgt_col = jnp.transpose(jnp.broadcast_to(tgt_row, (TOK, TOK)))

    h = hid_all[...].astype(F32)
    mean_val = row_sum(h) * (1.0 / DIM)
    cent = h - mean_val
    var_val = row_sum(cent * cent) * (1.0 / DIM)
    rstd = lax.rsqrt(var_val + LN_EPS)
    xh = cent * rstd
    xh_v[...] = xh
    rstd_v[...] = jnp.broadcast_to(rstd, (TOK, TOK))
    x_ref[...] = (xh * gain_ref[...] + bias_ref[...]).astype(BF16)

    tgt_v[...] = tgt_col - me * VOCAB
    lane_blk = lax.broadcasted_iota(jnp.int32, (BLK, TOK), 1)
    plain = [(s, TILE) for s in range(0, TURNED, TILE)]
    other = [(s, min(TILE, VOCAB - s)) for s in range(TURNED, VOCAB, TILE)]
    tiles = []
    while plain or other:
        if other:
            tiles.append(other.pop(0))
        if plain:
            tiles.append(plain.pop(0))
    groups = []
    for n in FWD:
        groups.append(tiles[:n])
        tiles = tiles[n:]

    def logits(j):
        pos = 0
        for col, w in groups[j]:
            if col < TURNED:
                z = jnp.dot(x_ref[...], embt_v[:, pl.ds(col, w)], preferred_element_type=F32)
            else:
                z = lax.dot_general(
                    x_ref[...], emb_v[pl.ds(col, w), :], (((1,), (1,)), ((), ())), preferred_element_type=F32
                )
            z_v[j % 2, :, pl.ds(pos, w)] = z
            pos += w

    def softmax_pass(j):
        cols = [c for col, w in groups[j] for c in range(col, col + w, TOK)]
        for tb in range(TOK // BLK):
            rows = pl.ds(tb * BLK, BLK)
            tgt = tgt_v[rows, :]
            s_acc = acc_v[0, rows, :]
            t_acc = acc_v[1, rows, :]
            for c, col in enumerate(cols):
                t = jnp.tanh(z_v[j % 2, rows, pl.ds(c * TOK, TOK)] * (1.0 / SOFT_CAP))
                ok = valid_ref[col // TOK:col // TOK + 1, :].astype(F32)
                e = jnp.exp2(t * (SOFT_CAP * LOG2E)) * ok
                s_acc += e
                t_acc += jnp.where(tgt == lane_blk + col, t, 0.0)
                g_v[rows, pl.ds(col, TOK)] = e * (1.0 - t * t)
            acc_v[0, rows, :] = s_acc
            acc_v[1, rows, :] = t_acc

    for cp in emb_copies[TURN:]:
        cp.wait()
    acc_v[...] = jnp.zeros_like(acc_v)
    for j in range(len(groups)):
        logits(j)
        if j > 0:
            softmax_pass(j - 1)
    softmax_pass(len(groups) - 1)

    s_loc = jnp.sum(jnp.transpose(acc_v[0]), axis=0, keepdims=True)
    t_loc = jnp.sum(jnp.transpose(acc_v[1]), axis=0, keepdims=True)
    stat_v[my_meta, :] = jnp.concatenate([s_loc, t_loc, jnp.zeros((6, TOK), F32)], axis=0)
    second = push(lambda k: stat_v.at[my_meta, :], stat_v.at[my_meta, :], 2)
    for cp in second:
        cp.wait_recv()
    stats = stat_v[0:8, :] + stat_v[8:16, :] + stat_v[16:24, :] + stat_v[24:32, :]
    sum_exp = stats[0:1, :]
    t_tgt = stats[1:2, :]
    lse = jnp.log(sum_exp)
    coef = mask_row / tok_count
    a_row = (1.0 + 2.0 * Z_COEF * lse) * coef / sum_exp
    c_row = coef * (1.0 - t_tgt * t_tgt)
    coef_ref[0] = jnp.transpose(jnp.broadcast_to(a_row, (TOK, TOK)))
    coef_ref[1] = jnp.transpose(jnp.broadcast_to(c_row, (TOK, TOK)))
    pad = jnp.zeros((1, DIM - TOK), F32)
    small_ref[...] = jnp.concatenate(
        [jnp.concatenate([row, pad], axis=1) for row in (sum_exp, t_tgt, mask_row)] + [gain_ref[...], jnp.zeros((4, DIM), F32)],
        axis=0,
    )
    for cp in first + second:
        cp.wait_send()


EARLY = 2
EARLY_ROWS = 2688
EARLY_TILES = [256, 640, 896, 896]
HEAD = 256
LATE_TILES = [512] + [768] * 12


def write_rows(dz_ref, x_ref, out_ref, stage, sem, start, first, tiles):
    copies = []
    for k, n in enumerate(tiles):
        rows = pl.ds(start, n)
        local = pl.ds(start - first, n)
        stage[local, :] = lax.dot_general(
            dz_ref[:, rows], x_ref[...], (((0,), (0,)), ((), ())), preferred_element_type=F32
        )
        cp = pltpu.make_async_copy(stage.at[local, :], out_ref.at[rows, :], sem.at[k])
        cp.start(priority=k % 2)
        copies.append(cp)
        start += n
    return copies


def grad_kernel(
    g_ref, emb_ref, x_ref, xh_ref, coef_ref, tgt_ref, demb_ref, dz_ref, head_ref, pay0, pay1, pay2, pay3, stage, dx_v, out_sem
):
    me = lax.axis_index("tp")
    lane_blk = lax.broadcasted_iota(jnp.int32, (BLK, TOK), 1)
    groups = [(j * GROUP, GROUP) for j in range(GROUPS - 1)]
    groups.append(((GROUPS - 1) * GROUP, GROUP + TAIL))

    def logit_grad(g0, n):
        for tb in range(TOK // BLK):
            rows = pl.ds(tb * BLK, BLK)
            tgt = tgt_ref[rows, :]
            a_blk = coef_ref[0, rows, :]
            c_blk = coef_ref[1, rows, :]
            for c in range(n // TOK):
                cols = pl.ds(g0 + c * TOK, TOK)
                hit = tgt == lane_blk + (g0 + c * TOK)
                dz_ref[rows, cols] = (a_blk * g_ref[rows, cols] - jnp.where(hit, c_blk, 0.0)).astype(BF16)

    for g0, n in groups[:EARLY]:
        logit_grad(g0, n)
    copies = write_rows(dz_ref, x_ref, demb_ref, stage, out_sem, 0, 0, EARLY_TILES)
    head_ref[...] = lax.dot_general(
        dz_ref[:, pl.ds(EARLY_ROWS, HEAD)], x_ref[...], (((0,), (0,)), ((), ())), preferred_element_type=F32
    )
    dx = 0.0
    for j, (g0, n) in enumerate(groups):
        if j >= EARLY:
            logit_grad(g0, n)
        dx += jnp.dot(dz_ref[:, pl.ds(g0, n)], emb_ref[pl.ds(g0, n), :], preferred_element_type=F32)
    dx_v[...] = dx
    gb = jnp.concatenate(
        [jnp.sum(dx * xh_ref[...], axis=0, keepdims=True), jnp.sum(dx, axis=0, keepdims=True), jnp.zeros((6, DIM), F32)], axis=0
    )
    for k, pay in enumerate((pay0, pay1, pay2, pay3)):
        pay[0:LOC, :] = dx_v[pl.ds(pl.multiple_of((me ^ k) * LOC, LOC), LOC), :]
        pay[LOC:, :] = gb
    for cp in copies:
        cp.wait()


def embed_kernel(demb_in, dz_ref, head_ref, x_ref, small_ref, demb_ref, tok_ref, mean_ref, stage, out_sem, head_sem):
    head = pltpu.make_async_copy(head_ref, demb_ref.at[pl.ds(EARLY_ROWS, HEAD), :], head_sem)
    head.start()
    copies = write_rows(dz_ref, x_ref, demb_ref, stage, out_sem, EARLY_ROWS + HEAD, EARLY_ROWS + HEAD, LATE_TILES)
    copies.append(head)
    mask_row = small_ref[2:3, 0:TOK]
    lse = jnp.log(small_ref[0:1, 0:TOK])
    loss = (lse - SOFT_CAP * small_ref[1:2, 0:TOK] + Z_COEF * lse * lse) * mask_row
    mean_ref[...] = row_sum(loss) / row_sum(mask_row)
    tok_ref[...] = pltpu.roll(loss, lax.rem(TOK - lax.axis_index("tp") * LOC, TOK), 1)[:, 0:LOC]
    for cp in copies:
        cp.wait()


def norm_kernel(p0, p1, p2, p3, xh_ref, rstd_ref, gain_in, dhid_ref, gain_ref, bias_ref, gb_v):
    me = lax.axis_index("tp")
    for k, pay in enumerate((p0, p1, p2, p3)):
        gb_v[me ^ k] = pay[LOC:, :]
    gb = gb_v[0] + gb_v[1] + gb_v[2] + gb_v[3]
    gain_ref[...] = gb[0:1, :]
    bias_ref[...] = gb[1:2, :]
    my_rows = pl.ds(pl.multiple_of(me * LOC, LOC), LOC)
    xh = xh_ref[my_rows, :]
    dxh = (p0[0:LOC, :] + p1[0:LOC, :] + p2[0:LOC, :] + p3[0:LOC, :]) * gain_in[3:4, :]
    m1 = row_sum(dxh) * (1.0 / DIM)
    m2 = row_sum(dxh * xh) * (1.0 / DIM)
    dhid_ref[...] = (rstd_ref[my_rows, 0:1] * (dxh - m1 - xh * m2)).astype(BF16)


def solution(mesh):
    vmem = pl.BlockSpec(memory_space=pltpu.VMEM)
    hbm = pl.BlockSpec(memory_space=pltpu.HBM)

    def group_step(hidden, ln_gain, ln_bias, out_embed, vocab_valid, targets, loss_mask):
        shape = jax.ShapeDtypeStruct
        small, xh, rstd, coef, tgt, x_all, g_all, emb = pl.pallas_call(
            main_kernel,
            out_shape=(
                shape((8, DIM), F32), shape((TOK, DIM), F32), shape((TOK, TOK), F32), shape((2, TOK, TOK), F32),
                shape((TOK, TOK), jnp.int32), shape((TOK, DIM), BF16), shape((TOK, VOCAB), F32), shape((VOCAB, DIM), BF16),
            ),
            in_specs=[hbm] * 7,
            out_specs=(vmem,) * 8,
            scratch_shapes=[
                pltpu.VMEM((LOC, DIM), BF16),
                pltpu.VMEM((1, DIM), F32),
                pltpu.VMEM((1, DIM), F32),
                pltpu.VMEM((VOCAB // TOK, TOK), jnp.int32),
                pltpu.VMEM((1, LOC), jnp.int32),
                pltpu.VMEM((1, LOC), jnp.int32),
                pltpu.VMEM((TOK, DIM), BF16),
                pltpu.VMEM((8 * TP, TOK), jnp.int32),
                pltpu.VMEM((8 * TP, TOK), F32),
                pltpu.VMEM((2, TOK, TOK), F32),
                pltpu.VMEM((2, TOK, GROUP), F32),
                pltpu.VMEM((DIM, TURNED), BF16),
                pltpu.SemaphoreType.DMA((GROUPS,)),
                pltpu.SemaphoreType.DMA((9,)),
                pltpu.SemaphoreType.DMA((9,)),
                pltpu.SemaphoreType.DMA((6,)),
            ],
            compiler_params=pltpu.CompilerParams(collective_id=0, has_side_effects=True, vmem_limit_bytes=30 * 1024 * 1024),
            name="main",
        )(
            *(
                pltpu.with_memory_space_constraint(val, pltpu.HBM)
                for val in (
                    hidden, ln_gain.reshape(1, DIM), ln_bias.reshape(1, DIM), out_embed,
                    vocab_valid.reshape(VOCAB // TOK, TOK), targets.reshape(1, LOC), loss_mask.reshape(1, LOC),
                )
            )
        )
        part = shape((LOC + 8, DIM), F32)
        early, dz, head, *pays = pl.pallas_call(
            grad_kernel,
            out_shape=(shape((VOCAB, DIM), F32), shape((TOK, VOCAB), BF16), shape((HEAD, DIM), F32), part, part, part, part),
            in_specs=[vmem] * 6,
            out_specs=(hbm,) + (vmem,) * 6,
            scratch_shapes=[
                pltpu.VMEM((EARLY_ROWS, DIM), F32), pltpu.VMEM((TOK, DIM), F32), pltpu.SemaphoreType.DMA((len(EARLY_TILES),)),
            ],
            compiler_params=pltpu.CompilerParams(vmem_limit_bytes=16 * 1024 * 1024),
            name="grad",
        )(g_all, emb, x_all, xh, coef, tgt)
        moved = [lax.ppermute(pays[k], "tp", [(i, i ^ k) for i in range(TP)]) for k in range(1, TP)]
        d_embed, tok, mean = pl.pallas_call(
            embed_kernel,
            out_shape=(shape((VOCAB, DIM), F32), shape((1, LOC), F32), shape((1, 1), F32)),
            in_specs=[hbm] + [vmem] * 4,
            out_specs=(hbm, vmem, vmem),
            input_output_aliases={0: 0},
            scratch_shapes=[
                pltpu.VMEM((VOCAB - EARLY_ROWS - HEAD, DIM), F32), pltpu.SemaphoreType.DMA((len(LATE_TILES),)), pltpu.SemaphoreType.DMA,
            ],
            compiler_params=pltpu.CompilerParams(vmem_limit_bytes=30 * 1024 * 1024),
            cost_estimate=pl.CostEstimate(flops=2 * TOK * VOCAB * DIM, bytes_accessed=4 * VOCAB * DIM, transcendentals=0),
            name="embed",
        )(early, dz, head, x_all, small)
        d_hidden, d_gain, d_bias = pl.pallas_call(
            norm_kernel,
            out_shape=(shape((LOC, DIM), BF16), shape((1, DIM), F32), shape((1, DIM), F32)),
            in_specs=[vmem] * 7,
            out_specs=(vmem,) * 3,
            scratch_shapes=[pltpu.VMEM((TP, 8, DIM), F32)],
            compiler_params=pltpu.CompilerParams(vmem_limit_bytes=8 * 1024 * 1024),
            name="norm",
        )(pays[0], *moved, xh, rstd, small)
        return tok.reshape(LOC), mean.reshape(1), d_hidden, d_embed, d_gain.reshape(DIM), d_bias.reshape(DIM)

    row_spec = P(("dp", "tp"))
    mat_spec = P(("dp", "tp"), None)
    return jax.shard_map(
        group_step, mesh=mesh,
        in_specs=(mat_spec, P(None), P(None), P("tp", None), P("tp"), row_spec, row_spec),
        out_specs=(row_spec, P("dp"), mat_spec, mat_spec, P("dp"), P("dp")), check_vma=False,
    )
```

```python
import functools

import jax
import jax.numpy as jnp
from jax import lax
from jax.experimental import pallas as pl
from jax.experimental.pallas import tpu as pltpu
from jax.sharding import PartitionSpec as P

SOFT_CAP = 30.0
Z_COEF = 1e-4
LN_EPS = 1e-5
LOG2E = 1.4426950408889634
MESH = pl.DeviceIdType.MESH
F32 = jnp.float32
BF16 = jnp.bfloat16

TP = 4
TOK = 128
LOC = TOK // TP
DIM = 512
VOCAB = 12672
TILE = 256
GROUP = 7 * TILE
GROUPS = VOCAB // GROUP
TAIL = VOCAB - GROUP * GROUPS
BLK = 32
TURN = 3
TURNED = TURN * GROUP
FWD = [7] * 6 + [4, 2, 2]


def row_sum(val):
    return jnp.sum(val, axis=-1, keepdims=True)


def main_kernel(
    hid_hbm, gain_hbm, bias_hbm, emb_ref, valid_hbm, tgt_hbm, mask_hbm,
    small_ref, xh_v, rstd_v, coef_ref, tgt_v, x_ref, g_v, emb_v,
    hid_ref, gain_ref, bias_ref, valid_ref, tgt_ref, mask_ref,
    hid_all, meta_v, stat_v, acc_v, z_v, embt_v,
    emb_sem, send_sem, recv_sem, in_sem,
):
    me = lax.axis_index("tp")
    dp = lax.axis_index("dp")
    ins = [
        pltpu.make_async_copy(src, dst, in_sem.at[k])
        for k, (src, dst) in enumerate([
            (hid_hbm, hid_ref), (tgt_hbm, tgt_ref), (mask_hbm, mask_ref),
            (gain_hbm, gain_ref), (bias_hbm, bias_ref), (valid_hbm, valid_ref),
        ])
    ]
    for cp in ins:
        cp.start()
    chunks = [(j * GROUP, GROUP) for j in range(GROUPS - 1)]
    chunks.append(((GROUPS - 1) * GROUP, GROUP + TAIL))
    emb_copies = [
        pltpu.make_async_copy(emb_ref.at[pl.ds(s, n), :], emb_v.at[pl.ds(s, n), :], emb_sem.at[k])
        for k, (s, n) in enumerate(chunks)
    ]
    for cp in emb_copies:
        cp.start()

    barrier = pltpu.get_barrier_semaphore()
    for k in range(1, TP):
        pl.semaphore_signal(barrier, inc=1, device_id=(dp, lax.rem(me + k, TP)), device_id_type=MESH)

    for cp in ins[:3]:
        cp.wait()
    lane = lax.broadcasted_iota(jnp.int32, (1, TOK), 1)
    mine = (lane // LOC) == me
    tgt4 = jnp.concatenate([tgt_ref[...]] * TP, axis=1)
    mask4 = jnp.concatenate([mask_ref[...]] * TP, axis=1)
    my_rows = pl.ds(pl.multiple_of(me * LOC, LOC), LOC)
    my_meta = pl.ds(pl.multiple_of(me * 8, 8), 8)
    meta_v[my_meta, :] = jnp.concatenate(
        [jnp.where(mine, tgt4, 0), jnp.where(mine, mask4, 0), jnp.zeros((6, TOK), jnp.int32)], axis=0
    )
    hid_all[my_rows, :] = hid_ref[...]
    pl.semaphore_wait(barrier, TP - 1)

    def push(src, dst, idx):
        copies = []
        for k in range(1, TP):
            cp = pltpu.make_async_remote_copy(
                src_ref=src(k), dst_ref=dst, send_sem=send_sem.at[3 * idx + k - 1], recv_sem=recv_sem.at[3 * idx + k - 1],
                device_id=(dp, lax.rem(me + k, TP)), device_id_type=MESH,
            )
            cp.start()
            copies.append(cp)
        return copies

    first = push(lambda k: hid_ref, hid_all.at[my_rows, :], 0)
    first += push(lambda k: meta_v.at[my_meta, :], meta_v.at[my_meta, :], 1)
    for cp in ins[3:]:
        cp.wait()
    for cp, (g0, n) in zip(emb_copies[:TURN], chunks):
        cp.wait()
        for s in range(g0, g0 + n, TILE):
            embt_v[:, pl.ds(s, TILE)] = jnp.transpose(emb_v[pl.ds(s, TILE), :])
    for cp in first:
        cp.wait_recv()

    meta = meta_v[0:8, :] + meta_v[8:16, :] + meta_v[16:24, :] + meta_v[24:32, :]
    tgt_row = meta[0:1, :]
    mask_row = meta[1:2, :].astype(F32)
    tok_count = row_sum(mask_row)
    tgt_col = jnp.transpose(jnp.broadcast_to(tgt_row, (TOK, TOK)))

    h = hid_all[...].astype(F32)
    mean_val = row_sum(h) * (1.0 / DIM)
    cent = h - mean_val
    var_val = row_sum(cent * cent) * (1.0 / DIM)
    rstd = lax.rsqrt(var_val + LN_EPS)
    xh = cent * rstd
    xh_v[...] = xh
    rstd_v[...] = jnp.broadcast_to(rstd, (TOK, TOK))
    x_ref[...] = (xh * gain_ref[...] + bias_ref[...]).astype(BF16)

    tgt_v[...] = tgt_col - me * VOCAB
    lane_blk = lax.broadcasted_iota(jnp.int32, (BLK, TOK), 1)
    plain = [(s, TILE) for s in range(0, TURNED, TILE)]
    other = [(s, min(TILE, VOCAB - s)) for s in range(TURNED, VOCAB, TILE)]
    tiles = []
    while plain or other:
        if other:
            tiles.append(other.pop(0))
        if plain:
            tiles.append(plain.pop(0))
    groups = []
    for n in FWD:
        groups.append(tiles[:n])
        tiles = tiles[n:]

    def logits(j):
        pos = 0
        for col, w in groups[j]:
            if col < TURNED:
                z = jnp.dot(x_ref[...], embt_v[:, pl.ds(col, w)], preferred_element_type=F32)
            else:
                z = lax.dot_general(
                    x_ref[...], emb_v[pl.ds(col, w), :], (((1,), (1,)), ((), ())), preferred_element_type=F32
                )
            z_v[j % 2, :, pl.ds(pos, w)] = z
            pos += w

    def softmax_pass(j):
        cols = [c for col, w in groups[j] for c in range(col, col + w, TOK)]
        for tb in range(TOK // BLK):
            rows = pl.ds(tb * BLK, BLK)
            tgt = tgt_v[rows, :]
            s_acc = acc_v[0, rows, :]
            t_acc = acc_v[1, rows, :]
            for c, col in enumerate(cols):
                t = jnp.tanh(z_v[j % 2, rows, pl.ds(c * TOK, TOK)] * (1.0 / SOFT_CAP))
                ok = valid_ref[col // TOK:col // TOK + 1, :].astype(F32)
                e = jnp.exp2(t * (SOFT_CAP * LOG2E)) * ok
                s_acc += e
                t_acc += jnp.where(tgt == lane_blk + col, t, 0.0)
                g_v[rows, pl.ds(col, TOK)] = e * (1.0 - t * t)
            acc_v[0, rows, :] = s_acc
            acc_v[1, rows, :] = t_acc

    for cp in emb_copies[TURN:]:
        cp.wait()
    acc_v[...] = jnp.zeros_like(acc_v)
    for j in range(len(groups)):
        logits(j)
        if j > 0:
            softmax_pass(j - 1)
    softmax_pass(len(groups) - 1)

    s_loc = jnp.sum(jnp.transpose(acc_v[0]), axis=0, keepdims=True)
    t_loc = jnp.sum(jnp.transpose(acc_v[1]), axis=0, keepdims=True)
    stat_v[my_meta, :] = jnp.concatenate([s_loc, t_loc, jnp.zeros((6, TOK), F32)], axis=0)
    second = push(lambda k: stat_v.at[my_meta, :], stat_v.at[my_meta, :], 2)
    for cp in second:
        cp.wait_recv()
    stats = stat_v[0:8, :] + stat_v[8:16, :] + stat_v[16:24, :] + stat_v[24:32, :]
    sum_exp = stats[0:1, :]
    t_tgt = stats[1:2, :]
    lse = jnp.log(sum_exp)
    coef = mask_row / tok_count
    a_row = (1.0 + 2.0 * Z_COEF * lse) * coef / sum_exp
    c_row = coef * (1.0 - t_tgt * t_tgt)
    coef_ref[0] = jnp.transpose(jnp.broadcast_to(a_row, (TOK, TOK)))
    coef_ref[1] = jnp.transpose(jnp.broadcast_to(c_row, (TOK, TOK)))
    pad = jnp.zeros((1, DIM - TOK), F32)
    small_ref[...] = jnp.concatenate(
        [jnp.concatenate([row, pad], axis=1) for row in (sum_exp, t_tgt, mask_row)] + [gain_ref[...], jnp.zeros((4, DIM), F32)],
        axis=0,
    )
    for cp in first + second:
        cp.wait_send()


EARLY = 2
EARLY_ROWS = 2688
EARLY_TILES = [256, 640, 896, 896]
HEAD = 256
LATE_TILES = [512] + [768] * 12


def write_rows(dz_ref, x_ref, out_ref, stage, sem, start, first, tiles):
    copies = []
    for k, n in enumerate(tiles):
        rows = pl.ds(start, n)
        local = pl.ds(start - first, n)
        stage[local, :] = lax.dot_general(
            dz_ref[:, rows], x_ref[...], (((0,), (0,)), ((), ())), preferred_element_type=F32
        )
        cp = pltpu.make_async_copy(stage.at[local, :], out_ref.at[rows, :], sem.at[k])
        cp.start(priority=k % 2)
        copies.append(cp)
        start += n
    return copies


def grad_kernel(
    g_ref, emb_ref, x_ref, xh_ref, coef_ref, tgt_ref, demb_ref, dz_ref, head_ref, pay0, pay1, pay2, pay3, stage, dx_v, out_sem
):
    me = lax.axis_index("tp")
    lane_blk = lax.broadcasted_iota(jnp.int32, (BLK, TOK), 1)
    groups = [(j * GROUP, GROUP) for j in range(GROUPS - 1)]
    groups.append(((GROUPS - 1) * GROUP, GROUP + TAIL))

    def logit_grad(g0, n):
        for tb in range(TOK // BLK):
            rows = pl.ds(tb * BLK, BLK)
            tgt = tgt_ref[rows, :]
            a_blk = coef_ref[0, rows, :]
            c_blk = coef_ref[1, rows, :]
            for c in range(n // TOK):
                cols = pl.ds(g0 + c * TOK, TOK)
                hit = tgt == lane_blk + (g0 + c * TOK)
                dz_ref[rows, cols] = (a_blk * g_ref[rows, cols] - jnp.where(hit, c_blk, 0.0)).astype(BF16)

    for g0, n in groups[:EARLY]:
        logit_grad(g0, n)
    copies = write_rows(dz_ref, x_ref, demb_ref, stage, out_sem, 0, 0, EARLY_TILES)
    head_ref[...] = lax.dot_general(
        dz_ref[:, pl.ds(EARLY_ROWS, HEAD)], x_ref[...], (((0,), (0,)), ((), ())), preferred_element_type=F32
    )
    dx = 0.0
    for j, (g0, n) in enumerate(groups):
        if j >= EARLY:
            logit_grad(g0, n)
        dx += jnp.dot(dz_ref[:, pl.ds(g0, n)], emb_ref[pl.ds(g0, n), :], preferred_element_type=F32)
    dx_v[...] = dx
    gb = jnp.concatenate(
        [jnp.sum(dx * xh_ref[...], axis=0, keepdims=True), jnp.sum(dx, axis=0, keepdims=True), jnp.zeros((6, DIM), F32)], axis=0
    )
    for k, pay in enumerate((pay0, pay1, pay2, pay3)):
        pay[0:LOC, :] = dx_v[pl.ds(pl.multiple_of((me ^ k) * LOC, LOC), LOC), :]
        pay[LOC:, :] = gb
    for cp in copies:
        cp.wait()


def embed_kernel(
    demb_in, dz_ref, head_ref, x_ref, small_ref, demb_ref, tok_ref, mean_ref, stage, tok_v, mean_v, out_sem, side_sem
):
    sides = [
        pltpu.make_async_copy(src, dst, side_sem.at[k])
        for k, (src, dst) in enumerate([
            (head_ref, demb_ref.at[pl.ds(EARLY_ROWS, HEAD), :]), (tok_v, tok_ref), (mean_v, mean_ref),
        ])
    ]
    sides[0].start()
    copies = write_rows(dz_ref, x_ref, demb_ref, stage, out_sem, EARLY_ROWS + HEAD, EARLY_ROWS + HEAD, LATE_TILES)
    mask_row = small_ref[2:3, 0:TOK]
    lse = jnp.log(small_ref[0:1, 0:TOK])
    loss = (lse - SOFT_CAP * small_ref[1:2, 0:TOK] + Z_COEF * lse * lse) * mask_row
    mean_v[...] = row_sum(loss) / row_sum(mask_row)
    tok_v[...] = pltpu.roll(loss, lax.rem(TOK - lax.axis_index("tp") * LOC, TOK), 1)[:, 0:LOC]
    for cp in sides[1:]:
        cp.start()
    for cp in copies + sides:
        cp.wait()


def norm_kernel(p0, p1, p2, p3, xh_ref, rstd_ref, gain_in, dhid_ref, gain_ref, bias_ref, gb_v):
    me = lax.axis_index("tp")
    for k, pay in enumerate((p0, p1, p2, p3)):
        gb_v[me ^ k] = pay[LOC:, :]
    gb = gb_v[0] + gb_v[1] + gb_v[2] + gb_v[3]
    gain_ref[...] = gb[0:1, :]
    bias_ref[...] = gb[1:2, :]
    my_rows = pl.ds(pl.multiple_of(me * LOC, LOC), LOC)
    xh = xh_ref[my_rows, :]
    dxh = (p0[0:LOC, :] + p1[0:LOC, :] + p2[0:LOC, :] + p3[0:LOC, :]) * gain_in[3:4, :]
    m1 = row_sum(dxh) * (1.0 / DIM)
    m2 = row_sum(dxh * xh) * (1.0 / DIM)
    dhid_ref[...] = (rstd_ref[my_rows, 0:1] * (dxh - m1 - xh * m2)).astype(BF16)


def solution(mesh):
    vmem = pl.BlockSpec(memory_space=pltpu.VMEM)
    hbm = pl.BlockSpec(memory_space=pltpu.HBM)

    def group_step(hidden, ln_gain, ln_bias, out_embed, vocab_valid, targets, loss_mask):
        shape = jax.ShapeDtypeStruct
        small, xh, rstd, coef, tgt, x_all, g_all, emb = pl.pallas_call(
            main_kernel,
            out_shape=(
                shape((8, DIM), F32), shape((TOK, DIM), F32), shape((TOK, TOK), F32), shape((2, TOK, TOK), F32),
                shape((TOK, TOK), jnp.int32), shape((TOK, DIM), BF16), shape((TOK, VOCAB), F32), shape((VOCAB, DIM), BF16),
            ),
            in_specs=[hbm] * 7,
            out_specs=(vmem,) * 8,
            scratch_shapes=[
                pltpu.VMEM((LOC, DIM), BF16),
                pltpu.VMEM((1, DIM), F32),
                pltpu.VMEM((1, DIM), F32),
                pltpu.VMEM((VOCAB // TOK, TOK), jnp.int32),
                pltpu.VMEM((1, LOC), jnp.int32),
                pltpu.VMEM((1, LOC), jnp.int32),
                pltpu.VMEM((TOK, DIM), BF16),
                pltpu.VMEM((8 * TP, TOK), jnp.int32),
                pltpu.VMEM((8 * TP, TOK), F32),
                pltpu.VMEM((2, TOK, TOK), F32),
                pltpu.VMEM((2, TOK, GROUP), F32),
                pltpu.VMEM((DIM, TURNED), BF16),
                pltpu.SemaphoreType.DMA((GROUPS,)),
                pltpu.SemaphoreType.DMA((9,)),
                pltpu.SemaphoreType.DMA((9,)),
                pltpu.SemaphoreType.DMA((6,)),
            ],
            compiler_params=pltpu.CompilerParams(collective_id=0, has_side_effects=True, vmem_limit_bytes=30 * 1024 * 1024),
            name="main",
        )(
            *(
                pltpu.with_memory_space_constraint(val, pltpu.HBM)
                for val in (
                    hidden, ln_gain.reshape(1, DIM), ln_bias.reshape(1, DIM), out_embed,
                    vocab_valid.reshape(VOCAB // TOK, TOK), targets.reshape(1, LOC), loss_mask.reshape(1, LOC),
                )
            )
        )
        part = shape((LOC + 8, DIM), F32)
        early, dz, head, *pays = pl.pallas_call(
            grad_kernel,
            out_shape=(shape((VOCAB, DIM), F32), shape((TOK, VOCAB), BF16), shape((HEAD, DIM), F32), part, part, part, part),
            in_specs=[vmem] * 6,
            out_specs=(hbm,) + (vmem,) * 6,
            scratch_shapes=[
                pltpu.VMEM((EARLY_ROWS, DIM), F32), pltpu.VMEM((TOK, DIM), F32), pltpu.SemaphoreType.DMA((len(EARLY_TILES),)),
            ],
            compiler_params=pltpu.CompilerParams(vmem_limit_bytes=16 * 1024 * 1024),
            name="grad",
        )(g_all, emb, x_all, xh, coef, tgt)
        moved = [lax.ppermute(pays[k], "tp", [(i, i ^ k) for i in range(TP)]) for k in range(1, TP)]
        d_embed, tok, mean = pl.pallas_call(
            embed_kernel,
            out_shape=(shape((VOCAB, DIM), F32), shape((1, LOC), F32), shape((1, 1), F32)),
            in_specs=[hbm] + [vmem] * 4,
            out_specs=(hbm, hbm, hbm),
            input_output_aliases={0: 0},
            scratch_shapes=[
                pltpu.VMEM((VOCAB - EARLY_ROWS - HEAD, DIM), F32), pltpu.VMEM((1, LOC), F32), pltpu.VMEM((1, 1), F32),
                pltpu.SemaphoreType.DMA((len(LATE_TILES),)), pltpu.SemaphoreType.DMA((3,)),
            ],
            compiler_params=pltpu.CompilerParams(vmem_limit_bytes=30 * 1024 * 1024),
            cost_estimate=pl.CostEstimate(flops=2 * TOK * VOCAB * DIM, bytes_accessed=4 * VOCAB * DIM, transcendentals=0),
            name="embed",
        )(early, dz, head, x_all, small)
        d_hidden, d_gain, d_bias = pl.pallas_call(
            norm_kernel,
            out_shape=(shape((LOC, DIM), BF16), shape((1, DIM), F32), shape((1, DIM), F32)),
            in_specs=[vmem] * 7,
            out_specs=(vmem,) * 3,
            scratch_shapes=[pltpu.VMEM((TP, 8, DIM), F32)],
            compiler_params=pltpu.CompilerParams(vmem_limit_bytes=8 * 1024 * 1024),
            name="norm",
        )(pays[0], *moved, xh, rstd, small)
        return tok.reshape(LOC), mean.reshape(1), d_hidden, d_embed, d_gain.reshape(DIM), d_bias.reshape(DIM)

    row_spec = P(("dp", "tp"))
    mat_spec = P(("dp", "tp"), None)
    return jax.shard_map(
        group_step, mesh=mesh,
        in_specs=(mat_spec, P(None), P(None), P("tp", None), P("tp"), row_spec, row_spec),
        out_specs=(row_spec, P("dp"), mat_spec, mat_spec, P("dp"), P("dp")), check_vma=False,
    )
```

```python
import functools

import jax
import jax.numpy as jnp
from jax import lax
from jax.experimental import pallas as pl
from jax.experimental.pallas import tpu as pltpu
from jax.sharding import PartitionSpec as P

SOFT_CAP = 30.0
Z_COEF = 1e-4
LN_EPS = 1e-5
LOG2E = 1.4426950408889634
MESH = pl.DeviceIdType.MESH
F32 = jnp.float32
BF16 = jnp.bfloat16

TP = 4
TOK = 128
LOC = TOK // TP
DIM = 512
VOCAB = 12672
TILE = 256
GROUP = 7 * TILE
GROUPS = VOCAB // GROUP
TAIL = VOCAB - GROUP * GROUPS
BLK = 32
TURN = 3
TURNED = TURN * GROUP
FWD = [7] * 6 + [4, 2, 2]


def row_sum(val):
    return jnp.sum(val, axis=-1, keepdims=True)


def main_kernel(
    hid_hbm, gain_hbm, bias_hbm, emb_ref, valid_hbm, tgt_hbm, mask_hbm,
    small_ref, xh_v, rstd_v, coef_ref, tgt_v, x_ref, g_v, emb_v,
    hid_ref, gain_ref, bias_ref, valid_ref, tgt_ref, mask_ref,
    hid_all, meta_v, stat_v, acc_v, z_v, embt_v, ok_v,
    emb_sem, send_sem, recv_sem, in_sem,
):
    me = lax.axis_index("tp")
    dp = lax.axis_index("dp")
    ins = [
        pltpu.make_async_copy(src, dst, in_sem.at[k])
        for k, (src, dst) in enumerate([
            (hid_hbm, hid_ref), (tgt_hbm, tgt_ref), (mask_hbm, mask_ref),
            (gain_hbm, gain_ref), (bias_hbm, bias_ref), (valid_hbm, valid_ref),
        ])
    ]
    for cp in ins:
        cp.start()
    chunks = [(j * GROUP, GROUP) for j in range(GROUPS - 1)]
    chunks.append(((GROUPS - 1) * GROUP, GROUP + TAIL))
    emb_copies = [
        pltpu.make_async_copy(emb_ref.at[pl.ds(s, n), :], emb_v.at[pl.ds(s, n), :], emb_sem.at[k])
        for k, (s, n) in enumerate(chunks)
    ]
    for cp in emb_copies:
        cp.start()

    barrier = pltpu.get_barrier_semaphore()
    for k in range(1, TP):
        pl.semaphore_signal(barrier, inc=1, device_id=(dp, lax.rem(me + k, TP)), device_id_type=MESH)

    for cp in ins[:3]:
        cp.wait()
    lane = lax.broadcasted_iota(jnp.int32, (1, TOK), 1)
    mine = (lane // LOC) == me
    tgt4 = jnp.concatenate([tgt_ref[...]] * TP, axis=1)
    mask4 = jnp.concatenate([mask_ref[...]] * TP, axis=1)
    my_rows = pl.ds(pl.multiple_of(me * LOC, LOC), LOC)
    my_meta = pl.ds(pl.multiple_of(me * 8, 8), 8)
    meta_v[my_meta, :] = jnp.concatenate(
        [jnp.where(mine, tgt4, 0), jnp.where(mine, mask4, 0), jnp.zeros((6, TOK), jnp.int32)], axis=0
    )
    hid_all[my_rows, :] = hid_ref[...]
    pl.semaphore_wait(barrier, TP - 1)

    def push(src, dst, idx):
        copies = []
        for k in range(1, TP):
            cp = pltpu.make_async_remote_copy(
                src_ref=src(k), dst_ref=dst, send_sem=send_sem.at[3 * idx + k - 1], recv_sem=recv_sem.at[3 * idx + k - 1],
                device_id=(dp, lax.rem(me + k, TP)), device_id_type=MESH,
            )
            cp.start()
            copies.append(cp)
        return copies

    first = push(lambda k: hid_ref, hid_all.at[my_rows, :], 0)
    first += push(lambda k: meta_v.at[my_meta, :], meta_v.at[my_meta, :], 1)
    for cp in ins[3:]:
        cp.wait()
    ok_v[...] = valid_ref[...].astype(F32)
    for cp, (g0, n) in zip(emb_copies[:TURN], chunks):
        cp.wait()
        for s in range(g0, g0 + n, TILE):
            embt_v[:, pl.ds(s, TILE)] = jnp.transpose(emb_v[pl.ds(s, TILE), :])
    for cp in first:
        cp.wait_recv()

    meta = meta_v[0:8, :] + meta_v[8:16, :] + meta_v[16:24, :] + meta_v[24:32, :]
    tgt_row = meta[0:1, :]
    mask_row = meta[1:2, :].astype(F32)
    tok_count = row_sum(mask_row)
    tgt_col = jnp.transpose(jnp.broadcast_to(tgt_row, (TOK, TOK)))

    h = hid_all[...].astype(F32)
    mean_val = row_sum(h) * (1.0 / DIM)
    cent = h - mean_val
    var_val = row_sum(cent * cent) * (1.0 / DIM)
    rstd = lax.rsqrt(var_val + LN_EPS)
    xh = cent * rstd
    xh_v[...] = xh
    rstd_v[...] = jnp.broadcast_to(rstd, (TOK, TOK))
    x_ref[...] = (xh * gain_ref[...] + bias_ref[...]).astype(BF16)

    tgt_v[...] = tgt_col - me * VOCAB
    lane_blk = lax.broadcasted_iota(jnp.int32, (BLK, TOK), 1)
    plain = [(s, TILE) for s in range(0, TURNED, TILE)]
    other = [(s, min(TILE, VOCAB - s)) for s in range(TURNED, VOCAB, TILE)]
    tiles = []
    while plain or other:
        if other:
            tiles.append(other.pop(0))
        if plain:
            tiles.append(plain.pop(0))
    groups = []
    for n in FWD:
        groups.append(tiles[:n])
        tiles = tiles[n:]

    def logits(j):
        pos = 0
        for col, w in groups[j]:
            if col < TURNED:
                z = jnp.dot(x_ref[...], embt_v[:, pl.ds(col, w)], preferred_element_type=F32)
            else:
                z = lax.dot_general(
                    x_ref[...], emb_v[pl.ds(col, w), :], (((1,), (1,)), ((), ())), preferred_element_type=F32
                )
            z_v[j % 2, :, pl.ds(pos, w)] = z
            pos += w

    def softmax_pass(j):
        cols = [c for col, w in groups[j] for c in range(col, col + w, TOK)]
        for tb in range(TOK // BLK):
            rows = pl.ds(tb * BLK, BLK)
            tgt = tgt_v[rows, :]
            s_acc = acc_v[0, rows, :]
            t_acc = acc_v[1, rows, :]
            for first_c in range(0, len(cols), 2):
                pick = 0.0
                for c in range(first_c, min(first_c + 2, len(cols))):
                    col = cols[c]
                    t = jnp.tanh(z_v[j % 2, rows, pl.ds(c * TOK, TOK)] * (1.0 / SOFT_CAP))
                    e = jnp.exp2(t * (SOFT_CAP * LOG2E)) * ok_v[col // TOK:col // TOK + 1, :]
                    pick = jnp.where(tgt == lane_blk + col, t, pick)
                    g_v[rows, pl.ds(col, TOK)] = e * (1.0 - t * t)
                    s_acc += e
                t_acc += pick
            acc_v[0, rows, :] = s_acc
            acc_v[1, rows, :] = t_acc

    for cp in emb_copies[TURN:]:
        cp.wait()
    acc_v[...] = jnp.zeros_like(acc_v)
    for j in range(len(groups)):
        logits(j)
        if j > 0:
            softmax_pass(j - 1)
    softmax_pass(len(groups) - 1)

    s_loc = jnp.sum(jnp.transpose(acc_v[0]), axis=0, keepdims=True)
    t_loc = jnp.sum(jnp.transpose(acc_v[1]), axis=0, keepdims=True)
    stat_v[my_meta, :] = jnp.concatenate([s_loc, t_loc, jnp.zeros((6, TOK), F32)], axis=0)
    second = push(lambda k: stat_v.at[my_meta, :], stat_v.at[my_meta, :], 2)
    for cp in first:
        cp.wait_send()
    for cp in second:
        cp.wait_recv()
    stats = stat_v[0:8, :] + stat_v[8:16, :] + stat_v[16:24, :] + stat_v[24:32, :]
    sum_exp = stats[0:1, :]
    t_tgt = stats[1:2, :]
    lse = jnp.log(sum_exp)
    coef = mask_row / tok_count
    a_row = (1.0 + 2.0 * Z_COEF * lse) * coef / sum_exp
    c_row = coef * (1.0 - t_tgt * t_tgt)
    coef_ref[0] = jnp.transpose(jnp.broadcast_to(a_row, (TOK, TOK)))
    coef_ref[1] = jnp.transpose(jnp.broadcast_to(c_row, (TOK, TOK)))
    pad = jnp.zeros((1, DIM - TOK), F32)
    small_ref[...] = jnp.concatenate(
        [jnp.concatenate([row, pad], axis=1) for row in (sum_exp, t_tgt, mask_row)] + [gain_ref[...], jnp.zeros((4, DIM), F32)],
        axis=0,
    )
    for cp in second:
        cp.wait_send()


EARLY = 2
EARLY_ROWS = 2688
EARLY_TILES = [256, 640, 896, 896]
HEAD = 256
LATE_TILES = [512] + [768] * 12


def write_rows(dz_ref, x_ref, out_ref, stage, sem, start, first, tiles):
    copies = []
    for k, n in enumerate(tiles):
        rows = pl.ds(start, n)
        local = pl.ds(start - first, n)
        stage[local, :] = lax.dot_general(
            dz_ref[:, rows], x_ref[...], (((0,), (0,)), ((), ())), preferred_element_type=F32
        )
        cp = pltpu.make_async_copy(stage.at[local, :], out_ref.at[rows, :], sem.at[k])
        cp.start(priority=k % 2)
        copies.append(cp)
        start += n
    return copies


def grad_kernel(
    g_ref, emb_ref, x_ref, xh_ref, coef_ref, tgt_ref, demb_ref, dz_ref, head_ref, pay0, pay1, pay2, pay3, stage, dx_v, out_sem
):
    me = lax.axis_index("tp")
    lane_blk = lax.broadcasted_iota(jnp.int32, (BLK, TOK), 1)
    groups = [(j * GROUP, GROUP) for j in range(GROUPS - 1)]
    groups.append(((GROUPS - 1) * GROUP, GROUP + TAIL))

    def logit_grad(g0, n):
        for tb in range(TOK // BLK):
            rows = pl.ds(tb * BLK, BLK)
            tgt = tgt_ref[rows, :]
            a_blk = coef_ref[0, rows, :]
            c_blk = coef_ref[1, rows, :]
            for c in range(n // TOK):
                cols = pl.ds(g0 + c * TOK, TOK)
                hit = tgt == lane_blk + (g0 + c * TOK)
                dz_ref[rows, cols] = (a_blk * g_ref[rows, cols] - jnp.where(hit, c_blk, 0.0)).astype(BF16)

    for g0, n in groups[:EARLY]:
        logit_grad(g0, n)
    copies = write_rows(dz_ref, x_ref, demb_ref, stage, out_sem, 0, 0, EARLY_TILES)
    head_ref[...] = lax.dot_general(
        dz_ref[:, pl.ds(EARLY_ROWS, HEAD)], x_ref[...], (((0,), (0,)), ((), ())), preferred_element_type=F32
    )
    dx = 0.0
    for j, (g0, n) in enumerate(groups):
        if j >= EARLY:
            logit_grad(g0, n)
        dx += jnp.dot(dz_ref[:, pl.ds(g0, n)], emb_ref[pl.ds(g0, n), :], preferred_element_type=F32)
    dx_v[...] = dx
    gb = jnp.concatenate(
        [jnp.sum(dx * xh_ref[...], axis=0, keepdims=True), jnp.sum(dx, axis=0, keepdims=True), jnp.zeros((6, DIM), F32)], axis=0
    )
    for k, pay in enumerate((pay0, pay1, pay2, pay3)):
        pay[0:LOC, :] = dx_v[pl.ds(pl.multiple_of((me ^ k) * LOC, LOC), LOC), :]
        pay[LOC:, :] = gb
    for cp in copies:
        cp.wait()


def embed_kernel(
    demb_in, dz_ref, head_ref, x_ref, small_ref, demb_ref, tok_ref, mean_ref, stage, tok_v, mean_v, out_sem, side_sem
):
    sides = [
        pltpu.make_async_copy(src, dst, side_sem.at[k])
        for k, (src, dst) in enumerate([
            (head_ref, demb_ref.at[pl.ds(EARLY_ROWS, HEAD), :]), (tok_v, tok_ref), (mean_v, mean_ref),
        ])
    ]
    sides[0].start()
    copies = write_rows(dz_ref, x_ref, demb_ref, stage, out_sem, EARLY_ROWS + HEAD, EARLY_ROWS + HEAD, LATE_TILES)
    mask_row = small_ref[2:3, 0:TOK]
    lse = jnp.log(small_ref[0:1, 0:TOK])
    loss = (lse - SOFT_CAP * small_ref[1:2, 0:TOK] + Z_COEF * lse * lse) * mask_row
    mean_v[...] = row_sum(loss) / row_sum(mask_row)
    tok_v[...] = pltpu.roll(loss, lax.rem(TOK - lax.axis_index("tp") * LOC, TOK), 1)[:, 0:LOC]
    for cp in sides[1:]:
        cp.start()
    for cp in copies + sides:
        cp.wait()


def norm_kernel(p0, p1, p2, p3, xh_ref, rstd_ref, gain_in, dhid_ref, gain_ref, bias_ref, gb_v):
    me = lax.axis_index("tp")
    for k, pay in enumerate((p0, p1, p2, p3)):
        gb_v[me ^ k] = pay[LOC:, :]
    gb = gb_v[0] + gb_v[1] + gb_v[2] + gb_v[3]
    gain_ref[...] = gb[0:1, :]
    bias_ref[...] = gb[1:2, :]
    my_rows = pl.ds(pl.multiple_of(me * LOC, LOC), LOC)
    xh = xh_ref[my_rows, :]
    dxh = (p0[0:LOC, :] + p1[0:LOC, :] + p2[0:LOC, :] + p3[0:LOC, :]) * gain_in[3:4, :]
    m1 = row_sum(dxh) * (1.0 / DIM)
    m2 = row_sum(dxh * xh) * (1.0 / DIM)
    dhid_ref[...] = (rstd_ref[my_rows, 0:1] * (dxh - m1 - xh * m2)).astype(BF16)


def solution(mesh):
    vmem = pl.BlockSpec(memory_space=pltpu.VMEM)
    hbm = pl.BlockSpec(memory_space=pltpu.HBM)

    def group_step(hidden, ln_gain, ln_bias, out_embed, vocab_valid, targets, loss_mask):
        shape = jax.ShapeDtypeStruct
        small, xh, rstd, coef, tgt, x_all, g_all, emb = pl.pallas_call(
            main_kernel,
            out_shape=(
                shape((8, DIM), F32), shape((TOK, DIM), F32), shape((TOK, TOK), F32), shape((2, TOK, TOK), F32),
                shape((TOK, TOK), jnp.int32), shape((TOK, DIM), BF16), shape((TOK, VOCAB), F32), shape((VOCAB, DIM), BF16),
            ),
            in_specs=[hbm] * 7,
            out_specs=(vmem,) * 8,
            scratch_shapes=[
                pltpu.VMEM((LOC, DIM), BF16),
                pltpu.VMEM((1, DIM), F32),
                pltpu.VMEM((1, DIM), F32),
                pltpu.VMEM((VOCAB // TOK, TOK), jnp.int32),
                pltpu.VMEM((1, LOC), jnp.int32),
                pltpu.VMEM((1, LOC), jnp.int32),
                pltpu.VMEM((TOK, DIM), BF16),
                pltpu.VMEM((8 * TP, TOK), jnp.int32),
                pltpu.VMEM((8 * TP, TOK), F32),
                pltpu.VMEM((2, TOK, TOK), F32),
                pltpu.VMEM((2, TOK, GROUP), F32),
                pltpu.VMEM((DIM, TURNED), BF16),
                pltpu.VMEM((VOCAB // TOK, TOK), F32),
                pltpu.SemaphoreType.DMA((GROUPS,)),
                pltpu.SemaphoreType.DMA((9,)),
                pltpu.SemaphoreType.DMA((9,)),
                pltpu.SemaphoreType.DMA((6,)),
            ],
            compiler_params=pltpu.CompilerParams(collective_id=0, has_side_effects=True, vmem_limit_bytes=30 * 1024 * 1024),
            name="main",
        )(
            *(
                pltpu.with_memory_space_constraint(val, pltpu.HBM)
                for val in (
                    hidden, ln_gain.reshape(1, DIM), ln_bias.reshape(1, DIM), out_embed,
                    vocab_valid.reshape(VOCAB // TOK, TOK), targets.reshape(1, LOC), loss_mask.reshape(1, LOC),
                )
            )
        )
        part = shape((LOC + 8, DIM), F32)
        early, dz, head, *pays = pl.pallas_call(
            grad_kernel,
            out_shape=(shape((VOCAB, DIM), F32), shape((TOK, VOCAB), BF16), shape((HEAD, DIM), F32), part, part, part, part),
            in_specs=[vmem] * 6,
            out_specs=(hbm,) + (vmem,) * 6,
            scratch_shapes=[
                pltpu.VMEM((EARLY_ROWS, DIM), F32), pltpu.VMEM((TOK, DIM), F32), pltpu.SemaphoreType.DMA((len(EARLY_TILES),)),
            ],
            compiler_params=pltpu.CompilerParams(vmem_limit_bytes=16 * 1024 * 1024),
            name="grad",
        )(g_all, emb, x_all, xh, coef, tgt)
        moved = [lax.ppermute(pays[k], "tp", [(i, i ^ k) for i in range(TP)]) for k in range(1, TP)]
        d_embed, tok, mean = pl.pallas_call(
            embed_kernel,
            out_shape=(shape((VOCAB, DIM), F32), shape((1, LOC), F32), shape((1, 1), F32)),
            in_specs=[hbm] + [vmem] * 4,
            out_specs=(hbm, hbm, hbm),
            input_output_aliases={0: 0},
            scratch_shapes=[
                pltpu.VMEM((VOCAB - EARLY_ROWS - HEAD, DIM), F32), pltpu.VMEM((1, LOC), F32), pltpu.VMEM((1, 1), F32),
                pltpu.SemaphoreType.DMA((len(LATE_TILES),)), pltpu.SemaphoreType.DMA((3,)),
            ],
            compiler_params=pltpu.CompilerParams(vmem_limit_bytes=30 * 1024 * 1024),
            cost_estimate=pl.CostEstimate(flops=2 * TOK * VOCAB * DIM, bytes_accessed=4 * VOCAB * DIM, transcendentals=0),
            name="embed",
        )(early, dz, head, x_all, small)
        d_hidden, d_gain, d_bias = pl.pallas_call(
            norm_kernel,
            out_shape=(shape((LOC, DIM), BF16), shape((1, DIM), F32), shape((1, DIM), F32)),
            in_specs=[vmem] * 7,
            out_specs=(vmem,) * 3,
            scratch_shapes=[pltpu.VMEM((TP, 8, DIM), F32)],
            compiler_params=pltpu.CompilerParams(vmem_limit_bytes=8 * 1024 * 1024),
            name="norm",
        )(pays[0], *moved, xh, rstd, small)
        return tok.reshape(LOC), mean.reshape(1), d_hidden, d_embed, d_gain.reshape(DIM), d_bias.reshape(DIM)

    row_spec = P(("dp", "tp"))
    mat_spec = P(("dp", "tp"), None)
    return jax.shard_map(
        group_step, mesh=mesh,
        in_specs=(mat_spec, P(None), P(None), P("tp", None), P("tp"), row_spec, row_spec),
        out_specs=(row_spec, P("dp"), mat_spec, mat_spec, P("dp"), P("dp")), check_vma=False,
    )
```

```python
import functools

import jax
import jax.numpy as jnp
from jax import lax
from jax.experimental import pallas as pl
from jax.experimental.pallas import tpu as pltpu
from jax.sharding import PartitionSpec as P

SOFT_CAP = 30.0
Z_COEF = 1e-4
LN_EPS = 1e-5
LOG2E = 1.4426950408889634
MESH = pl.DeviceIdType.MESH
F32 = jnp.float32
BF16 = jnp.bfloat16

TP = 4
TOK = 128
LOC = TOK // TP
DIM = 512
VOCAB = 12672
TILE = 256
GROUP = 7 * TILE
GROUPS = VOCAB // GROUP
TAIL = VOCAB - GROUP * GROUPS
BLK = 32
TURN = 3
TURNED = TURN * GROUP
FWD = [7] * 6 + [4, 2, 2]


def row_sum(val):
    return jnp.sum(val, axis=-1, keepdims=True)


def main_kernel(
    hid_hbm, gain_hbm, bias_hbm, emb_ref, valid_hbm, tgt_hbm, mask_hbm,
    small_ref, xh_v, rstd_v, coef_ref, tgt_v, x_ref, g_v, emb_v,
    hid_ref, gain_ref, bias_ref, valid_ref, tgt_ref, mask_ref,
    hid_all, meta_v, stat_v, acc_v, z_v, embt_v, ok_v,
    emb_sem, send_sem, recv_sem, in_sem,
):
    me = lax.axis_index("tp")
    dp = lax.axis_index("dp")
    barrier = pltpu.get_barrier_semaphore()
    for k in range(1, TP):
        pl.semaphore_signal(barrier, inc=1, device_id=(dp, lax.rem(me + k, TP)), device_id_type=MESH)

    ins = [
        pltpu.make_async_copy(src, dst, in_sem.at[k])
        for k, (src, dst) in enumerate([
            (hid_hbm, hid_ref), (tgt_hbm, tgt_ref), (mask_hbm, mask_ref),
            (gain_hbm, gain_ref), (bias_hbm, bias_ref), (valid_hbm, valid_ref),
        ])
    ]
    for cp in ins:
        cp.start()
    chunks = [(j * GROUP, GROUP) for j in range(GROUPS - 1)]
    chunks.append(((GROUPS - 1) * GROUP, GROUP + TAIL))
    emb_copies = [
        pltpu.make_async_copy(emb_ref.at[pl.ds(s, n), :], emb_v.at[pl.ds(s, n), :], emb_sem.at[k])
        for k, (s, n) in enumerate(chunks)
    ]
    for cp in emb_copies:
        cp.start()

    my_rows = pl.ds(pl.multiple_of(me * LOC, LOC), LOC)
    my_meta = pl.ds(pl.multiple_of(me * 8, 8), 8)
    ins[0].wait()
    pl.semaphore_wait(barrier, TP - 1)

    def push(src, dst, idx):
        copies = []
        for k in range(1, TP):
            cp = pltpu.make_async_remote_copy(
                src_ref=src(k), dst_ref=dst, send_sem=send_sem.at[3 * idx + k - 1], recv_sem=recv_sem.at[3 * idx + k - 1],
                device_id=(dp, lax.rem(me + k, TP)), device_id_type=MESH,
            )
            cp.start()
            copies.append(cp)
        return copies

    first = push(lambda k: hid_ref, hid_all.at[my_rows, :], 0)
    for cp in ins[1:3]:
        cp.wait()
    lane = lax.broadcasted_iota(jnp.int32, (1, TOK), 1)
    mine = (lane // LOC) == me
    tgt4 = jnp.concatenate([tgt_ref[...]] * TP, axis=1)
    mask4 = jnp.concatenate([mask_ref[...]] * TP, axis=1)
    meta_v[my_meta, :] = jnp.concatenate(
        [jnp.where(mine, tgt4, 0), jnp.where(mine, mask4, 0), jnp.zeros((6, TOK), jnp.int32)], axis=0
    )
    hid_all[my_rows, :] = hid_ref[...]
    first += push(lambda k: meta_v.at[my_meta, :], meta_v.at[my_meta, :], 1)
    for cp in ins[3:]:
        cp.wait()
    ok_v[...] = valid_ref[...].astype(F32)
    for cp, (g0, n) in zip(emb_copies[:TURN], chunks):
        cp.wait()
        for s in range(g0, g0 + n, TILE):
            embt_v[:, pl.ds(s, TILE)] = jnp.transpose(emb_v[pl.ds(s, TILE), :])
    for cp in first:
        cp.wait_recv()

    meta = meta_v[0:8, :] + meta_v[8:16, :] + meta_v[16:24, :] + meta_v[24:32, :]
    tgt_row = meta[0:1, :]
    mask_row = meta[1:2, :].astype(F32)
    tok_count = row_sum(mask_row)
    tgt_col = jnp.transpose(jnp.broadcast_to(tgt_row, (TOK, TOK)))

    h = hid_all[...].astype(F32)
    mean_val = row_sum(h) * (1.0 / DIM)
    cent = h - mean_val
    var_val = row_sum(cent * cent) * (1.0 / DIM)
    rstd = lax.rsqrt(var_val + LN_EPS)
    xh = cent * rstd
    xh_v[...] = xh
    rstd_v[...] = jnp.broadcast_to(rstd, (TOK, TOK))
    x_ref[...] = (xh * gain_ref[...] + bias_ref[...]).astype(BF16)

    tgt_v[...] = tgt_col - me * VOCAB
    lane_blk = lax.broadcasted_iota(jnp.int32, (BLK, TOK), 1)
    plain = [(s, TILE) for s in range(0, TURNED, TILE)]
    other = [(s, min(TILE, VOCAB - s)) for s in range(TURNED, VOCAB, TILE)]
    tiles = []
    while plain or other:
        if other:
            tiles.append(other.pop(0))
        if plain:
            tiles.append(plain.pop(0))
    groups = []
    for n in FWD:
        groups.append(tiles[:n])
        tiles = tiles[n:]

    def logits(j):
        pos = 0
        for col, w in groups[j]:
            if col < TURNED:
                z = jnp.dot(x_ref[...], embt_v[:, pl.ds(col, w)], preferred_element_type=F32)
            else:
                z = lax.dot_general(
                    x_ref[...], emb_v[pl.ds(col, w), :], (((1,), (1,)), ((), ())), preferred_element_type=F32
                )
            z_v[j % 2, :, pl.ds(pos, w)] = z
            pos += w

    def softmax_pass(j):
        cols = [c for col, w in groups[j] for c in range(col, col + w, TOK)]
        for tb in range(TOK // BLK):
            rows = pl.ds(tb * BLK, BLK)
            tgt = tgt_v[rows, :]
            s_acc = acc_v[0, rows, :]
            t_acc = acc_v[1, rows, :]
            for first_c in range(0, len(cols), 2):
                pick = 0.0
                for c in range(first_c, min(first_c + 2, len(cols))):
                    col = cols[c]
                    t = jnp.tanh(z_v[j % 2, rows, pl.ds(c * TOK, TOK)] * (1.0 / SOFT_CAP))
                    e = jnp.exp2(t * (SOFT_CAP * LOG2E)) * ok_v[col // TOK:col // TOK + 1, :]
                    pick = jnp.where(tgt == lane_blk + col, t, pick)
                    g_v[rows, pl.ds(col, TOK)] = e * (1.0 - t * t)
                    s_acc += e
                t_acc += pick
            acc_v[0, rows, :] = s_acc
            acc_v[1, rows, :] = t_acc

    for cp in emb_copies[TURN:]:
        cp.wait()
    acc_v[...] = jnp.zeros_like(acc_v)
    for j in range(len(groups)):
        logits(j)
        if j > 0:
            softmax_pass(j - 1)
    softmax_pass(len(groups) - 1)

    s_loc = jnp.sum(jnp.transpose(acc_v[0]), axis=0, keepdims=True)
    t_loc = jnp.sum(jnp.transpose(acc_v[1]), axis=0, keepdims=True)
    stat_v[my_meta, :] = jnp.concatenate([s_loc, t_loc, jnp.zeros((6, TOK), F32)], axis=0)
    second = push(lambda k: stat_v.at[my_meta, :], stat_v.at[my_meta, :], 2)
    for cp in first:
        cp.wait_send()
    for cp in second:
        cp.wait_recv()
    stats = stat_v[0:8, :] + stat_v[8:16, :] + stat_v[16:24, :] + stat_v[24:32, :]
    sum_exp = stats[0:1, :]
    t_tgt = stats[1:2, :]
    lse = jnp.log(sum_exp)
    coef = mask_row / tok_count
    a_row = (1.0 + 2.0 * Z_COEF * lse) * coef / sum_exp
    c_row = coef * (1.0 - t_tgt * t_tgt)
    coef_ref[0] = jnp.transpose(jnp.broadcast_to(a_row, (TOK, TOK)))
    coef_ref[1] = jnp.transpose(jnp.broadcast_to(c_row, (TOK, TOK)))
    pad = jnp.zeros((1, DIM - TOK), F32)
    small_ref[...] = jnp.concatenate(
        [jnp.concatenate([row, pad], axis=1) for row in (sum_exp, t_tgt, mask_row)] + [gain_ref[...], jnp.zeros((4, DIM), F32)],
        axis=0,
    )
    for cp in second:
        cp.wait_send()


EARLY = 2
EARLY_ROWS = 2688
EARLY_TILES = [256, 640, 896, 896]
HEAD = 256
LATE_TILES = [256, 256] + [768] * 12


def write_rows(dz_ref, x_ref, out_ref, stage, sem, start, first, tiles):
    copies = []
    for k, n in enumerate(tiles):
        rows = pl.ds(start, n)
        local = pl.ds(start - first, n)
        stage[local, :] = lax.dot_general(
            dz_ref[:, rows], x_ref[...], (((0,), (0,)), ((), ())), preferred_element_type=F32
        )
        cp = pltpu.make_async_copy(stage.at[local, :], out_ref.at[rows, :], sem.at[k])
        cp.start(priority=k % 2)
        copies.append(cp)
        start += n
    return copies


def grad_kernel(
    g_ref, emb_ref, x_ref, xh_ref, coef_ref, tgt_ref, demb_ref, dz_ref, head_ref, pay0, pay1, pay2, pay3, stage, dx_v, out_sem
):
    me = lax.axis_index("tp")
    lane_blk = lax.broadcasted_iota(jnp.int32, (BLK, TOK), 1)
    groups = [(j * GROUP, GROUP) for j in range(GROUPS - 1)]
    groups.append(((GROUPS - 1) * GROUP, GROUP + TAIL))

    def logit_grad(g0, n):
        for tb in range(TOK // BLK):
            rows = pl.ds(tb * BLK, BLK)
            tgt = tgt_ref[rows, :]
            a_blk = coef_ref[0, rows, :]
            c_blk = coef_ref[1, rows, :]
            for c in range(n // TOK):
                cols = pl.ds(g0 + c * TOK, TOK)
                hit = tgt == lane_blk + (g0 + c * TOK)
                dz_ref[rows, cols] = (a_blk * g_ref[rows, cols] - jnp.where(hit, c_blk, 0.0)).astype(BF16)

    for g0, n in groups[:EARLY]:
        logit_grad(g0, n)
    copies = write_rows(dz_ref, x_ref, demb_ref, stage, out_sem, 0, 0, EARLY_TILES)
    head_ref[...] = lax.dot_general(
        dz_ref[:, pl.ds(EARLY_ROWS, HEAD)], x_ref[...], (((0,), (0,)), ((), ())), preferred_element_type=F32
    )
    dx = 0.0
    for j, (g0, n) in enumerate(groups):
        if j >= EARLY:
            logit_grad(g0, n)
        dx += jnp.dot(dz_ref[:, pl.ds(g0, n)], emb_ref[pl.ds(g0, n), :], preferred_element_type=F32)
    dx_v[...] = dx
    gb = jnp.concatenate(
        [jnp.sum(dx * xh_ref[...], axis=0, keepdims=True), jnp.sum(dx, axis=0, keepdims=True), jnp.zeros((6, DIM), F32)], axis=0
    )
    for k, pay in enumerate((pay0, pay1, pay2, pay3)):
        pay[0:LOC, :] = dx_v[pl.ds(pl.multiple_of((me ^ k) * LOC, LOC), LOC), :]
        pay[LOC:, :] = gb
    for cp in copies:
        cp.wait()


def embed_kernel(
    demb_in, dz_ref, head_ref, x_ref, small_ref, demb_ref, tok_ref, mean_ref, stage, tok_v, mean_v, out_sem, side_sem
):
    sides = [
        pltpu.make_async_copy(src, dst, side_sem.at[k])
        for k, (src, dst) in enumerate([
            (head_ref, demb_ref.at[pl.ds(EARLY_ROWS, HEAD), :]), (tok_v, tok_ref), (mean_v, mean_ref),
        ])
    ]
    sides[0].start()
    copies = write_rows(dz_ref, x_ref, demb_ref, stage, out_sem, EARLY_ROWS + HEAD, EARLY_ROWS + HEAD, LATE_TILES)
    mask_row = small_ref[2:3, 0:TOK]
    lse = jnp.log(small_ref[0:1, 0:TOK])
    loss = (lse - SOFT_CAP * small_ref[1:2, 0:TOK] + Z_COEF * lse * lse) * mask_row
    mean_v[...] = row_sum(loss) / row_sum(mask_row)
    tok_v[...] = pltpu.roll(loss, lax.rem(TOK - lax.axis_index("tp") * LOC, TOK), 1)[:, 0:LOC]
    for cp in sides[1:]:
        cp.start()
    for cp in copies + sides:
        cp.wait()


def norm_kernel(p0, p1, p2, p3, xh_ref, rstd_ref, gain_in, dhid_ref, gain_ref, bias_ref, gb_v):
    me = lax.axis_index("tp")
    for k, pay in enumerate((p0, p1, p2, p3)):
        gb_v[me ^ k] = pay[LOC:, :]
    gb = gb_v[0] + gb_v[1] + gb_v[2] + gb_v[3]
    gain_ref[...] = gb[0:1, :]
    bias_ref[...] = gb[1:2, :]
    my_rows = pl.ds(pl.multiple_of(me * LOC, LOC), LOC)
    xh = xh_ref[my_rows, :]
    dxh = (p0[0:LOC, :] + p1[0:LOC, :] + p2[0:LOC, :] + p3[0:LOC, :]) * gain_in[3:4, :]
    m1 = row_sum(dxh) * (1.0 / DIM)
    m2 = row_sum(dxh * xh) * (1.0 / DIM)
    dhid_ref[...] = (rstd_ref[my_rows, 0:1] * (dxh - m1 - xh * m2)).astype(BF16)


def solution(mesh):
    vmem = pl.BlockSpec(memory_space=pltpu.VMEM)
    hbm = pl.BlockSpec(memory_space=pltpu.HBM)

    def group_step(hidden, ln_gain, ln_bias, out_embed, vocab_valid, targets, loss_mask):
        shape = jax.ShapeDtypeStruct
        small, xh, rstd, coef, tgt, x_all, g_all, emb = pl.pallas_call(
            main_kernel,
            out_shape=(
                shape((8, DIM), F32), shape((TOK, DIM), F32), shape((TOK, TOK), F32), shape((2, TOK, TOK), F32),
                shape((TOK, TOK), jnp.int32), shape((TOK, DIM), BF16), shape((TOK, VOCAB), F32), shape((VOCAB, DIM), BF16),
            ),
            in_specs=[hbm] * 7,
            out_specs=(vmem,) * 8,
            scratch_shapes=[
                pltpu.VMEM((LOC, DIM), BF16),
                pltpu.VMEM((1, DIM), F32),
                pltpu.VMEM((1, DIM), F32),
                pltpu.VMEM((VOCAB // TOK, TOK), jnp.int32),
                pltpu.VMEM((1, LOC), jnp.int32),
                pltpu.VMEM((1, LOC), jnp.int32),
                pltpu.VMEM((TOK, DIM), BF16),
                pltpu.VMEM((8 * TP, TOK), jnp.int32),
                pltpu.VMEM((8 * TP, TOK), F32),
                pltpu.VMEM((2, TOK, TOK), F32),
                pltpu.VMEM((2, TOK, GROUP), F32),
                pltpu.VMEM((DIM, TURNED), BF16),
                pltpu.VMEM((VOCAB // TOK, TOK), F32),
                pltpu.SemaphoreType.DMA((GROUPS,)),
                pltpu.SemaphoreType.DMA((9,)),
                pltpu.SemaphoreType.DMA((9,)),
                pltpu.SemaphoreType.DMA((6,)),
            ],
            compiler_params=pltpu.CompilerParams(collective_id=0, has_side_effects=True, vmem_limit_bytes=30 * 1024 * 1024),
            name="main",
        )(
            *(
                pltpu.with_memory_space_constraint(val, pltpu.HBM)
                for val in (
                    hidden, ln_gain.reshape(1, DIM), ln_bias.reshape(1, DIM), out_embed,
                    vocab_valid.reshape(VOCAB // TOK, TOK), targets.reshape(1, LOC), loss_mask.reshape(1, LOC),
                )
            )
        )
        part = shape((LOC + 8, DIM), F32)
        early, dz, head, *pays = pl.pallas_call(
            grad_kernel,
            out_shape=(shape((VOCAB, DIM), F32), shape((TOK, VOCAB), BF16), shape((HEAD, DIM), F32), part, part, part, part),
            in_specs=[vmem] * 6,
            out_specs=(hbm,) + (vmem,) * 6,
            scratch_shapes=[
                pltpu.VMEM((EARLY_ROWS, DIM), F32), pltpu.VMEM((TOK, DIM), F32), pltpu.SemaphoreType.DMA((len(EARLY_TILES),)),
            ],
            compiler_params=pltpu.CompilerParams(vmem_limit_bytes=16 * 1024 * 1024),
            name="grad",
        )(g_all, emb, x_all, xh, coef, tgt)
        moved = [lax.ppermute(pays[k], "tp", [(i, i ^ k) for i in range(TP)]) for k in range(1, TP)]
        d_embed, tok, mean = pl.pallas_call(
            embed_kernel,
            out_shape=(shape((VOCAB, DIM), F32), shape((1, LOC), F32), shape((1, 1), F32)),
            in_specs=[hbm] + [vmem] * 4,
            out_specs=(hbm, hbm, hbm),
            input_output_aliases={0: 0},
            scratch_shapes=[
                pltpu.VMEM((VOCAB - EARLY_ROWS - HEAD, DIM), F32), pltpu.VMEM((1, LOC), F32), pltpu.VMEM((1, 1), F32),
                pltpu.SemaphoreType.DMA((len(LATE_TILES),)), pltpu.SemaphoreType.DMA((3,)),
            ],
            compiler_params=pltpu.CompilerParams(vmem_limit_bytes=30 * 1024 * 1024),
            cost_estimate=pl.CostEstimate(flops=2 * TOK * VOCAB * DIM, bytes_accessed=4 * VOCAB * DIM, transcendentals=0),
            name="embed",
        )(early, dz, head, x_all, small)
        d_hidden, d_gain, d_bias = pl.pallas_call(
            norm_kernel,
            out_shape=(shape((LOC, DIM), BF16), shape((1, DIM), F32), shape((1, DIM), F32)),
            in_specs=[vmem] * 7,
            out_specs=(vmem,) * 3,
            scratch_shapes=[pltpu.VMEM((TP, 8, DIM), F32)],
            compiler_params=pltpu.CompilerParams(vmem_limit_bytes=8 * 1024 * 1024),
            name="norm",
        )(pays[0], *moved, xh, rstd, small)
        return tok.reshape(LOC), mean.reshape(1), d_hidden, d_embed, d_gain.reshape(DIM), d_bias.reshape(DIM)

    row_spec = P(("dp", "tp"))
    mat_spec = P(("dp", "tp"), None)
    return jax.shard_map(
        group_step, mesh=mesh,
        in_specs=(mat_spec, P(None), P(None), P("tp", None), P("tp"), row_spec, row_spec),
        out_specs=(row_spec, P("dp"), mat_spec, mat_spec, P("dp"), P("dp")), check_vma=False,
    )
```

```python
import functools

import jax
import jax.numpy as jnp
from jax import lax
from jax.experimental import pallas as pl
from jax.experimental.pallas import tpu as pltpu
from jax.sharding import PartitionSpec as P

SOFT_CAP = 30.0
Z_COEF = 1e-4
LN_EPS = 1e-5
LOG2E = 1.4426950408889634
MESH = pl.DeviceIdType.MESH
F32 = jnp.float32
BF16 = jnp.bfloat16

TP = 4
TOK = 128
LOC = TOK // TP
DIM = 512
VOCAB = 12672
TILE = 256
GROUP = 7 * TILE
GROUPS = VOCAB // GROUP
TAIL = VOCAB - GROUP * GROUPS
BLK = 32
TURN = 4
TURNED = TURN * GROUP
FWD = [7] * 6 + [4, 2, 2]


def row_sum(val):
    return jnp.sum(val, axis=-1, keepdims=True)


def main_kernel(
    hid_hbm, gain_hbm, bias_hbm, emb_ref, valid_hbm, tgt_hbm, mask_hbm,
    small_ref, xh_v, rstd_v, coef_ref, tgt_v, x_ref, g_v, emb_v,
    hid_ref, gain_ref, bias_ref, valid_ref, tgt_ref, mask_ref,
    hid_all, meta_v, stat_v, acc_v, z_v, embt_v, ok_v,
    emb_sem, send_sem, recv_sem, in_sem,
):
    me = lax.axis_index("tp")
    dp = lax.axis_index("dp")
    barrier = pltpu.get_barrier_semaphore()
    for k in (2, 3, 1):
        pl.semaphore_signal(barrier, inc=1, device_id=(dp, me ^ k), device_id_type=MESH)

    ins = [
        pltpu.make_async_copy(src, dst, in_sem.at[k])
        for k, (src, dst) in enumerate([
            (hid_hbm, hid_ref), (tgt_hbm, tgt_ref), (mask_hbm, mask_ref),
            (gain_hbm, gain_ref), (bias_hbm, bias_ref), (valid_hbm, valid_ref),
        ])
    ]
    for cp in ins:
        cp.start()
    chunks = [(j * GROUP, GROUP) for j in range(GROUPS - 1)]
    chunks.append(((GROUPS - 1) * GROUP, GROUP + TAIL))
    emb_copies = [
        pltpu.make_async_copy(emb_ref.at[pl.ds(s, n), :], emb_v.at[pl.ds(s, n), :], emb_sem.at[k])
        for k, (s, n) in enumerate(chunks)
    ]
    for cp in emb_copies:
        cp.start()

    my_rows = pl.ds(pl.multiple_of(me * LOC, LOC), LOC)
    my_meta = pl.ds(pl.multiple_of(me * 8, 8), 8)
    ins[0].wait()
    pl.semaphore_wait(barrier, TP - 1)

    def push(src, dst, idx):
        copies = []
        for k in (2, 3, 1):
            cp = pltpu.make_async_remote_copy(
                src_ref=src(k), dst_ref=dst, send_sem=send_sem.at[3 * idx + k - 1], recv_sem=recv_sem.at[3 * idx + k - 1],
                device_id=(dp, me ^ k), device_id_type=MESH,
            )
            cp.start()
            copies.append(cp)
        return copies

    first = push(lambda k: hid_ref, hid_all.at[my_rows, :], 0)
    for cp in ins[1:3]:
        cp.wait()
    lane = lax.broadcasted_iota(jnp.int32, (1, TOK), 1)
    mine = (lane // LOC) == me
    tgt4 = jnp.concatenate([tgt_ref[...]] * TP, axis=1)
    mask4 = jnp.concatenate([mask_ref[...]] * TP, axis=1)
    meta_v[my_meta, :] = jnp.concatenate(
        [jnp.where(mine, tgt4, 0), jnp.where(mine, mask4, 0), jnp.zeros((6, TOK), jnp.int32)], axis=0
    )
    hid_all[my_rows, :] = hid_ref[...]
    first += push(lambda k: meta_v.at[my_meta, :], meta_v.at[my_meta, :], 1)
    for cp in ins[3:]:
        cp.wait()
    ok_v[...] = valid_ref[...].astype(F32)
    for cp, (g0, n) in zip(emb_copies[:TURN], chunks):
        cp.wait()
        for s in range(g0, g0 + n, TILE):
            embt_v[:, pl.ds(s, TILE)] = jnp.transpose(emb_v[pl.ds(s, TILE), :])
    for cp in first:
        cp.wait_recv()

    meta = meta_v[0:8, :] + meta_v[8:16, :] + meta_v[16:24, :] + meta_v[24:32, :]
    tgt_row = meta[0:1, :]
    mask_row = meta[1:2, :].astype(F32)
    tok_count = row_sum(mask_row)
    tgt_col = jnp.transpose(jnp.broadcast_to(tgt_row, (TOK, TOK)))

    h = hid_all[...].astype(F32)
    mean_val = row_sum(h) * (1.0 / DIM)
    cent = h - mean_val
    var_val = row_sum(cent * cent) * (1.0 / DIM)
    rstd = lax.rsqrt(var_val + LN_EPS)
    xh = cent * rstd
    xh_v[...] = xh
    rstd_v[...] = jnp.broadcast_to(rstd, (TOK, TOK))
    x_ref[...] = (xh * gain_ref[...] + bias_ref[...]).astype(BF16)

    tgt_v[...] = tgt_col - me * VOCAB
    lane_blk = lax.broadcasted_iota(jnp.int32, (BLK, TOK), 1)
    plain = [(s, TILE) for s in range(0, TURNED, TILE)]
    other = [(s, min(TILE, VOCAB - s)) for s in range(TURNED, VOCAB, TILE)]
    tiles = []
    while plain or other:
        if other:
            tiles.append(other.pop(0))
        if plain:
            tiles.append(plain.pop(0))
    groups = []
    for n in FWD:
        groups.append(tiles[:n])
        tiles = tiles[n:]

    def logits(j):
        pos = 0
        for col, w in groups[j]:
            if col < TURNED:
                z = jnp.dot(x_ref[...], embt_v[:, pl.ds(col, w)], preferred_element_type=F32)
            else:
                z = lax.dot_general(
                    x_ref[...], emb_v[pl.ds(col, w), :], (((1,), (1,)), ((), ())), preferred_element_type=F32
                )
            z_v[j % 2, :, pl.ds(pos, w)] = z
            pos += w

    def softmax_pass(j):
        cols = [c for col, w in groups[j] for c in range(col, col + w, TOK)]
        for tb in range(TOK // BLK):
            rows = pl.ds(tb * BLK, BLK)
            tgt = tgt_v[rows, :]
            s_acc = acc_v[0, rows, :]
            t_acc = acc_v[1, rows, :]
            for first_c in range(0, len(cols), 2):
                pick = 0.0
                for c in range(first_c, min(first_c + 2, len(cols))):
                    col = cols[c]
                    t = jnp.tanh(z_v[j % 2, rows, pl.ds(c * TOK, TOK)] * (1.0 / SOFT_CAP))
                    e = jnp.exp2(t * (SOFT_CAP * LOG2E)) * ok_v[col // TOK:col // TOK + 1, :]
                    pick = jnp.where(tgt == lane_blk + col, t, pick)
                    g_v[rows, pl.ds(col, TOK)] = e * (1.0 - t * t)
                    s_acc += e
                t_acc += pick
            acc_v[0, rows, :] = s_acc
            acc_v[1, rows, :] = t_acc

    for cp in emb_copies[TURN:]:
        cp.wait()
    acc_v[...] = jnp.zeros_like(acc_v)
    for j in range(len(groups)):
        logits(j)
        if j > 0:
            softmax_pass(j - 1)
    softmax_pass(len(groups) - 1)

    s_loc = jnp.sum(jnp.transpose(acc_v[0]), axis=0, keepdims=True)
    t_loc = jnp.sum(jnp.transpose(acc_v[1]), axis=0, keepdims=True)
    stat_v[my_meta, :] = jnp.concatenate([s_loc, t_loc, jnp.zeros((6, TOK), F32)], axis=0)
    second = push(lambda k: stat_v.at[my_meta, :], stat_v.at[my_meta, :], 2)
    for cp in first:
        cp.wait_send()
    for cp in second:
        cp.wait_recv()
    stats = stat_v[0:8, :] + stat_v[8:16, :] + stat_v[16:24, :] + stat_v[24:32, :]
    sum_exp = stats[0:1, :]
    t_tgt = stats[1:2, :]
    lse = jnp.log(sum_exp)
    coef = mask_row / tok_count
    a_row = (1.0 + 2.0 * Z_COEF * lse) * coef / sum_exp
    c_row = coef * (1.0 - t_tgt * t_tgt)
    coef_ref[0] = jnp.transpose(jnp.broadcast_to(a_row, (TOK, TOK)))
    coef_ref[1] = jnp.transpose(jnp.broadcast_to(c_row, (TOK, TOK)))
    pad = jnp.zeros((1, DIM - TOK), F32)
    small_ref[...] = jnp.concatenate(
        [jnp.concatenate([row, pad], axis=1) for row in (sum_exp, t_tgt, mask_row)] + [gain_ref[...], jnp.zeros((4, DIM), F32)],
        axis=0,
    )
    for cp in second:
        cp.wait_send()


EARLY = 2
EARLY_ROWS = 2688
EARLY_TILES = [256, 640, 896, 896]
HEAD = 256
LATE_TILES = [256, 256] + [768] * 12


def write_rows(dz_ref, x_ref, out_ref, stage, sem, start, first, tiles):
    copies = []
    for k, n in enumerate(tiles):
        rows = pl.ds(start, n)
        local = pl.ds(start - first, n)
        stage[local, :] = lax.dot_general(
            dz_ref[:, rows], x_ref[...], (((0,), (0,)), ((), ())), preferred_element_type=F32
        )
        cp = pltpu.make_async_copy(stage.at[local, :], out_ref.at[rows, :], sem.at[k])
        cp.start(priority=k % 2)
        copies.append(cp)
        start += n
    return copies


def grad_kernel(
    g_ref, emb_ref, x_ref, xh_ref, coef_ref, tgt_ref, demb_ref, dz_ref, head_ref, pay0, pay1, pay2, pay3, stage, dx_v, out_sem
):
    me = lax.axis_index("tp")
    lane_blk = lax.broadcasted_iota(jnp.int32, (BLK, TOK), 1)
    groups = [(j * GROUP, GROUP) for j in range(GROUPS - 1)]
    groups.append(((GROUPS - 1) * GROUP, GROUP + TAIL))

    def logit_grad(g0, n):
        for tb in range(TOK // BLK):
            rows = pl.ds(tb * BLK, BLK)
            tgt = tgt_ref[rows, :]
            a_blk = coef_ref[0, rows, :]
            c_blk = coef_ref[1, rows, :]
            for c in range(n // TOK):
                cols = pl.ds(g0 + c * TOK, TOK)
                hit = tgt == lane_blk + (g0 + c * TOK)
                dz_ref[rows, cols] = (a_blk * g_ref[rows, cols] - jnp.where(hit, c_blk, 0.0)).astype(BF16)

    for g0, n in groups[:EARLY]:
        logit_grad(g0, n)
    copies = write_rows(dz_ref, x_ref, demb_ref, stage, out_sem, 0, 0, EARLY_TILES)
    head_ref[...] = lax.dot_general(
        dz_ref[:, pl.ds(EARLY_ROWS, HEAD)], x_ref[...], (((0,), (0,)), ((), ())), preferred_element_type=F32
    )
    dx = 0.0
    for j, (g0, n) in enumerate(groups):
        if j >= EARLY:
            logit_grad(g0, n)
        dx += jnp.dot(dz_ref[:, pl.ds(g0, n)], emb_ref[pl.ds(g0, n), :], preferred_element_type=F32)
    dx_v[...] = dx
    gb = jnp.concatenate(
        [jnp.sum(dx * xh_ref[...], axis=0, keepdims=True), jnp.sum(dx, axis=0, keepdims=True), jnp.zeros((6, DIM), F32)], axis=0
    )
    for k, pay in enumerate((pay0, pay1, pay2, pay3)):
        pay[0:LOC, :] = dx_v[pl.ds(pl.multiple_of((me ^ k) * LOC, LOC), LOC), :]
        pay[LOC:, :] = gb
    for cp in copies:
        cp.wait()


def embed_kernel(
    demb_in, dz_ref, head_ref, x_ref, small_ref, demb_ref, tok_ref, mean_ref, stage, tok_v, mean_v, out_sem, side_sem
):
    sides = [
        pltpu.make_async_copy(src, dst, side_sem.at[k])
        for k, (src, dst) in enumerate([
            (head_ref, demb_ref.at[pl.ds(EARLY_ROWS, HEAD), :]), (tok_v, tok_ref), (mean_v, mean_ref),
        ])
    ]
    sides[0].start()
    copies = write_rows(dz_ref, x_ref, demb_ref, stage, out_sem, EARLY_ROWS + HEAD, EARLY_ROWS + HEAD, LATE_TILES)
    mask_row = small_ref[2:3, 0:TOK]
    lse = jnp.log(small_ref[0:1, 0:TOK])
    loss = (lse - SOFT_CAP * small_ref[1:2, 0:TOK] + Z_COEF * lse * lse) * mask_row
    mean_v[...] = row_sum(loss) / row_sum(mask_row)
    tok_v[...] = pltpu.roll(loss, lax.rem(TOK - lax.axis_index("tp") * LOC, TOK), 1)[:, 0:LOC]
    for cp in sides[1:]:
        cp.start()
    for cp in copies + sides:
        cp.wait()


def norm_kernel(p0, p1, p2, p3, xh_ref, rstd_ref, gain_in, dhid_ref, gain_ref, bias_ref, gb_v):
    me = lax.axis_index("tp")
    for k, pay in enumerate((p0, p1, p2, p3)):
        gb_v[me ^ k] = pay[LOC:, :]
    gb = gb_v[0] + gb_v[1] + gb_v[2] + gb_v[3]
    gain_ref[...] = gb[0:1, :]
    bias_ref[...] = gb[1:2, :]
    my_rows = pl.ds(pl.multiple_of(me * LOC, LOC), LOC)
    xh = xh_ref[my_rows, :]
    dxh = (p0[0:LOC, :] + p1[0:LOC, :] + p2[0:LOC, :] + p3[0:LOC, :]) * gain_in[3:4, :]
    m1 = row_sum(dxh) * (1.0 / DIM)
    m2 = row_sum(dxh * xh) * (1.0 / DIM)
    dhid_ref[...] = (rstd_ref[my_rows, 0:1] * (dxh - m1 - xh * m2)).astype(BF16)


def solution(mesh):
    vmem = pl.BlockSpec(memory_space=pltpu.VMEM)
    hbm = pl.BlockSpec(memory_space=pltpu.HBM)

    def group_step(hidden, ln_gain, ln_bias, out_embed, vocab_valid, targets, loss_mask):
        shape = jax.ShapeDtypeStruct
        small, xh, rstd, coef, tgt, x_all, g_all, emb = pl.pallas_call(
            main_kernel,
            out_shape=(
                shape((8, DIM), F32), shape((TOK, DIM), F32), shape((TOK, TOK), F32), shape((2, TOK, TOK), F32),
                shape((TOK, TOK), jnp.int32), shape((TOK, DIM), BF16), shape((TOK, VOCAB), F32), shape((VOCAB, DIM), BF16),
            ),
            in_specs=[hbm] * 7,
            out_specs=(vmem,) * 8,
            scratch_shapes=[
                pltpu.VMEM((LOC, DIM), BF16),
                pltpu.VMEM((1, DIM), F32),
                pltpu.VMEM((1, DIM), F32),
                pltpu.VMEM((VOCAB // TOK, TOK), jnp.int32),
                pltpu.VMEM((1, LOC), jnp.int32),
                pltpu.VMEM((1, LOC), jnp.int32),
                pltpu.VMEM((TOK, DIM), BF16),
                pltpu.VMEM((8 * TP, TOK), jnp.int32),
                pltpu.VMEM((8 * TP, TOK), F32),
                pltpu.VMEM((2, TOK, TOK), F32),
                pltpu.VMEM((2, TOK, GROUP), F32),
                pltpu.VMEM((DIM, TURNED), BF16),
                pltpu.VMEM((VOCAB // TOK, TOK), F32),
                pltpu.SemaphoreType.DMA((GROUPS,)),
                pltpu.SemaphoreType.DMA((9,)),
                pltpu.SemaphoreType.DMA((9,)),
                pltpu.SemaphoreType.DMA((6,)),
            ],
            compiler_params=pltpu.CompilerParams(collective_id=0, has_side_effects=True, vmem_limit_bytes=30 * 1024 * 1024),
            name="main",
        )(
            *(
                pltpu.with_memory_space_constraint(val, pltpu.HBM)
                for val in (
                    hidden, ln_gain.reshape(1, DIM), ln_bias.reshape(1, DIM), out_embed,
                    vocab_valid.reshape(VOCAB // TOK, TOK), targets.reshape(1, LOC), loss_mask.reshape(1, LOC),
                )
            )
        )
        part = shape((LOC + 8, DIM), F32)
        early, dz, head, *pays = pl.pallas_call(
            grad_kernel,
            out_shape=(shape((VOCAB, DIM), F32), shape((TOK, VOCAB), BF16), shape((HEAD, DIM), F32), part, part, part, part),
            in_specs=[vmem] * 6,
            out_specs=(hbm,) + (vmem,) * 6,
            scratch_shapes=[
                pltpu.VMEM((EARLY_ROWS, DIM), F32), pltpu.VMEM((TOK, DIM), F32), pltpu.SemaphoreType.DMA((len(EARLY_TILES),)),
            ],
            compiler_params=pltpu.CompilerParams(vmem_limit_bytes=16 * 1024 * 1024),
            name="grad",
        )(g_all, emb, x_all, xh, coef, tgt)
        moved = [lax.ppermute(pays[k], "tp", [(i, i ^ k) for i in range(TP)]) for k in range(1, TP)]
        d_embed, tok, mean = pl.pallas_call(
            embed_kernel,
            out_shape=(shape((VOCAB, DIM), F32), shape((1, LOC), F32), shape((1, 1), F32)),
            in_specs=[hbm] + [vmem] * 4,
            out_specs=(hbm, hbm, hbm),
            input_output_aliases={0: 0},
            scratch_shapes=[
                pltpu.VMEM((VOCAB - EARLY_ROWS - HEAD, DIM), F32), pltpu.VMEM((1, LOC), F32), pltpu.VMEM((1, 1), F32),
                pltpu.SemaphoreType.DMA((len(LATE_TILES),)), pltpu.SemaphoreType.DMA((3,)),
            ],
            compiler_params=pltpu.CompilerParams(vmem_limit_bytes=30 * 1024 * 1024),
            cost_estimate=pl.CostEstimate(flops=2 * TOK * VOCAB * DIM, bytes_accessed=4 * VOCAB * DIM, transcendentals=0),
            name="embed",
        )(early, dz, head, x_all, small)
        d_hidden, d_gain, d_bias = pl.pallas_call(
            norm_kernel,
            out_shape=(shape((LOC, DIM), BF16), shape((1, DIM), F32), shape((1, DIM), F32)),
            in_specs=[vmem] * 7,
            out_specs=(vmem,) * 3,
            scratch_shapes=[pltpu.VMEM((TP, 8, DIM), F32)],
            compiler_params=pltpu.CompilerParams(vmem_limit_bytes=8 * 1024 * 1024),
            name="norm",
        )(pays[0], *moved, xh, rstd, small)
        return tok.reshape(LOC), mean.reshape(1), d_hidden, d_embed, d_gain.reshape(DIM), d_bias.reshape(DIM)

    row_spec = P(("dp", "tp"))
    mat_spec = P(("dp", "tp"), None)
    return jax.shard_map(
        group_step, mesh=mesh,
        in_specs=(mat_spec, P(None), P(None), P("tp", None), P("tp"), row_spec, row_spec),
        out_specs=(row_spec, P("dp"), mat_spec, mat_spec, P("dp"), P("dp")), check_vma=False,
    )
```

```python
import functools

import jax
import jax.numpy as jnp
from jax import lax
from jax.experimental import pallas as pl
from jax.experimental.pallas import tpu as pltpu
from jax.sharding import PartitionSpec as P

SOFT_CAP = 30.0
Z_COEF = 1e-4
LN_EPS = 1e-5
LOG2E = 1.4426950408889634
MESH = pl.DeviceIdType.MESH
F32 = jnp.float32
BF16 = jnp.bfloat16

TP = 4
TOK = 128
LOC = TOK // TP
DIM = 512
VOCAB = 12672
TILE = 256
GROUP = 7 * TILE
GROUPS = VOCAB // GROUP
TAIL = VOCAB - GROUP * GROUPS
BLK = 32
TURN = 2
TURNED = TURN * GROUP
FWD = [7] * 6 + [4, 2, 2]


def row_sum(val):
    return jnp.sum(val, axis=-1, keepdims=True)


def main_kernel(
    hid_hbm, gain_hbm, bias_hbm, emb_ref, valid_hbm, tgt_hbm, mask_hbm,
    small_ref, xh_v, rstd_v, coef_ref, tgt_v, x_ref, g_v, emb_v,
    hid_ref, gain_ref, bias_ref, valid_ref, tgt_ref, mask_ref,
    hid_all, meta_v, stat_v, acc_v, z_v, embt_v, ok_v,
    emb_sem, send_sem, recv_sem, in_sem,
):
    me = lax.axis_index("tp")
    dp = lax.axis_index("dp")
    barrier = pltpu.get_barrier_semaphore()
    for k in range(1, TP):
        pl.semaphore_signal(barrier, inc=1, device_id=(dp, lax.rem(me + k, TP)), device_id_type=MESH)

    ins = [
        pltpu.make_async_copy(src, dst, in_sem.at[k])
        for k, (src, dst) in enumerate([
            (hid_hbm, hid_ref), (tgt_hbm, tgt_ref), (mask_hbm, mask_ref),
            (gain_hbm, gain_ref), (bias_hbm, bias_ref), (valid_hbm, valid_ref),
        ])
    ]
    for cp in ins:
        cp.start()
    chunks = [(j * GROUP, GROUP) for j in range(GROUPS - 1)]
    chunks.append(((GROUPS - 1) * GROUP, GROUP + TAIL))
    emb_copies = [
        pltpu.make_async_copy(emb_ref.at[pl.ds(s, n), :], emb_v.at[pl.ds(s, n), :], emb_sem.at[k])
        for k, (s, n) in enumerate(chunks)
    ]
    for cp in emb_copies:
        cp.start()

    my_rows = pl.ds(pl.multiple_of(me * LOC, LOC), LOC)
    my_meta = pl.ds(pl.multiple_of(me * 8, 8), 8)
    ins[0].wait()
    pl.semaphore_wait(barrier, TP - 1)

    def push(src, dst, idx):
        copies = []
        for k in range(1, TP):
            cp = pltpu.make_async_remote_copy(
                src_ref=src(k), dst_ref=dst, send_sem=send_sem.at[3 * idx + k - 1], recv_sem=recv_sem.at[3 * idx + k - 1],
                device_id=(dp, lax.rem(me + k, TP)), device_id_type=MESH,
            )
            cp.start()
            copies.append(cp)
        return copies

    first = push(lambda k: hid_ref, hid_all.at[my_rows, :], 0)
    for cp in ins[1:3]:
        cp.wait()
    lane = lax.broadcasted_iota(jnp.int32, (1, TOK), 1)
    mine = (lane // LOC) == me
    tgt4 = jnp.concatenate([tgt_ref[...]] * TP, axis=1)
    mask4 = jnp.concatenate([mask_ref[...]] * TP, axis=1)
    meta_v[my_meta, :] = jnp.concatenate(
        [jnp.where(mine, tgt4, 0), jnp.where(mine, mask4, 0), jnp.zeros((6, TOK), jnp.int32)], axis=0
    )
    hid_all[my_rows, :] = hid_ref[...]
    first += push(lambda k: meta_v.at[my_meta, :], meta_v.at[my_meta, :], 1)
    for cp in ins[3:]:
        cp.wait()
    ok_v[...] = valid_ref[...].astype(F32)
    for cp, (g0, n) in zip(emb_copies[:TURN], chunks):
        cp.wait()
        for s in range(g0, g0 + n, TILE):
            embt_v[:, pl.ds(s, TILE)] = jnp.transpose(emb_v[pl.ds(s, TILE), :])
    for cp in first:
        cp.wait_recv()

    meta = meta_v[0:8, :] + meta_v[8:16, :] + meta_v[16:24, :] + meta_v[24:32, :]
    tgt_row = meta[0:1, :]
    mask_row = meta[1:2, :].astype(F32)
    tok_count = row_sum(mask_row)
    tgt_col = jnp.transpose(jnp.broadcast_to(tgt_row, (TOK, TOK)))

    h = hid_all[...].astype(F32)
    mean_val = row_sum(h) * (1.0 / DIM)
    cent = h - mean_val
    var_val = row_sum(cent * cent) * (1.0 / DIM)
    rstd = lax.rsqrt(var_val + LN_EPS)
    xh = cent * rstd
    xh_v[...] = xh
    rstd_v[...] = jnp.broadcast_to(rstd, (TOK, TOK))
    x_ref[...] = (xh * gain_ref[...] + bias_ref[...]).astype(BF16)

    tgt_v[...] = tgt_col - me * VOCAB
    lane_blk = lax.broadcasted_iota(jnp.int32, (BLK, TOK), 1)
    plain = [(s, TILE) for s in range(0, TURNED, TILE)]
    other = [(s, min(TILE, VOCAB - s)) for s in range(TURNED, VOCAB, TILE)]
    tiles = []
    while plain or other:
        if other:
            tiles.append(other.pop(0))
        if plain:
            tiles.append(plain.pop(0))
    groups = []
    for n in FWD:
        groups.append(tiles[:n])
        tiles = tiles[n:]

    def logits(j):
        pos = 0
        for col, w in groups[j]:
            if col < TURNED:
                z = jnp.dot(x_ref[...], embt_v[:, pl.ds(col, w)], preferred_element_type=F32)
            else:
                z = lax.dot_general(
                    x_ref[...], emb_v[pl.ds(col, w), :], (((1,), (1,)), ((), ())), preferred_element_type=F32
                )
            z_v[j % 2, :, pl.ds(pos, w)] = z
            pos += w

    def softmax_pass(j):
        cols = [c for col, w in groups[j] for c in range(col, col + w, TOK)]
        for tb in range(TOK // BLK):
            rows = pl.ds(tb * BLK, BLK)
            tgt = tgt_v[rows, :]
            s_acc = acc_v[0, rows, :]
            t_acc = acc_v[1, rows, :]
            for first_c in range(0, len(cols), 2):
                pick = 0.0
                for c in range(first_c, min(first_c + 2, len(cols))):
                    col = cols[c]
                    t = jnp.tanh(z_v[j % 2, rows, pl.ds(c * TOK, TOK)] * (1.0 / SOFT_CAP))
                    e = jnp.exp2(t * (SOFT_CAP * LOG2E)) * ok_v[col // TOK:col // TOK + 1, :]
                    pick = jnp.where(tgt == lane_blk + col, t, pick)
                    g_v[rows, pl.ds(col, TOK)] = e * (1.0 - t * t)
                    s_acc += e
                t_acc += pick
            acc_v[0, rows, :] = s_acc
            acc_v[1, rows, :] = t_acc

    for cp in emb_copies[TURN:]:
        cp.wait()
    acc_v[...] = jnp.zeros_like(acc_v)
    for j in range(len(groups)):
        logits(j)
        if j > 0:
            softmax_pass(j - 1)
    softmax_pass(len(groups) - 1)

    s_loc = jnp.sum(jnp.transpose(acc_v[0]), axis=0, keepdims=True)
    t_loc = jnp.sum(jnp.transpose(acc_v[1]), axis=0, keepdims=True)
    stat_v[my_meta, :] = jnp.concatenate([s_loc, t_loc, jnp.zeros((6, TOK), F32)], axis=0)
    second = push(lambda k: stat_v.at[my_meta, :], stat_v.at[my_meta, :], 2)
    for cp in first:
        cp.wait_send()
    for cp in second:
        cp.wait_recv()
    stats = stat_v[0:8, :] + stat_v[8:16, :] + stat_v[16:24, :] + stat_v[24:32, :]
    sum_exp = stats[0:1, :]
    t_tgt = stats[1:2, :]
    lse = jnp.log(sum_exp)
    coef = mask_row / tok_count
    a_row = (1.0 + 2.0 * Z_COEF * lse) * coef / sum_exp
    c_row = coef * (1.0 - t_tgt * t_tgt)
    coef_ref[0] = jnp.transpose(jnp.broadcast_to(a_row, (TOK, TOK)))
    coef_ref[1] = jnp.transpose(jnp.broadcast_to(c_row, (TOK, TOK)))
    pad = jnp.zeros((1, DIM - TOK), F32)
    small_ref[...] = jnp.concatenate(
        [jnp.concatenate([row, pad], axis=1) for row in (sum_exp, t_tgt, mask_row)] + [gain_ref[...], jnp.zeros((4, DIM), F32)],
        axis=0,
    )
    for cp in second:
        cp.wait_send()


EARLY = 2
EARLY_ROWS = 2688
EARLY_TILES = [256, 640, 896, 896]
HEAD = 256
LATE_TILES = [256, 256] + [768] * 12


def write_rows(dz_ref, x_ref, out_ref, stage, sem, start, first, tiles):
    copies = []
    for k, n in enumerate(tiles):
        rows = pl.ds(start, n)
        local = pl.ds(start - first, n)
        stage[local, :] = lax.dot_general(
            dz_ref[:, rows], x_ref[...], (((0,), (0,)), ((), ())), preferred_element_type=F32
        )
        cp = pltpu.make_async_copy(stage.at[local, :], out_ref.at[rows, :], sem.at[k])
        cp.start(priority=k % 2)
        copies.append(cp)
        start += n
    return copies


def grad_kernel(
    g_ref, emb_ref, x_ref, xh_ref, coef_ref, tgt_ref, demb_ref, dz_ref, head_ref, pay0, pay1, pay2, pay3, stage, dx_v, out_sem
):
    me = lax.axis_index("tp")
    lane_blk = lax.broadcasted_iota(jnp.int32, (BLK, TOK), 1)
    groups = [(j * GROUP, GROUP) for j in range(GROUPS - 1)]
    groups.append(((GROUPS - 1) * GROUP, GROUP + TAIL))

    def logit_grad(g0, n):
        for tb in range(TOK // BLK):
            rows = pl.ds(tb * BLK, BLK)
            tgt = tgt_ref[rows, :]
            a_blk = coef_ref[0, rows, :]
            c_blk = coef_ref[1, rows, :]
            for c in range(n // TOK):
                cols = pl.ds(g0 + c * TOK, TOK)
                hit = tgt == lane_blk + (g0 + c * TOK)
                dz_ref[rows, cols] = (a_blk * g_ref[rows, cols] - jnp.where(hit, c_blk, 0.0)).astype(BF16)

    for g0, n in groups[:EARLY]:
        logit_grad(g0, n)
    copies = write_rows(dz_ref, x_ref, demb_ref, stage, out_sem, 0, 0, EARLY_TILES)
    head_ref[...] = lax.dot_general(
        dz_ref[:, pl.ds(EARLY_ROWS, HEAD)], x_ref[...], (((0,), (0,)), ((), ())), preferred_element_type=F32
    )
    dx = 0.0
    for j, (g0, n) in enumerate(groups):
        if j >= EARLY:
            logit_grad(g0, n)
        dx += jnp.dot(dz_ref[:, pl.ds(g0, n)], emb_ref[pl.ds(g0, n), :], preferred_element_type=F32)
    dx_v[...] = dx
    gb = jnp.concatenate(
        [jnp.sum(dx * xh_ref[...], axis=0, keepdims=True), jnp.sum(dx, axis=0, keepdims=True), jnp.zeros((6, DIM), F32)], axis=0
    )
    for k, pay in enumerate((pay0, pay1, pay2, pay3)):
        pay[0:LOC, :] = dx_v[pl.ds(pl.multiple_of((me ^ k) * LOC, LOC), LOC), :]
        pay[LOC:, :] = gb
    for cp in copies:
        cp.wait()


def embed_kernel(
    demb_in, dz_ref, head_ref, x_ref, small_ref, demb_ref, tok_ref, mean_ref, stage, tok_v, mean_v, out_sem, side_sem
):
    sides = [
        pltpu.make_async_copy(src, dst, side_sem.at[k])
        for k, (src, dst) in enumerate([
            (head_ref, demb_ref.at[pl.ds(EARLY_ROWS, HEAD), :]), (tok_v, tok_ref), (mean_v, mean_ref),
        ])
    ]
    sides[0].start()
    copies = write_rows(dz_ref, x_ref, demb_ref, stage, out_sem, EARLY_ROWS + HEAD, EARLY_ROWS + HEAD, LATE_TILES)
    mask_row = small_ref[2:3, 0:TOK]
    lse = jnp.log(small_ref[0:1, 0:TOK])
    loss = (lse - SOFT_CAP * small_ref[1:2, 0:TOK] + Z_COEF * lse * lse) * mask_row
    mean_v[...] = row_sum(loss) / row_sum(mask_row)
    tok_v[...] = pltpu.roll(loss, lax.rem(TOK - lax.axis_index("tp") * LOC, TOK), 1)[:, 0:LOC]
    for cp in sides[1:]:
        cp.start()
    for cp in copies + sides:
        cp.wait()


def norm_kernel(p0, p1, p2, p3, xh_ref, rstd_ref, gain_in, dhid_ref, gain_ref, bias_ref, gb_v):
    me = lax.axis_index("tp")
    for k, pay in enumerate((p0, p1, p2, p3)):
        gb_v[me ^ k] = pay[LOC:, :]
    gb = gb_v[0] + gb_v[1] + gb_v[2] + gb_v[3]
    gain_ref[...] = gb[0:1, :]
    bias_ref[...] = gb[1:2, :]
    my_rows = pl.ds(pl.multiple_of(me * LOC, LOC), LOC)
    xh = xh_ref[my_rows, :]
    dxh = (p0[0:LOC, :] + p1[0:LOC, :] + p2[0:LOC, :] + p3[0:LOC, :]) * gain_in[3:4, :]
    m1 = row_sum(dxh) * (1.0 / DIM)
    m2 = row_sum(dxh * xh) * (1.0 / DIM)
    dhid_ref[...] = (rstd_ref[my_rows, 0:1] * (dxh - m1 - xh * m2)).astype(BF16)


def solution(mesh):
    vmem = pl.BlockSpec(memory_space=pltpu.VMEM)
    hbm = pl.BlockSpec(memory_space=pltpu.HBM)

    def group_step(hidden, ln_gain, ln_bias, out_embed, vocab_valid, targets, loss_mask):
        shape = jax.ShapeDtypeStruct
        small, xh, rstd, coef, tgt, x_all, g_all, emb = pl.pallas_call(
            main_kernel,
            out_shape=(
                shape((8, DIM), F32), shape((TOK, DIM), F32), shape((TOK, TOK), F32), shape((2, TOK, TOK), F32),
                shape((TOK, TOK), jnp.int32), shape((TOK, DIM), BF16), shape((TOK, VOCAB), F32), shape((VOCAB, DIM), BF16),
            ),
            in_specs=[hbm] * 7,
            out_specs=(vmem,) * 8,
            scratch_shapes=[
                pltpu.VMEM((LOC, DIM), BF16),
                pltpu.VMEM((1, DIM), F32),
                pltpu.VMEM((1, DIM), F32),
                pltpu.VMEM((VOCAB // TOK, TOK), jnp.int32),
                pltpu.VMEM((1, LOC), jnp.int32),
                pltpu.VMEM((1, LOC), jnp.int32),
                pltpu.VMEM((TOK, DIM), BF16),
                pltpu.VMEM((8 * TP, TOK), jnp.int32),
                pltpu.VMEM((8 * TP, TOK), F32),
                pltpu.VMEM((2, TOK, TOK), F32),
                pltpu.VMEM((2, TOK, GROUP), F32),
                pltpu.VMEM((DIM, TURNED), BF16),
                pltpu.VMEM((VOCAB // TOK, TOK), F32),
                pltpu.SemaphoreType.DMA((GROUPS,)),
                pltpu.SemaphoreType.DMA((9,)),
                pltpu.SemaphoreType.DMA((9,)),
                pltpu.SemaphoreType.DMA((6,)),
            ],
            compiler_params=pltpu.CompilerParams(collective_id=0, has_side_effects=True, vmem_limit_bytes=30 * 1024 * 1024),
            name="main",
        )(
            *(
                pltpu.with_memory_space_constraint(val, pltpu.HBM)
                for val in (
                    hidden, ln_gain.reshape(1, DIM), ln_bias.reshape(1, DIM), out_embed,
                    vocab_valid.reshape(VOCAB // TOK, TOK), targets.reshape(1, LOC), loss_mask.reshape(1, LOC),
                )
            )
        )
        part = shape((LOC + 8, DIM), F32)
        early, dz, head, *pays = pl.pallas_call(
            grad_kernel,
            out_shape=(shape((VOCAB, DIM), F32), shape((TOK, VOCAB), BF16), shape((HEAD, DIM), F32), part, part, part, part),
            in_specs=[vmem] * 6,
            out_specs=(hbm,) + (vmem,) * 6,
            scratch_shapes=[
                pltpu.VMEM((EARLY_ROWS, DIM), F32), pltpu.VMEM((TOK, DIM), F32), pltpu.SemaphoreType.DMA((len(EARLY_TILES),)),
            ],
            compiler_params=pltpu.CompilerParams(vmem_limit_bytes=16 * 1024 * 1024),
            name="grad",
        )(g_all, emb, x_all, xh, coef, tgt)
        moved = [lax.ppermute(pays[k], "tp", [(i, i ^ k) for i in range(TP)]) for k in range(1, TP)]
        d_embed, tok, mean = pl.pallas_call(
            embed_kernel,
            out_shape=(shape((VOCAB, DIM), F32), shape((1, LOC), F32), shape((1, 1), F32)),
            in_specs=[hbm] + [vmem] * 4,
            out_specs=(hbm, hbm, hbm),
            input_output_aliases={0: 0},
            scratch_shapes=[
                pltpu.VMEM((VOCAB - EARLY_ROWS - HEAD, DIM), F32), pltpu.VMEM((1, LOC), F32), pltpu.VMEM((1, 1), F32),
                pltpu.SemaphoreType.DMA((len(LATE_TILES),)), pltpu.SemaphoreType.DMA((3,)),
            ],
            compiler_params=pltpu.CompilerParams(vmem_limit_bytes=30 * 1024 * 1024),
            cost_estimate=pl.CostEstimate(flops=2 * TOK * VOCAB * DIM, bytes_accessed=4 * VOCAB * DIM, transcendentals=0),
            name="embed",
        )(early, dz, head, x_all, small)
        d_hidden, d_gain, d_bias = pl.pallas_call(
            norm_kernel,
            out_shape=(shape((LOC, DIM), BF16), shape((1, DIM), F32), shape((1, DIM), F32)),
            in_specs=[vmem] * 7,
            out_specs=(vmem,) * 3,
            scratch_shapes=[pltpu.VMEM((TP, 8, DIM), F32)],
            compiler_params=pltpu.CompilerParams(vmem_limit_bytes=8 * 1024 * 1024),
            name="norm",
        )(pays[0], *moved, xh, rstd, small)
        return tok.reshape(LOC), mean.reshape(1), d_hidden, d_embed, d_gain.reshape(DIM), d_bias.reshape(DIM)

    row_spec = P(("dp", "tp"))
    mat_spec = P(("dp", "tp"), None)
    return jax.shard_map(
        group_step, mesh=mesh,
        in_specs=(mat_spec, P(None), P(None), P("tp", None), P("tp"), row_spec, row_spec),
        out_specs=(row_spec, P("dp"), mat_spec, mat_spec, P("dp"), P("dp")), check_vma=False,
    )
```

```python
import functools

import jax
import jax.numpy as jnp
from jax import lax
from jax.experimental import pallas as pl
from jax.experimental.pallas import tpu as pltpu
from jax.sharding import PartitionSpec as P

SOFT_CAP = 30.0
Z_COEF = 1e-4
LN_EPS = 1e-5
LOG2E = 1.4426950408889634
MESH = pl.DeviceIdType.MESH
F32 = jnp.float32
BF16 = jnp.bfloat16

TP = 4
TOK = 128
LOC = TOK // TP
DIM = 512
VOCAB = 12672
TILE = 256
GROUP = 7 * TILE
GROUPS = VOCAB // GROUP
TAIL = VOCAB - GROUP * GROUPS
BLK = 32
TURN = 2
TURNED = TURN * GROUP
FWD = [7] * 6 + [4, 2, 2]


def row_sum(val):
    return jnp.sum(val, axis=-1, keepdims=True)


def main_kernel(
    hid_hbm, gain_hbm, bias_hbm, emb_ref, valid_hbm, tgt_hbm, mask_hbm,
    small_ref, xh_v, rstd_v, coef_ref, tgt_v, x_ref, g_v, emb_v,
    hid_ref, gain_ref, bias_ref, valid_ref, tgt_ref, mask_ref,
    hid_all, meta_v, stat_v, acc_v, z_v, embt_v, ok_v,
    emb_sem, send_sem, recv_sem, in_sem,
):
    me = lax.axis_index("tp")
    dp = lax.axis_index("dp")
    barrier = pltpu.get_barrier_semaphore()
    for k in (2, 3, 1):
        pl.semaphore_signal(barrier, inc=1, device_id=(dp, me ^ k), device_id_type=MESH)

    ins = [
        pltpu.make_async_copy(src, dst, in_sem.at[k])
        for k, (src, dst) in enumerate([
            (hid_hbm, hid_ref), (tgt_hbm, tgt_ref), (mask_hbm, mask_ref),
            (gain_hbm, gain_ref), (bias_hbm, bias_ref), (valid_hbm, valid_ref),
        ])
    ]
    for cp in ins:
        cp.start()
    chunks = [(j * GROUP, GROUP) for j in range(GROUPS - 1)]
    chunks.append(((GROUPS - 1) * GROUP, GROUP + TAIL))
    emb_copies = [
        pltpu.make_async_copy(emb_ref.at[pl.ds(s, n), :], emb_v.at[pl.ds(s, n), :], emb_sem.at[k])
        for k, (s, n) in enumerate(chunks)
    ]
    for cp in emb_copies:
        cp.start()

    my_rows = pl.ds(pl.multiple_of(me * LOC, LOC), LOC)
    my_meta = pl.ds(pl.multiple_of(me * 8, 8), 8)
    ins[0].wait()
    pl.semaphore_wait(barrier, TP - 1)

    def push(src, dst, idx):
        copies = []
        for k in (2, 3, 1):
            cp = pltpu.make_async_remote_copy(
                src_ref=src(k), dst_ref=dst, send_sem=send_sem.at[3 * idx + k - 1], recv_sem=recv_sem.at[3 * idx + k - 1],
                device_id=(dp, me ^ k), device_id_type=MESH,
            )
            cp.start()
            copies.append(cp)
        return copies

    first = push(lambda k: hid_ref, hid_all.at[my_rows, :], 0)
    for cp in ins[1:3]:
        cp.wait()
    lane = lax.broadcasted_iota(jnp.int32, (1, TOK), 1)
    mine = (lane // LOC) == me
    tgt4 = jnp.concatenate([tgt_ref[...]] * TP, axis=1)
    mask4 = jnp.concatenate([mask_ref[...]] * TP, axis=1)
    meta_v[my_meta, :] = jnp.concatenate(
        [jnp.where(mine, tgt4, 0), jnp.where(mine, mask4, 0), jnp.zeros((6, TOK), jnp.int32)], axis=0
    )
    hid_all[my_rows, :] = hid_ref[...]
    first += push(lambda k: meta_v.at[my_meta, :], meta_v.at[my_meta, :], 1)
    for cp in ins[3:]:
        cp.wait()
    ok_v[...] = valid_ref[...].astype(F32)
    for cp, (g0, n) in zip(emb_copies[:TURN], chunks):
        cp.wait()
        for s in range(g0, g0 + n, TILE):
            embt_v[:, pl.ds(s, TILE)] = jnp.transpose(emb_v[pl.ds(s, TILE), :])
    for cp in first:
        cp.wait_recv()

    meta = meta_v[0:8, :] + meta_v[8:16, :] + meta_v[16:24, :] + meta_v[24:32, :]
    tgt_row = meta[0:1, :]
    mask_row = meta[1:2, :].astype(F32)
    tok_count = row_sum(mask_row)
    tgt_col = jnp.transpose(jnp.broadcast_to(tgt_row, (TOK, TOK)))

    h = hid_all[...].astype(F32)
    mean_val = row_sum(h) * (1.0 / DIM)
    cent = h - mean_val
    var_val = row_sum(cent * cent) * (1.0 / DIM)
    rstd = lax.rsqrt(var_val + LN_EPS)
    xh = cent * rstd
    xh_v[...] = xh
    rstd_v[...] = jnp.broadcast_to(rstd, (TOK, TOK))
    x_ref[...] = (xh * gain_ref[...] + bias_ref[...]).astype(BF16)

    tgt_v[...] = tgt_col - me * VOCAB
    lane_blk = lax.broadcasted_iota(jnp.int32, (BLK, TOK), 1)
    plain = [(s, TILE) for s in range(0, TURNED, TILE)]
    other = [(s, min(TILE, VOCAB - s)) for s in range(TURNED, VOCAB, TILE)]
    tiles = []
    while plain or other:
        if other:
            tiles.append(other.pop(0))
        if plain:
            tiles.append(plain.pop(0))
    groups = []
    for n in FWD:
        groups.append(tiles[:n])
        tiles = tiles[n:]

    def logits(j):
        pos = 0
        for col, w in groups[j]:
            if col < TURNED:
                z = jnp.dot(x_ref[...], embt_v[:, pl.ds(col, w)], preferred_element_type=F32)
            else:
                z = lax.dot_general(
                    x_ref[...], emb_v[pl.ds(col, w), :], (((1,), (1,)), ((), ())), preferred_element_type=F32
                )
            z_v[j % 2, :, pl.ds(pos, w)] = z
            pos += w

    def softmax_pass(j):
        cols = [c for col, w in groups[j] for c in range(col, col + w, TOK)]
        for tb in range(TOK // BLK):
            rows = pl.ds(tb * BLK, BLK)
            tgt = tgt_v[rows, :]
            s_acc = acc_v[0, rows, :]
            t_acc = acc_v[1, rows, :]
            for first_c in range(0, len(cols), 2):
                pick = 0.0
                for c in range(first_c, min(first_c + 2, len(cols))):
                    col = cols[c]
                    t = jnp.tanh(z_v[j % 2, rows, pl.ds(c * TOK, TOK)] * (1.0 / SOFT_CAP))
                    e = jnp.exp2(t * (SOFT_CAP * LOG2E)) * ok_v[col // TOK:col // TOK + 1, :]
                    pick = jnp.where(tgt == lane_blk + col, t, pick)
                    g_v[rows, pl.ds(col, TOK)] = e * (1.0 - t * t)
                    s_acc += e
                t_acc += pick
            acc_v[0, rows, :] = s_acc
            acc_v[1, rows, :] = t_acc

    for cp in emb_copies[TURN:]:
        cp.wait()
    acc_v[...] = jnp.zeros_like(acc_v)
    for j in range(len(groups)):
        logits(j)
        if j > 0:
            softmax_pass(j - 1)
    softmax_pass(len(groups) - 1)

    s_loc = jnp.sum(jnp.transpose(acc_v[0]), axis=0, keepdims=True)
    t_loc = jnp.sum(jnp.transpose(acc_v[1]), axis=0, keepdims=True)
    stat_v[my_meta, :] = jnp.concatenate([s_loc, t_loc, jnp.zeros((6, TOK), F32)], axis=0)
    second = push(lambda k: stat_v.at[my_meta, :], stat_v.at[my_meta, :], 2)
    for cp in first:
        cp.wait_send()
    for cp in second:
        cp.wait_recv()
    stats = stat_v[0:8, :] + stat_v[8:16, :] + stat_v[16:24, :] + stat_v[24:32, :]
    sum_exp = stats[0:1, :]
    t_tgt = stats[1:2, :]
    lse = jnp.log(sum_exp)
    coef = mask_row / tok_count
    a_row = (1.0 + 2.0 * Z_COEF * lse) * coef / sum_exp
    c_row = coef * (1.0 - t_tgt * t_tgt)
    coef_ref[0] = jnp.transpose(jnp.broadcast_to(a_row, (TOK, TOK)))
    coef_ref[1] = jnp.transpose(jnp.broadcast_to(c_row, (TOK, TOK)))
    pad = jnp.zeros((1, DIM - TOK), F32)
    small_ref[...] = jnp.concatenate(
        [jnp.concatenate([row, pad], axis=1) for row in (sum_exp, t_tgt, mask_row)] + [gain_ref[...], jnp.zeros((4, DIM), F32)],
        axis=0,
    )
    for cp in second:
        cp.wait_send()


EARLY = 2
EARLY_ROWS = 2688
EARLY_TILES = [256, 640, 896, 896]
HEAD = 256
LATE_TILES = [256, 256] + [768] * 12


def write_rows(dz_ref, x_ref, out_ref, stage, sem, start, first, tiles):
    copies = []
    for k, n in enumerate(tiles):
        rows = pl.ds(start, n)
        local = pl.ds(start - first, n)
        stage[local, :] = lax.dot_general(
            dz_ref[:, rows], x_ref[...], (((0,), (0,)), ((), ())), preferred_element_type=F32
        )
        cp = pltpu.make_async_copy(stage.at[local, :], out_ref.at[rows, :], sem.at[k])
        cp.start(priority=k % 2)
        copies.append(cp)
        start += n
    return copies


def grad_kernel(
    g_ref, emb_ref, x_ref, xh_ref, coef_ref, tgt_ref, demb_ref, dz_ref, head_ref, pay0, pay1, pay2, pay3, stage, dx_v, out_sem
):
    me = lax.axis_index("tp")
    lane_blk = lax.broadcasted_iota(jnp.int32, (BLK, TOK), 1)
    groups = [(j * GROUP, GROUP) for j in range(GROUPS - 1)]
    groups.append(((GROUPS - 1) * GROUP, GROUP + TAIL))

    def logit_grad(g0, n):
        for tb in range(TOK // BLK):
            rows = pl.ds(tb * BLK, BLK)
            tgt = tgt_ref[rows, :]
            a_blk = coef_ref[0, rows, :]
            c_blk = coef_ref[1, rows, :]
            for c in range(n // TOK):
                cols = pl.ds(g0 + c * TOK, TOK)
                hit = tgt == lane_blk + (g0 + c * TOK)
                dz_ref[rows, cols] = (a_blk * g_ref[rows, cols] - jnp.where(hit, c_blk, 0.0)).astype(BF16)

    for g0, n in groups[:EARLY]:
        logit_grad(g0, n)
    copies = write_rows(dz_ref, x_ref, demb_ref, stage, out_sem, 0, 0, EARLY_TILES)
    head_ref[...] = lax.dot_general(
        dz_ref[:, pl.ds(EARLY_ROWS, HEAD)], x_ref[...], (((0,), (0,)), ((), ())), preferred_element_type=F32
    )
    dx = 0.0
    for j, (g0, n) in enumerate(groups):
        if j >= EARLY:
            logit_grad(g0, n)
        dx += jnp.dot(dz_ref[:, pl.ds(g0, n)], emb_ref[pl.ds(g0, n), :], preferred_element_type=F32)
    dx_v[...] = dx
    gb = jnp.concatenate(
        [jnp.sum(dx * xh_ref[...], axis=0, keepdims=True), jnp.sum(dx, axis=0, keepdims=True), jnp.zeros((6, DIM), F32)], axis=0
    )
    for k, pay in enumerate((pay0, pay1, pay2, pay3)):
        pay[0:LOC, :] = dx_v[pl.ds(pl.multiple_of((me ^ k) * LOC, LOC), LOC), :]
        pay[LOC:, :] = gb
    for cp in copies:
        cp.wait()


def embed_kernel(
    demb_in, dz_ref, head_ref, x_ref, small_ref, demb_ref, tok_ref, mean_ref, stage, tok_v, mean_v, out_sem, side_sem
):
    sides = [
        pltpu.make_async_copy(src, dst, side_sem.at[k])
        for k, (src, dst) in enumerate([
            (head_ref, demb_ref.at[pl.ds(EARLY_ROWS, HEAD), :]), (tok_v, tok_ref), (mean_v, mean_ref),
        ])
    ]
    sides[0].start()
    copies = write_rows(dz_ref, x_ref, demb_ref, stage, out_sem, EARLY_ROWS + HEAD, EARLY_ROWS + HEAD, LATE_TILES)
    mask_row = small_ref[2:3, 0:TOK]
    lse = jnp.log(small_ref[0:1, 0:TOK])
    loss = (lse - SOFT_CAP * small_ref[1:2, 0:TOK] + Z_COEF * lse * lse) * mask_row
    mean_v[...] = row_sum(loss) / row_sum(mask_row)
    tok_v[...] = pltpu.roll(loss, lax.rem(TOK - lax.axis_index("tp") * LOC, TOK), 1)[:, 0:LOC]
    for cp in sides[1:]:
        cp.start()
    for cp in copies + sides:
        cp.wait()


def norm_kernel(p0, p1, p2, p3, xh_ref, rstd_ref, gain_in, dhid_ref, gain_ref, bias_ref, gb_v):
    me = lax.axis_index("tp")
    for k, pay in enumerate((p0, p1, p2, p3)):
        gb_v[me ^ k] = pay[LOC:, :]
    gb = gb_v[0] + gb_v[1] + gb_v[2] + gb_v[3]
    gain_ref[...] = gb[0:1, :]
    bias_ref[...] = gb[1:2, :]
    my_rows = pl.ds(pl.multiple_of(me * LOC, LOC), LOC)
    xh = xh_ref[my_rows, :]
    dxh = (p0[0:LOC, :] + p1[0:LOC, :] + p2[0:LOC, :] + p3[0:LOC, :]) * gain_in[3:4, :]
    m1 = row_sum(dxh) * (1.0 / DIM)
    m2 = row_sum(dxh * xh) * (1.0 / DIM)
    dhid_ref[...] = (rstd_ref[my_rows, 0:1] * (dxh - m1 - xh * m2)).astype(BF16)


def solution(mesh):
    vmem = pl.BlockSpec(memory_space=pltpu.VMEM)
    hbm = pl.BlockSpec(memory_space=pltpu.HBM)

    def group_step(hidden, ln_gain, ln_bias, out_embed, vocab_valid, targets, loss_mask):
        shape = jax.ShapeDtypeStruct
        small, xh, rstd, coef, tgt, x_all, g_all, emb = pl.pallas_call(
            main_kernel,
            out_shape=(
                shape((8, DIM), F32), shape((TOK, DIM), F32), shape((TOK, TOK), F32), shape((2, TOK, TOK), F32),
                shape((TOK, TOK), jnp.int32), shape((TOK, DIM), BF16), shape((TOK, VOCAB), F32), shape((VOCAB, DIM), BF16),
            ),
            in_specs=[hbm] * 7,
            out_specs=(vmem,) * 8,
            scratch_shapes=[
                pltpu.VMEM((LOC, DIM), BF16),
                pltpu.VMEM((1, DIM), F32),
                pltpu.VMEM((1, DIM), F32),
                pltpu.VMEM((VOCAB // TOK, TOK), jnp.int32),
                pltpu.VMEM((1, LOC), jnp.int32),
                pltpu.VMEM((1, LOC), jnp.int32),
                pltpu.VMEM((TOK, DIM), BF16),
                pltpu.VMEM((8 * TP, TOK), jnp.int32),
                pltpu.VMEM((8 * TP, TOK), F32),
                pltpu.VMEM((2, TOK, TOK), F32),
                pltpu.VMEM((2, TOK, GROUP), F32),
                pltpu.VMEM((DIM, TURNED), BF16),
                pltpu.VMEM((VOCAB // TOK, TOK), F32),
                pltpu.SemaphoreType.DMA((GROUPS,)),
                pltpu.SemaphoreType.DMA((9,)),
                pltpu.SemaphoreType.DMA((9,)),
                pltpu.SemaphoreType.DMA((6,)),
            ],
            compiler_params=pltpu.CompilerParams(collective_id=0, has_side_effects=True, vmem_limit_bytes=30 * 1024 * 1024),
            name="main",
        )(
            *(
                pltpu.with_memory_space_constraint(val, pltpu.HBM)
                for val in (
                    hidden, ln_gain.reshape(1, DIM), ln_bias.reshape(1, DIM), out_embed,
                    vocab_valid.reshape(VOCAB // TOK, TOK), targets.reshape(1, LOC), loss_mask.reshape(1, LOC),
                )
            )
        )
        part = shape((LOC + 8, DIM), F32)
        early, dz, head, *pays = pl.pallas_call(
            grad_kernel,
            out_shape=(shape((VOCAB, DIM), F32), shape((TOK, VOCAB), BF16), shape((HEAD, DIM), F32), part, part, part, part),
            in_specs=[vmem] * 6,
            out_specs=(hbm,) + (vmem,) * 6,
            scratch_shapes=[
                pltpu.VMEM((EARLY_ROWS, DIM), F32), pltpu.VMEM((TOK, DIM), F32), pltpu.SemaphoreType.DMA((len(EARLY_TILES),)),
            ],
            compiler_params=pltpu.CompilerParams(vmem_limit_bytes=16 * 1024 * 1024),
            name="grad",
        )(g_all, emb, x_all, xh, coef, tgt)
        moved = [lax.ppermute(pays[k], "tp", [(i, i ^ k) for i in range(TP)]) for k in range(1, TP)]
        d_embed, tok, mean = pl.pallas_call(
            embed_kernel,
            out_shape=(shape((VOCAB, DIM), F32), shape((1, LOC), F32), shape((1, 1), F32)),
            in_specs=[hbm] + [vmem] * 4,
            out_specs=(hbm, hbm, hbm),
            input_output_aliases={0: 0},
            scratch_shapes=[
                pltpu.VMEM((VOCAB - EARLY_ROWS - HEAD, DIM), F32), pltpu.VMEM((1, LOC), F32), pltpu.VMEM((1, 1), F32),
                pltpu.SemaphoreType.DMA((len(LATE_TILES),)), pltpu.SemaphoreType.DMA((3,)),
            ],
            compiler_params=pltpu.CompilerParams(vmem_limit_bytes=30 * 1024 * 1024),
            cost_estimate=pl.CostEstimate(flops=2 * TOK * VOCAB * DIM, bytes_accessed=4 * VOCAB * DIM, transcendentals=0),
            name="embed",
        )(early, dz, head, x_all, small)
        d_hidden, d_gain, d_bias = pl.pallas_call(
            norm_kernel,
            out_shape=(shape((LOC, DIM), BF16), shape((1, DIM), F32), shape((1, DIM), F32)),
            in_specs=[vmem] * 7,
            out_specs=(vmem,) * 3,
            scratch_shapes=[pltpu.VMEM((TP, 8, DIM), F32)],
            compiler_params=pltpu.CompilerParams(vmem_limit_bytes=8 * 1024 * 1024),
            name="norm",
        )(pays[0], *moved, xh, rstd, small)
        return tok.reshape(LOC), mean.reshape(1), d_hidden, d_embed, d_gain.reshape(DIM), d_bias.reshape(DIM)

    row_spec = P(("dp", "tp"))
    mat_spec = P(("dp", "tp"), None)
    return jax.shard_map(
        group_step, mesh=mesh,
        in_specs=(mat_spec, P(None), P(None), P("tp", None), P("tp"), row_spec, row_spec),
        out_specs=(row_spec, P("dp"), mat_spec, mat_spec, P("dp"), P("dp")), check_vma=False,
    )
```
